128 devices in a mesh: blk: 2 (over core), dp: 64 (over z, y, x).
Axes of the slice: x: 4, y: 4, z: 4, core: 2. Of those that a mesh axis runs over, the one named last changes fastest.
Arguments:
- queries: bfloat16 [16384, 256], P(('blk', 'dp')), may hold values from -1 to 1, as said below
- items: bfloat16 [16384, 256], P(('blk', 'dp')), may hold values from -1 to 1, as said below
Outputs:
- loss: float32 [], replicated
- question_slope: float32 [16384, 256], P(('blk', 'dp'))
- candidate_slope: float32 [16384, 256], P(('blk', 'dp'))
The draws below stay inside these ranges and needn't reach their ends.
Inputs may be any that keep to these rules, and one draw needn't show every extreme that they name: queries: entries lie between -1 and 1 and no row is zero; each query is close to its own item and to one item of the batch chosen by a random permutation (which may be its own). items: entries lie between -1 and 1 and no row is zero.
All inputs are finite; a program needn't handle non-finite values.
Results may differ from the reference program's by a relative error of at most 0.008.
Values may be sent and summed in bfloat16 or wider, within the bound.
No kernel may reach another device: no remote copies, remote signals or barrier semaphores. Data moves between devices by JAX's collectives and lax.ppermute only.
A program may use at most 64 MiB of HBM per device.

```python
import jax
import jax.numpy as jnp
from jax import lax

ROWS = 128
D = 256
BATCH = 16384


def pair_draw(key):
    items_raw = jax.random.truncated_normal(jax.random.fold_in(key, 11), -4.0, 4.0, (BATCH, D), jnp.float32) * 0.0625
    partner = jax.random.permutation(jax.random.fold_in(key, 12), BATCH)
    noise_part = jax.random.truncated_normal(jax.random.fold_in(key, 13), -4.0, 4.0, (BATCH, D), jnp.float32) * 0.0625
    mixture = 0.6 * items_raw + 0.6 * items_raw[partner] + 0.7 * noise_part
    return (mixture, items_raw)


def draw_queries(key, part):
    return pair_draw(key)[0].astype(jnp.bfloat16)


def draw_items(key, part):
    return pair_draw(key)[1].astype(jnp.bfloat16)


def setup_inputs(seed: int = 0) -> dict:
    seeds = jax.random.split(jax.random.key(seed), 3)
    queries = draw_queries(jax.random.fold_in(seeds[2], 71), 0)
    items = draw_items(jax.random.fold_in(seeds[2], 71), 0)
    return dict(queries=queries, items=items)


softmax_sharpness = 0.05
tiny_square = 1e-12

def unit_rows(matrix):
    widened = matrix.astype(jnp.float32)
    length = jnp.sqrt(lax.optimization_barrier(jnp.sum(widened * widened, axis=1, keepdims=True)) + tiny_square)
    return (widened / length, length)

def round_wide(values):
    return lax.optimization_barrier(values.astype(jnp.bfloat16)).astype(jnp.float32)

def direction_slope(grad, unit, length):
    along = lax.optimization_barrier(jnp.sum(unit * grad, axis=1, keepdims=True))
    return (grad - unit * along) / length

def reference(queries, items):
    question_direction, question_magnitude = unit_rows(queries)
    candidate_direction, candidate_magnitude = unit_rows(items)
    question_gathered_all = round_wide(question_direction)
    candidate_gathered_all = round_wide(candidate_direction)
    matching_score = lax.optimization_barrier(jnp.sum(question_gathered_all * candidate_gathered_all, axis=1)) / softmax_sharpness
    q_blocks = question_gathered_all.reshape(BATCH // ROWS, ROWS, D)

    def per_block(candidate_count_overall, question_portion):
        similarity_scores = jnp.dot(question_portion, candidate_gathered_all.T, precision=lax.Precision.HIGHEST) / softmax_sharpness
        new_peak = lax.optimization_barrier(jnp.max(similarity_scores, axis=1))
        log_norm = new_peak + jnp.log(lax.optimization_barrier(jnp.sum(jnp.exp(similarity_scores - new_peak[:, None]), axis=1)))
        weights = round_wide(jnp.exp(similarity_scores - log_norm[:, None]))
        question_count_overall = jnp.dot(weights, candidate_gathered_all, precision=lax.Precision.HIGHEST)
        candidate_count_overall = candidate_count_overall + jnp.dot(weights.T, question_portion, precision=lax.Precision.HIGHEST)
        return (candidate_count_overall, (log_norm, question_count_overall))
    candidate_count_overall, (log_norm, question_count_overall) = lax.scan(per_block, jnp.zeros((BATCH, D), jnp.float32), q_blocks)
    log_norm = log_norm.reshape(BATCH)
    question_count_overall = question_count_overall.reshape(BATCH, D)
    loss = jnp.mean(log_norm - matching_score)
    question_slope = direction_slope((question_count_overall - candidate_gathered_all) / softmax_sharpness, question_direction, question_magnitude)
    candidate_slope = direction_slope((candidate_count_overall - question_gathered_all) / softmax_sharpness, candidate_direction, candidate_magnitude)
    return (loss, question_slope, candidate_slope)
```

```python
import math

import jax
import jax.numpy as jnp
from jax import lax
from jax.experimental import pallas as pl
from jax.experimental.pallas import tpu as pltpu
from jax.sharding import Mesh
from jax.sharding import PartitionSpec as P

AXES = ("blk", "z", "y", "x")
RING = {(0, 0): 0, (1, 0): 1, (1, 1): 2, (0, 1): 3}
BITS = [(a, b, c) for a in (0, 1) for b in (0, 1) for c in (0, 1)]
GROUP = 8

sharpness = 0.05
tiny_square = 1e-12
log2_e = math.log2(math.e)
f32, bf16 = jnp.float32, jnp.bfloat16


def device_of(core, low, high):
    z, y, x = (RING[(l, h)] for l, h in zip(low, high))
    return ((core * 4 + z) * 4 + y) * 4 + x


LOW = [[device_of(c, low, high) for low in BITS] for c in (0, 1) for high in BITS]
HIGH = [[device_of(c, low, high) for high in BITS] for c in (0, 1) for low in BITS]


def exchange(pieces, groups):
    return lax.all_to_all(pieces, AXES, 0, 0, tiled=True, axis_index_groups=groups)


def swap_cores(value):
    return lax.ppermute(value, "blk", [(0, 1), (1, 0)])


def vmem_call(body, outs, name, flops=0, limit=24):
    spec = pl.BlockSpec(memory_space=pltpu.VMEM)
    return pl.pallas_call(
        body,
        out_shape=[jax.ShapeDtypeStruct(s, d) for s, d in outs],
        out_specs=[spec] * len(outs),
        compiler_params=pltpu.CompilerParams(vmem_limit_bytes=limit * 2**20),
        cost_estimate=pl.CostEstimate(flops=flops, bytes_accessed=0, transcendentals=0),
        name=name,
    )


def unit(matrix):
    wide = matrix.astype(f32)
    length = jnp.sqrt(jnp.sum(wide * wide, axis=1, keepdims=True) + tiny_square)
    return wide / length, length


def norm_body(q_ref, v_ref, qt_ref, vt_ref, pos_ref):
    q, v = unit(q_ref[...])[0].astype(bf16), unit(v_ref[...])[0].astype(bf16)
    for k in range(GROUP):
        qt_ref[k] = q
        vt_ref[k] = v
    total = jnp.sum(q.astype(f32) * v.astype(f32)) / sharpness
    pos_ref[...] = jnp.full((8, 128), total, f32)


def score_body(own_ref, oth_ref, q_ref, pos_ref, e_own_ref, e_oth_ref, s_ref, u_ref):
    cols = q_ref.shape[0] * q_ref.shape[1]
    q = q_ref[...].reshape(cols, q_ref.shape[2])
    total = jnp.zeros((1, cols), f32)
    pull = None
    for v_ref, e_ref in ((own_ref, e_own_ref), (oth_ref, e_oth_ref)):
        for k in range(0, GROUP, 2):
            v = v_ref[k : k + 2].reshape(256, 256)
            t = lax.dot_general(v, q, (((1,), (1,)), ((), ())), preferred_element_type=f32)
            e = jnp.exp2(t * (log2_e / sharpness))
            total = total + jnp.sum(e, axis=0, keepdims=True)
            eb = e.astype(bf16)
            e_ref[k * 128 : (k + 2) * 128] = eb
            part = lax.dot_general(v, eb, (((0,), (0,)), ((), ())), preferred_element_type=f32)
            pull = part if pull is None else pull + part
    for k in range(GROUP):
        u_ref[k] = pull[:, k * 128 : (k + 1) * 128].astype(bf16)
    for k in range(GROUP):
        for j in range(GROUP):
            s_ref[j, k : k + 1] = total[:, k * 128 : (k + 1) * 128]
    for j in range(GROUP):
        s_ref[j, 8:16] = pos_ref[...]


def row_sums(s_ref):
    total = s_ref[0]
    for j in range(1, GROUP):
        total = total + s_ref[j]
    return total


def weighted(e_ref, q_ref, r, k):
    rows = slice(k * 128, (k + 2) * 128)
    parts = [
        (e_ref[rows, j * 128 : (j + 1) * 128].astype(f32) * r[j : j + 1]).astype(bf16)
        for j in range(GROUP)
    ]
    p = jnp.concatenate(parts, axis=1)
    q = q_ref[...].reshape(q_ref.shape[0] * q_ref.shape[1], q_ref.shape[2])
    return jnp.dot(p, q, preferred_element_type=f32)


def give_body(e_ref, q_ref, s_ref, w_ref):
    sums = row_sums(s_ref)
    r = 1.0 / sums[:8]
    for k in range(0, GROUP, 2):
        w_ref[k * 128 : (k + 2) * 128] = weighted(e_ref, q_ref, r, k).astype(bf16)
    loss = jnp.sum(jnp.log(sums[:8])) - jnp.max(sums[8:9])
    high = jnp.full((8, 256), loss, f32).astype(bf16)
    low = (jnp.full((8, 256), loss, f32) - high.astype(f32)).astype(bf16)
    w_ref[1024:1040] = jnp.concatenate([high.astype(f32), low.astype(f32)], axis=0).astype(bf16)


def keep_body(e_ref, q_ref, s_ref, w_ref):
    r = 1.0 / row_sums(s_ref)[:8]
    for k in range(0, GROUP, 2):
        w_ref[k * 128 : (k + 2) * 128] = weighted(e_ref, q_ref, r, k)


def join_body(w_ref, got_ref, s_ref, out_ref):
    for k in range(GROUP):
        rows = slice(k * 128, (k + 1) * 128)
        out_ref[k, :128] = (w_ref[rows] + got_ref[rows].astype(f32)).astype(bf16)
    sums = row_sums(s_ref)
    loss = jnp.sum(jnp.log(sums[:8])) - jnp.max(sums[8:9])
    got = got_ref[1024:1040].astype(f32)
    both = got[:8] + got[8:] + loss
    high = both.astype(bf16)
    low = (both - high.astype(f32)).astype(bf16)
    tail = jnp.concatenate([high.astype(f32), low.astype(f32)], axis=0).astype(bf16)
    for k in range(GROUP):
        out_ref[k, 128:144] = tail


def slope(pull, hat, direction, length):
    grad = (pull - hat) / sharpness
    along = jnp.sum(direction * grad, axis=1, keepdims=True)
    return (grad - direction * along) / length


def final_body(high_ref, q_ref, v_ref, u_ref, w_ref, s_ref, loss_ref, qs_ref, vs_ref):
    q, q_len = unit(q_ref[...])
    v, v_len = unit(v_ref[...])
    q_hat, v_hat = q.astype(bf16).astype(f32), v.astype(bf16).astype(f32)
    ut = u_ref[0].astype(f32)
    w = w_ref[0, :128].astype(f32)
    tail = w_ref[0, 128:144].astype(f32)
    for k in range(1, GROUP):
        ut = ut + u_ref[k].astype(f32)
        w = w + w_ref[k, :128].astype(f32)
        tail = tail + w_ref[k, 128:144].astype(f32)
    sums = row_sums(s_ref)[:8]
    mine = lax.broadcasted_iota(jnp.int32, sums.shape, 0) == high_ref[0]
    own = jnp.sum(jnp.where(mine, sums, 0.0), axis=0, keepdims=True)
    u = (ut / own).T
    qs_ref[...] = slope(u, v_hat, q, q_len)
    vs_ref[...] = slope(w, q_hat, v, v_len)
    loss_ref[...] = (tail[:8] + tail[8:])[:, :128] / (128 * 128)


def high_index():
    bit = lambda a: (lax.axis_index(a) >= 2).astype(jnp.int32)
    return bit("z") * 4 + bit("y") * 2 + bit("x")


def per_device(queries, items):
    tile = (GROUP, 128, 256)
    qt, vt, pos = vmem_call(norm_body, [(tile, bf16), (tile, bf16), ((8, 128), f32)], "norm")(queries, items)
    own = exchange(vt, LOW)
    other = swap_cores(own)
    q = exchange(qt, HIGH)
    flops = 2 * 2048 * 1024 * 256
    e_own, e_oth, s, u = vmem_call(
        score_body,
        [((1024, 1024), bf16), ((1024, 1024), bf16), ((GROUP, 16, 128), f32), ((GROUP, 256, 128), bf16)],
        "score",
        2 * flops,
    )(own, other, q, pos)
    sums = exchange(s, HIGH)
    u = exchange(u, HIGH)
    (give,) = vmem_call(give_body, [((1040, 256), bf16)], "give", flops // 2)(e_oth, q, sums)
    got = swap_cores(give)
    (keep,) = vmem_call(keep_body, [((1024, 256), f32)], "keep", flops // 2)(e_own, q, sums)
    (w,) = vmem_call(join_body, [((GROUP, 144, 256), bf16)], "join")(keep, got, sums)
    w = exchange(w, LOW)
    loss, q_slope, v_slope = pl.pallas_call(
        final_body,
        in_specs=[pl.BlockSpec(memory_space=pltpu.SMEM)] + [pl.BlockSpec(memory_space=pltpu.VMEM)] * 5,
        out_specs=[pl.BlockSpec(memory_space=pltpu.VMEM)] * 3,
        out_shape=[
            jax.ShapeDtypeStruct((8, 128), f32),
            jax.ShapeDtypeStruct((128, 256), f32),
            jax.ShapeDtypeStruct((128, 256), f32),
        ],
        compiler_params=pltpu.CompilerParams(vmem_limit_bytes=24 * 2**20),
        name="final",
    )(high_index().reshape(1), queries, items, u, w, sums)
    return loss[0, 0], q_slope, v_slope


def solution(mesh):
    split = Mesh(mesh.devices.reshape(2, 4, 4, 4), AXES)
    rows = P(AXES, None)
    return jax.shard_map(
        per_device, mesh=split, in_specs=(rows, rows), out_specs=(P(), rows, rows), check_vma=False
    )
```

```python
import math

import jax
import jax.numpy as jnp
from jax import lax
from jax.experimental import pallas as pl
from jax.experimental.pallas import tpu as pltpu
from jax.sharding import Mesh
from jax.sharding import PartitionSpec as P

AXES = ("blk", "z", "y", "x")
RING = {(0, 0): 0, (1, 0): 1, (1, 1): 2, (0, 1): 3}
BITS = [(a, b, c) for a in (0, 1) for b in (0, 1) for c in (0, 1)]
GROUP = 8
ROWS, D = 128, 256

sharpness = 0.05
tiny_square = 1e-12
log2_e = math.log2(math.e)
f32, bf16 = jnp.float32, jnp.bfloat16


def device_of(core, low, high):
    z, y, x = (RING[(l, h)] for l, h in zip(low, high))
    return ((core * 4 + z) * 4 + y) * 4 + x


def low_cubes(core):
    return [[device_of(core, low, high) for low in BITS] for high in BITS]


def high_cubes(core):
    return [[device_of(core, low, high) for high in BITS] for low in BITS]


BULK = low_cubes(0) + high_cubes(1)
HIGH = high_cubes(0) + high_cubes(1)


def exchange(pieces, groups):
    return lax.all_to_all(pieces, AXES, 0, 0, tiled=True, axis_index_groups=groups)


def swap_cores(value):
    return lax.ppermute(value, "blk", [(0, 1), (1, 0)])


def call(body, outs, name, flops=0, ins=None, scratch=()):
    spec = pl.BlockSpec(memory_space=pltpu.VMEM)
    return pl.pallas_call(
        body,
        out_shape=[jax.ShapeDtypeStruct(s, d) for s, d, *_ in outs],
        out_specs=[pl.BlockSpec(memory_space=o[2]) if len(o) > 2 else spec for o in outs],
        **({"in_specs": ins} if ins else {}),
        scratch_shapes=list(scratch),
        compiler_params=pltpu.CompilerParams(vmem_limit_bytes=24 * 2**20),
        cost_estimate=pl.CostEstimate(flops=flops, bytes_accessed=0, transcendentals=0),
        name=name,
    )


def unit(matrix):
    wide = matrix.astype(f32)
    length = jnp.sqrt(jnp.sum(wide * wide, axis=1, keepdims=True) + tiny_square)
    return wide / length, length


def norm_body(q_hbm, v_hbm, mine_ref, give_ref, pos_ref, q_ref, v_ref, sem):
    copies = [
        pltpu.make_async_copy(q_hbm, q_ref, sem.at[0]),
        pltpu.make_async_copy(v_hbm, v_ref, sem.at[1]),
    ]
    for c in copies:
        c.start()
    core = lax.axis_index("blk")
    copies[0].wait()
    q = unit(q_ref[...])[0].astype(bf16)
    copies[1].wait()
    v = unit(v_ref[...])[0].astype(bf16)
    total = jnp.sum(q.astype(f32) * v.astype(f32)) / sharpness
    pos_ref[...] = jnp.full((8, 128), total, f32)

    @pl.when(core == 0)
    def _():
        mine_ref[...] = v
        give_ref[...] = q

    @pl.when(core == 1)
    def _():
        mine_ref[...] = q
        give_ref[...] = v


def tile_body(mine_ref, got_ref, out_ref):
    core = lax.axis_index("blk")
    mine, got = mine_ref[...], got_ref[...]
    for k in range(GROUP):
        out_ref[k, core] = mine
        out_ref[k, 1 - core] = got


def score_body(mine_ref, got_ref, pos_ref, e_ref, q_ref, s_ref, u_ref, v_ref):
    core = lax.axis_index("blk")

    @pl.when(core == 0)
    def _():
        v_ref[...] = mine_ref[...]
        q_ref[...] = got_ref[:, 0]

    @pl.when(core == 1)
    def _():
        v_ref[...] = got_ref[...]
        q_ref[...] = mine_ref[:, 1]

    cols = GROUP * ROWS
    q = q_ref[...].reshape(cols, D)
    total = jnp.zeros((1, cols), f32)
    pull = None
    for k in range(GROUP):
        v = v_ref[k].reshape(2 * ROWS, D)
        t = lax.dot_general(v, q, (((1,), (1,)), ((), ())), preferred_element_type=f32)
        e = jnp.exp2(t * (log2_e / sharpness))
        total = total + jnp.sum(e, axis=0, keepdims=True)
        eb = e.astype(bf16)
        e_ref[k] = eb
        part = lax.dot_general(v, eb, (((0,), (0,)), ((), ())), preferred_element_type=f32)
        pull = part if pull is None else pull + part
    for k in range(GROUP):
        cut = slice(k * ROWS, (k + 1) * ROWS)
        u_ref[k, :, :ROWS] = pull[:ROWS, cut].astype(bf16)
        u_ref[k, :, ROWS:] = pull[ROWS:, cut].astype(bf16)
        for j in range(GROUP):
            s_ref[j, k : k + 1] = total[:, cut]
    for j in range(GROUP):
        s_ref[j, 8:16] = pos_ref[...]


def row_sums(s_ref):
    total = s_ref[0]
    for j in range(1, GROUP):
        total = total + s_ref[j]
    return total


def split(value):
    high = value.astype(bf16)
    low = (value - high.astype(f32)).astype(bf16)
    return jnp.concatenate([high.astype(f32), low.astype(f32)], axis=0).astype(bf16)


def weigh_body(e_ref, q_ref, s_ref, keep_ref, give_ref):
    sums = row_sums(s_ref)
    r = 1.0 / sums[:8]
    q = q_ref[...].reshape(GROUP * ROWS, D)
    for k in range(GROUP):
        parts = [
            (e_ref[k, :, j * ROWS : (j + 1) * ROWS].astype(f32) * r[j : j + 1]).astype(bf16)
            for j in range(GROUP)
        ]
        w = jnp.dot(jnp.concatenate(parts, axis=1), q, preferred_element_type=f32)
        keep_ref[k] = w
        give_ref[k * 256 : (k + 1) * 256] = w.astype(bf16)
    loss = jnp.sum(jnp.log(sums[:8])) - jnp.max(sums[8:9])
    give_ref[2048:2064] = split(jnp.full((8, D), loss, f32))


def join_body(keep_ref, got_ref, u_ref, got_u_ref, s_ref, out_ref):
    core = lax.axis_index("blk")

    @pl.when(core == 0)
    def _():
        for k in range(GROUP):
            out_ref[k, :256] = (keep_ref[k] + got_ref[k * 256 : (k + 1) * 256].astype(f32)).astype(bf16)

    @pl.when(core == 1)
    def _():
        for k in range(GROUP):
            out_ref[k, :128] = got_u_ref[k]
            out_ref[k, 128:256] = u_ref[k]

    sums = row_sums(s_ref)
    loss = jnp.sum(jnp.log(sums[:8])) - jnp.max(sums[8:9])
    got = got_ref[2048:2064].astype(f32)
    tail = split(got[:8] + got[8:] + loss)
    for k in range(GROUP):
        out_ref[k, 256:272] = tail


def sum_body(w_ref, keep_ref, give_ref):
    core = lax.axis_index("blk")

    def summed(first, rows):
        at = pl.ds(first, rows)
        total = w_ref[0, at].astype(f32)
        for k in range(1, GROUP):
            total = total + w_ref[k, at].astype(f32)
        return total

    tail = summed(256, 16)
    tail = tail[:8] + tail[8:]
    keep_ref[:128] = summed(pl.multiple_of(core * 128, 128), 128)
    give_ref[:128] = summed(pl.multiple_of((1 - core) * 128, 128), 128)
    keep_ref[128:136] = tail
    give_ref[128:136] = tail


def slope(pull, hat, direction, length):
    grad = (pull - hat) / sharpness
    along = jnp.sum(direction * grad, axis=1, keepdims=True)
    return (grad - direction * along) / length


def high_index():
    bit = lambda a: (lax.axis_index(a) >= 2).astype(jnp.int32)
    return bit("z") * 4 + bit("y") * 2 + bit("x")


def final_body(q_ref, v_ref, keep_ref, got_ref, s_ref, qs_ref, vs_ref, loss_ref):
    first = lax.axis_index("blk") == 0
    q, q_len = unit(q_ref[...])
    v, v_len = unit(v_ref[...])
    q_hat, v_hat = q.astype(bf16).astype(f32), v.astype(bf16).astype(f32)
    keep, got = keep_ref[...], got_ref[...]
    w = jnp.where(first, keep, got)
    u = jnp.where(first, got, keep)
    sums = row_sums(s_ref)[:8]
    mine = lax.broadcasted_iota(jnp.int32, sums.shape, 0) == high_index()
    own = jnp.sum(jnp.where(mine, sums, 0.0), axis=0, keepdims=True)
    u = jnp.concatenate([(u[:128, :128] / own).T, (u[:128, 128:] / own).T], axis=1)
    qs_ref[...] = slope(u, v_hat, q, q_len)
    vs_ref[...] = slope(w[:128], q_hat, v, v_len)
    loss_ref[0, 0] = jnp.max(w[128:136]) / (128 * 128)


def per_device(queries, items):
    anyspace = pl.BlockSpec(memory_space=pl.ANY)
    rows = (ROWS, D)
    mine, give, pos = call(
        norm_body,
        [(rows, bf16), (rows, bf16), ((8, 128), f32)],
        "norm",
        ins=[anyspace] * 2,
        scratch=[pltpu.VMEM(rows, bf16), pltpu.VMEM(rows, bf16), pltpu.SemaphoreType.DMA((2,))],
    )(queries, items)
    bulk = (GROUP, 2, ROWS, D)
    (tile,) = call(tile_body, [(bulk, bf16)], "tile")(mine, swap_cores(give))
    block = exchange(tile, BULK)
    flops = 2 * 2048 * 1024 * 256
    e, q, s, u = call(
        score_body,
        [
            ((GROUP, 256, 1024), bf16),
            ((GROUP, ROWS, D), bf16),
            ((GROUP, 16, 128), f32),
            ((GROUP, ROWS, D), bf16),
        ],
        "score",
        2 * flops,
        scratch=[pltpu.VMEM(bulk, bf16)],
    )(block, swap_cores(block), pos)
    got_u = swap_cores(u)
    sums = exchange(s, HIGH)
    keep, give = call(
        weigh_body, [((GROUP, 256, D), f32), ((2064, D), bf16)], "weigh", flops
    )(e, q, sums)
    (out,) = call(join_body, [((GROUP, 272, D), bf16)], "join")(keep, swap_cores(give), u, got_u, sums)
    out = exchange(out, BULK)
    keep, give = call(sum_body, [((136, D), f32), ((136, D), f32)], "sum")(out)
    q_slope, v_slope, loss = call(
        final_body, [(rows, f32), (rows, f32), ((1, 1), f32, pltpu.SMEM)], "final"
    )(queries, items, keep, swap_cores(give), sums)
    return loss.reshape(()), q_slope, v_slope


def solution(mesh):
    split = Mesh(mesh.devices.reshape(2, 4, 4, 4), AXES)
    rows = P(AXES, None)
    return jax.shard_map(
        per_device, mesh=split, in_specs=(rows, rows), out_specs=(P(), rows, rows), check_vma=False
    )
```

```python
import functools
import math

import jax
import jax.numpy as jnp
from jax import lax
from jax.experimental import pallas as pl
from jax.experimental.pallas import tpu as pltpu
from jax.sharding import Mesh
from jax.sharding import PartitionSpec as P

AXES = ("blk", "z", "y", "x")
RING = {(0, 0): 0, (1, 0): 1, (1, 1): 2, (0, 1): 3}
BITS = [(a, b, c) for a in (0, 1) for b in (0, 1) for c in (0, 1)]
GROUP = 8
ROWS, D = 128, 256

sharpness = 0.05
tiny_square = 1e-12
log2_e = math.log2(math.e)
f32, bf16 = jnp.float32, jnp.bfloat16


def device_of(core, low, high):
    z, y, x = (RING[(l, h)] for l, h in zip(low, high))
    return ((core * 4 + z) * 4 + y) * 4 + x


def low_cubes(core):
    return [[device_of(core, low, high) for low in BITS] for high in BITS]


def high_cubes(core):
    return [[device_of(core, low, high) for high in BITS] for low in BITS]


BULK = low_cubes(0) + high_cubes(1)
HIGH = high_cubes(0) + high_cubes(1)


def exchange(pieces, groups):
    return lax.all_to_all(pieces, AXES, 0, 0, tiled=True, axis_index_groups=groups)


def swap_cores(value):
    return lax.ppermute(value, "blk", [(0, 1), (1, 0)])


def call(body, outs, name, flops=0, ins=None, scratch=()):
    spec = pl.BlockSpec(memory_space=pltpu.VMEM)
    return pl.pallas_call(
        body,
        out_shape=[jax.ShapeDtypeStruct(s, d) for s, d, *_ in outs],
        out_specs=[pl.BlockSpec(memory_space=o[2]) if len(o) > 2 else spec for o in outs],
        **({"in_specs": ins} if ins else {}),
        scratch_shapes=list(scratch),
        compiler_params=pltpu.CompilerParams(vmem_limit_bytes=24 * 2**20),
        cost_estimate=pl.CostEstimate(flops=flops, bytes_accessed=0, transcendentals=0),
        name=name,
    )


def unit(matrix):
    wide = matrix.astype(f32)
    length = jnp.sqrt(jnp.sum(wide * wide, axis=1, keepdims=True) + tiny_square)
    return wide / length, length


def norm_body(q_hbm, v_hbm, mine_ref, give_ref, pos_ref, q_ref, v_ref, sem):
    copies = [
        pltpu.make_async_copy(q_hbm, q_ref, sem.at[0]),
        pltpu.make_async_copy(v_hbm, v_ref, sem.at[1]),
    ]
    for c in copies:
        c.start()
    core = lax.axis_index("blk")
    copies[0].wait()
    q = unit(q_ref[...])[0].astype(bf16)
    copies[1].wait()
    v = unit(v_ref[...])[0].astype(bf16)
    total = jnp.sum(q.astype(f32) * v.astype(f32)) / sharpness
    pos_ref[...] = jnp.full((8, 128), total, f32)

    @pl.when(core == 0)
    def _():
        mine_ref[...] = v
        give_ref[...] = q

    @pl.when(core == 1)
    def _():
        mine_ref[...] = q
        give_ref[...] = v


def tile_body(mine_ref, got_ref, out_ref):
    core = lax.axis_index("blk")
    mine, got = mine_ref[...], got_ref[...]
    for k in range(GROUP):
        out_ref[k, core] = mine
        out_ref[k, 1 - core] = got


def score_body(mine_ref, got_ref, pos_ref, e_ref, q_ref, s_ref, u_ref, v_ref):
    core = lax.axis_index("blk")

    @pl.when(core == 0)
    def _():
        v_ref[...] = mine_ref[...]
        q_ref[...] = got_ref[:, 0]

    @pl.when(core == 1)
    def _():
        v_ref[...] = got_ref[...]
        q_ref[...] = mine_ref[:, 1]

    cols = GROUP * ROWS
    q = q_ref[...].reshape(cols, D)
    total = jnp.zeros((1, cols), f32)
    pull = None
    for k in range(GROUP):
        v = v_ref[k].reshape(2 * ROWS, D)
        t = lax.dot_general(v, q, (((1,), (1,)), ((), ())), preferred_element_type=f32)
        e = jnp.exp2(t * (log2_e / sharpness))
        total = total + jnp.sum(e, axis=0, keepdims=True)
        eb = e.astype(bf16)
        e_ref[k] = eb
        part = lax.dot_general(v, eb, (((0,), (0,)), ((), ())), preferred_element_type=f32)
        pull = part if pull is None else pull + part
    for k in range(GROUP):
        cut = slice(k * ROWS, (k + 1) * ROWS)
        rows = slice(k * ROWS, (k + 1) * ROWS)
        u_ref[rows, :ROWS] = pull[:ROWS, cut].astype(bf16)
        u_ref[rows, ROWS:] = pull[ROWS:, cut].astype(bf16)
        for j in range(GROUP):
            s_ref[j, k : k + 1] = total[:, cut]
    for j in range(GROUP):
        s_ref[j, 8:16] = pos_ref[...]


def row_sums(s_ref):
    total = s_ref[0]
    for j in range(1, GROUP):
        total = total + s_ref[j]
    return total


def split(value):
    high = value.astype(bf16)
    low = (value - high.astype(f32)).astype(bf16)
    return jnp.concatenate([high.astype(f32), low.astype(f32)], axis=0).astype(bf16)


def loss_part(sums):
    return jnp.sum(jnp.log(sums[:8])) - jnp.max(sums[8:9])


def weigh_body(first, *refs):
    *u_ref, e_ref, q_ref, s_ref, keep_ref, give_ref = refs
    core = lax.axis_index("blk")
    sums = row_sums(s_ref)
    r = 1.0 / sums[:8]
    q = q_ref[...].reshape(GROUP * ROWS, D)
    for k in range(GROUP // 2):
        parts = [
            (e_ref[first + k, :, j * ROWS : (j + 1) * ROWS].astype(f32) * r[j : j + 1]).astype(bf16)
            for j in range(GROUP)
        ]
        w = jnp.dot(jnp.concatenate(parts, axis=1), q, preferred_element_type=f32)
        keep_ref[k] = w
        give_ref[k * 256 : (k + 1) * 256] = w.astype(bf16)
    if u_ref:
        give_ref[1024:1040] = split(jnp.full((8, D), loss_part(sums), f32))

        @pl.when(core == 0)
        def _():
            give_ref[:1024] = u_ref[0][...]


def join_body(keep0_ref, keep1_ref, got0_ref, got1_ref, u_ref, s_ref, out_ref):
    core = lax.axis_index("blk")

    @pl.when(core == 0)
    def _():
        for k in range(GROUP):
            keep, got = (keep0_ref, got0_ref) if k < 4 else (keep1_ref, got1_ref)
            i = k % 4
            out_ref[k, :256] = (keep[i] + got[i * 256 : (i + 1) * 256].astype(f32)).astype(bf16)

    @pl.when(core == 1)
    def _():
        for k in range(GROUP):
            rows = slice(k * ROWS, (k + 1) * ROWS)
            out_ref[k, :128] = got0_ref[rows]
            out_ref[k, 128:256] = u_ref[rows]

    got = got0_ref[1024:1040].astype(f32)
    tail = split(got[:8] + got[8:] + loss_part(row_sums(s_ref)))
    for k in range(GROUP):
        out_ref[k, 256:272] = tail


def sum_body(w_ref, keep_ref, give_ref):
    core = lax.axis_index("blk")

    def summed(first, rows):
        at = pl.ds(first, rows)
        total = w_ref[0, at].astype(f32)
        for k in range(1, GROUP):
            total = total + w_ref[k, at].astype(f32)
        return total

    tail = summed(256, 16)
    tail = tail[:8] + tail[8:]
    keep_ref[:128] = summed(pl.multiple_of(core * 128, 128), 128)
    give_ref[:128] = summed(pl.multiple_of((1 - core) * 128, 128), 128)
    keep_ref[128:136] = tail
    give_ref[128:136] = tail


def slope(pull, hat, direction, length):
    grad = (pull - hat) / sharpness
    along = jnp.sum(direction * grad, axis=1, keepdims=True)
    return (grad - direction * along) / length


def high_index():
    bit = lambda a: (lax.axis_index(a) >= 2).astype(jnp.int32)
    return bit("z") * 4 + bit("y") * 2 + bit("x")


def final_body(q_ref, v_ref, keep_ref, got_ref, s_ref, qs_ref, vs_ref, loss_ref):
    first = lax.axis_index("blk") == 0
    q, q_len = unit(q_ref[...])
    v, v_len = unit(v_ref[...])
    q_hat, v_hat = q.astype(bf16).astype(f32), v.astype(bf16).astype(f32)
    keep, got = keep_ref[...], got_ref[...]
    w = jnp.where(first, keep, got)
    u = jnp.where(first, got, keep)
    sums = row_sums(s_ref)[:8]
    mine = lax.broadcasted_iota(jnp.int32, sums.shape, 0) == high_index()
    own = jnp.sum(jnp.where(mine, sums, 0.0), axis=0, keepdims=True)
    u = jnp.concatenate([(u[:128, :128] / own).T, (u[:128, 128:] / own).T], axis=1)
    qs_ref[...] = slope(u, v_hat, q, q_len)
    vs_ref[...] = slope(w[:128], q_hat, v, v_len)
    loss_ref[0, 0] = jnp.max(w[128:136]) / (128 * 128)


def per_device(queries, items):
    anyspace = pl.BlockSpec(memory_space=pltpu.HBM)
    rows = (ROWS, D)
    mine, give, pos = call(
        norm_body,
        [(rows, bf16), (rows, bf16), ((8, 128), f32)],
        "norm",
        ins=[anyspace] * 2,
        scratch=[pltpu.VMEM(rows, bf16), pltpu.VMEM(rows, bf16), pltpu.SemaphoreType.DMA((2,))],
    )(*(pltpu.with_memory_space_constraint(a, pltpu.HBM) for a in (queries, items)))
    bulk = (GROUP, 2, ROWS, D)
    (tile,) = call(tile_body, [(bulk, bf16)], "tile")(mine, swap_cores(give))
    block = exchange(tile, BULK)
    flops = 2 * 2048 * 1024 * 256
    e, q, s, u = call(
        score_body,
        [
            ((GROUP, 256, 1024), bf16),
            ((GROUP, ROWS, D), bf16),
            ((GROUP, 16, 128), f32),
            ((GROUP * ROWS, D), bf16),
        ],
        "score",
        2 * flops,
        scratch=[pltpu.VMEM(bulk, bf16)],
    )(block, swap_cores(block), pos)
    sums = exchange(s, HIGH)
    keep, got = [], []
    for half in (0, 1):
        k, g = call(
            functools.partial(weigh_body, half * 4),
            [((4, 256, D), f32), ((1040 - 16 * half, D), bf16)],
            f"weigh{half}",
            flops // 2,
        )(*([u] if half == 0 else []), e, q, sums)
        keep.append(k)
        got.append(swap_cores(g))
    (out,) = call(join_body, [((GROUP, 272, D), bf16)], "join")(*keep, *got, u, sums)
    out = exchange(out, BULK)
    keep, give = call(sum_body, [((136, D), f32), ((136, D), f32)], "sum")(out)
    q_slope, v_slope, loss = call(
        final_body, [(rows, f32), (rows, f32), ((1, 1), f32, pltpu.SMEM)], "final"
    )(queries, items, keep, swap_cores(give), sums)
    return loss.reshape(()), q_slope, v_slope


def solution(mesh):
    split = Mesh(mesh.devices.reshape(2, 4, 4, 4), AXES)
    rows = P(AXES, None)
    return jax.shard_map(
        per_device, mesh=split, in_specs=(rows, rows), out_specs=(P(), rows, rows), check_vma=False
    )
```

```python
import functools
import math

import jax
import jax.numpy as jnp
from jax import lax
from jax.experimental import pallas as pl
from jax.experimental.pallas import tpu as pltpu
from jax.sharding import Mesh
from jax.sharding import PartitionSpec as P

AXES = ("blk", "z", "y", "x")
RING = {(0, 0): 0, (1, 0): 1, (1, 1): 2, (0, 1): 3}
BITS = [(a, b, c) for a in (0, 1) for b in (0, 1) for c in (0, 1)]
GROUP = 8
ROWS, D = 128, 256

sharpness = 0.05
tiny_square = 1e-12
log2_e = math.log2(math.e)
f32, bf16 = jnp.float32, jnp.bfloat16


def device_of(core, low, high):
    z, y, x = (RING[(l, h)] for l, h in zip(low, high))
    return ((core * 4 + z) * 4 + y) * 4 + x


def low_cubes(core):
    return [[device_of(core, low, high) for low in BITS] for high in BITS]


def high_cubes(core):
    return [[device_of(core, low, high) for high in BITS] for low in BITS]


BULK = high_cubes(0) + low_cubes(1)
LOW = low_cubes(0) + low_cubes(1)


def exchange(pieces, groups):
    return lax.all_to_all(pieces, AXES, 0, 0, tiled=True, axis_index_groups=groups)


def swap_cores(value):
    return lax.ppermute(value, "blk", [(0, 1), (1, 0)])


def call(body, outs, name, flops=0, ins=None, scratch=()):
    spec = pl.BlockSpec(memory_space=pltpu.VMEM)
    return pl.pallas_call(
        body,
        out_shape=[jax.ShapeDtypeStruct(s, d) for s, d, *_ in outs],
        out_specs=[pl.BlockSpec(memory_space=o[2]) if len(o) > 2 else spec for o in outs],
        **({"in_specs": ins} if ins else {}),
        scratch_shapes=list(scratch),
        compiler_params=pltpu.CompilerParams(vmem_limit_bytes=24 * 2**20),
        cost_estimate=pl.CostEstimate(flops=flops, bytes_accessed=0, transcendentals=0),
        name=name,
    )


def unit(matrix):
    wide = matrix.astype(f32)
    length = jnp.sqrt(jnp.sum(wide * wide, axis=1, keepdims=True) + tiny_square)
    return wide / length, length


def norm_body(q_hbm, v_hbm, mine_ref, give_ref, pos_ref, q_ref, v_ref, sem):
    copies = [
        pltpu.make_async_copy(q_hbm, q_ref, sem.at[0]),
        pltpu.make_async_copy(v_hbm, v_ref, sem.at[1]),
    ]
    for c in copies:
        c.start()
    core = lax.axis_index("blk")
    copies[0].wait()
    q = unit(q_ref[...])[0].astype(bf16)
    copies[1].wait()
    v = unit(v_ref[...])[0].astype(bf16)
    total = jnp.sum(q.astype(f32) * v.astype(f32)) / sharpness
    pos_ref[...] = jnp.full((8, 128), total, f32)

    @pl.when(core == 0)
    def _():
        mine_ref[...] = v
        give_ref[...] = q

    @pl.when(core == 1)
    def _():
        mine_ref[...] = q
        give_ref[...] = v


def tile_body(mine_ref, got_ref, out_ref):
    core = lax.axis_index("blk")
    mine, got = mine_ref[...], got_ref[...]
    for k in range(GROUP):
        out_ref[k, core] = mine
        out_ref[k, 1 - core] = got


def score_body(mine_ref, got_ref, pos_ref, e_ref, q_ref, s_ref, u_ref, v_ref):
    core = lax.axis_index("blk")

    @pl.when(core == 0)
    def _():
        v_ref[...] = mine_ref[...]
        q_ref[...] = got_ref[:, 0]

    @pl.when(core == 1)
    def _():
        v_ref[...] = got_ref[...]
        q_ref[...] = mine_ref[:, 1]

    cols = GROUP * ROWS
    q = q_ref[...].reshape(cols, D)
    total = jnp.zeros((1, cols), f32)
    pull = None
    for k in range(GROUP):
        v = v_ref[k].reshape(2 * ROWS, D)
        t = lax.dot_general(v, q, (((1,), (1,)), ((), ())), preferred_element_type=f32)
        e = jnp.exp2(t * (log2_e / sharpness))
        total = total + jnp.sum(e, axis=0, keepdims=True)
        eb = e.astype(bf16)
        e_ref[k] = eb
        part = lax.dot_general(v, eb, (((0,), (0,)), ((), ())), preferred_element_type=f32)
        pull = part if pull is None else pull + part
    for k in range(GROUP):
        cut = slice(k * ROWS, (k + 1) * ROWS)
        rows = slice(k * ROWS, (k + 1) * ROWS)
        u_ref[rows, :ROWS] = pull[:ROWS, cut].astype(bf16)
        u_ref[rows, ROWS:] = pull[ROWS:, cut].astype(bf16)
        for j in range(GROUP):
            s_ref[j, k : k + 1] = total[:, cut]
    for j in range(GROUP):
        s_ref[j, 8:16] = pos_ref[...]


def row_sums(s_ref):
    total = s_ref[0]
    for j in range(1, GROUP):
        total = total + s_ref[j]
    return total


def split(value):
    high = value.astype(bf16)
    low = (value - high.astype(f32)).astype(bf16)
    return jnp.concatenate([high.astype(f32), low.astype(f32)], axis=0).astype(bf16)


def loss_part(sums):
    return jnp.sum(jnp.log(sums[:8])) - jnp.max(sums[8:9])


def weigh_body(first, *refs):
    *u_ref, e_ref, q_ref, s_ref, keep_ref, give_ref = refs
    core = lax.axis_index("blk")
    sums = row_sums(s_ref)
    r = 1.0 / sums[:8]
    q = q_ref[...].reshape(GROUP * ROWS, D)
    for k in range(GROUP // 2):
        parts = [
            (e_ref[first + k, :, j * ROWS : (j + 1) * ROWS].astype(f32) * r[j : j + 1]).astype(bf16)
            for j in range(GROUP)
        ]
        w = jnp.dot(jnp.concatenate(parts, axis=1), q, preferred_element_type=f32)
        keep_ref[k] = w
        give_ref[k * 256 : (k + 1) * 256] = w.astype(bf16)
    if u_ref:
        give_ref[1024:1040] = split(jnp.full((8, D), loss_part(sums), f32))

        @pl.when(core == 0)
        def _():
            give_ref[:1024] = u_ref[0][...]


def join_body(keep0_ref, keep1_ref, got0_ref, got1_ref, u_ref, s_ref, out_ref):
    core = lax.axis_index("blk")

    @pl.when(core == 0)
    def _():
        for k in range(GROUP):
            keep, got = (keep0_ref, got0_ref) if k < 4 else (keep1_ref, got1_ref)
            i = k % 4
            out_ref[k, :256] = (keep[i] + got[i * 256 : (i + 1) * 256].astype(f32)).astype(bf16)

    @pl.when(core == 1)
    def _():
        for k in range(GROUP):
            rows = slice(k * ROWS, (k + 1) * ROWS)
            out_ref[k, :128] = got0_ref[rows]
            out_ref[k, 128:256] = u_ref[rows]

    got = got0_ref[1024:1040].astype(f32)
    tail = split(got[:8] + got[8:] + loss_part(row_sums(s_ref)))
    for k in range(GROUP):
        out_ref[k, 256:272] = tail


def sum_body(w_ref, keep_ref, give_ref):
    core = lax.axis_index("blk")

    def summed(first, rows):
        at = pl.ds(first, rows)
        total = w_ref[0, at].astype(f32)
        for k in range(1, GROUP):
            total = total + w_ref[k, at].astype(f32)
        return total

    tail = summed(256, 16)
    tail = tail[:8] + tail[8:]
    keep_ref[:128] = summed(pl.multiple_of(core * 128, 128), 128)
    give_ref[:128] = summed(pl.multiple_of((1 - core) * 128, 128), 128)
    keep_ref[128:136] = tail
    give_ref[128:136] = tail


def slope(pull, hat, direction, length):
    grad = (pull - hat) / sharpness
    along = jnp.sum(direction * grad, axis=1, keepdims=True)
    return (grad - direction * along) / length


def low_index():
    at = [lax.axis_index(a) for a in "zyx"]
    z, y, x = (((a == 1) | (a == 2)).astype(jnp.int32) for a in at)
    return z * 4 + y * 2 + x


def final_body(q_ref, v_ref, keep_ref, got_ref, s_ref, qs_ref, vs_ref, loss_ref):
    first = lax.axis_index("blk") == 0
    q, q_len = unit(q_ref[...])
    v, v_len = unit(v_ref[...])
    q_hat, v_hat = q.astype(bf16).astype(f32), v.astype(bf16).astype(f32)
    keep, got = keep_ref[...], got_ref[...]
    w = jnp.where(first, keep, got)
    u = jnp.where(first, got, keep)
    sums = row_sums(s_ref)[:8]
    mine = lax.broadcasted_iota(jnp.int32, sums.shape, 0) == low_index()
    own = jnp.sum(jnp.where(mine, sums, 0.0), axis=0, keepdims=True)
    u = jnp.concatenate([(u[:128, :128] / own).T, (u[:128, 128:] / own).T], axis=1)
    qs_ref[...] = slope(u, v_hat, q, q_len)
    vs_ref[...] = slope(w[:128], q_hat, v, v_len)
    loss_ref[0, 0] = jnp.max(w[128:136]) / (128 * 128)


def per_device(queries, items):
    anyspace = pl.BlockSpec(memory_space=pltpu.HBM)
    rows = (ROWS, D)
    mine, give, pos = call(
        norm_body,
        [(rows, bf16), (rows, bf16), ((8, 128), f32)],
        "norm",
        ins=[anyspace] * 2,
        scratch=[pltpu.VMEM(rows, bf16), pltpu.VMEM(rows, bf16), pltpu.SemaphoreType.DMA((2,))],
    )(*(pltpu.with_memory_space_constraint(a, pltpu.HBM) for a in (queries, items)))
    bulk = (GROUP, 2, ROWS, D)
    (tile,) = call(tile_body, [(bulk, bf16)], "tile")(mine, swap_cores(give))
    block = exchange(tile, BULK)
    flops = 2 * 2048 * 1024 * 256
    e, q, s, u = call(
        score_body,
        [
            ((GROUP, 256, 1024), bf16),
            ((GROUP, ROWS, D), bf16),
            ((GROUP, 16, 128), f32),
            ((GROUP * ROWS, D), bf16),
        ],
        "score",
        2 * flops,
        scratch=[pltpu.VMEM(bulk, bf16)],
    )(block, swap_cores(block), pos)
    sums = exchange(s, LOW)
    keep, got = [], []
    for half in (0, 1):
        k, g = call(
            functools.partial(weigh_body, half * 4),
            [((4, 256, D), f32), ((1040 - 16 * half, D), bf16)],
            f"weigh{half}",
            flops // 2,
        )(*([u] if half == 0 else []), e, q, sums)
        keep.append(k)
        got.append(swap_cores(g))
    (out,) = call(join_body, [((GROUP, 272, D), bf16)], "join")(*keep, *got, u, sums)
    out = exchange(out, BULK)
    keep, give = call(sum_body, [((136, D), f32), ((136, D), f32)], "sum")(out)
    q_slope, v_slope, loss = call(
        final_body, [(rows, f32), (rows, f32), ((1, 1), f32, pltpu.SMEM)], "final"
    )(queries, items, keep, swap_cores(give), sums)
    return loss.reshape(()), q_slope, v_slope


def solution(mesh):
    split = Mesh(mesh.devices.reshape(2, 4, 4, 4), AXES)
    rows = P(AXES, None)
    return jax.shard_map(
        per_device, mesh=split, in_specs=(rows, rows), out_specs=(P(), rows, rows), check_vma=False
    )
```

```python
import functools
import math

import jax
import jax.numpy as jnp
from jax import lax
from jax.experimental import pallas as pl
from jax.experimental.pallas import tpu as pltpu
from jax.sharding import Mesh
from jax.sharding import PartitionSpec as P

AXES = ("blk", "z", "y", "x")
GROUP = 8
ROWS, D = 128, 256
ITEM = 1

sharpness = 0.05
tiny_square = 1e-12
log2_e = math.log2(math.e)
f32, bf16 = jnp.float32, jnp.bfloat16


def device_of(core, z, y, x):
    return ((core * 4 + z) * 4 + y) * 4 + x


def query_groups(core):
    return [[device_of(core, z, y, x) for y in pair for x in range(4)] for z in range(4) for pair in ((0, 1), (2, 3))]


def item_groups(core):
    return [[device_of(core, z, y, x) for y in pair for z in range(4)] for x in range(4) for pair in ((1, 2), (3, 0))]


def query_index():
    return lax.axis_index("y") % 2 * 4 + lax.axis_index("x")


BULK = item_groups(ITEM) + query_groups(1 - ITEM)
QUERY = query_groups(0) + query_groups(1)


def exchange(pieces, groups):
    return lax.all_to_all(pieces, AXES, 0, 0, tiled=True, axis_index_groups=groups)


def swap_cores(value):
    return lax.ppermute(value, "blk", [(0, 1), (1, 0)])


def call(body, outs, name, flops=0, ins=None, scratch=()):
    spec = pl.BlockSpec(memory_space=pltpu.VMEM)
    return pl.pallas_call(
        body,
        out_shape=[jax.ShapeDtypeStruct(s, d) for s, d, *_ in outs],
        out_specs=[pl.BlockSpec(memory_space=o[2]) if len(o) > 2 else spec for o in outs],
        **({"in_specs": ins} if ins else {}),
        scratch_shapes=list(scratch),
        compiler_params=pltpu.CompilerParams(vmem_limit_bytes=24 * 2**20),
        cost_estimate=pl.CostEstimate(flops=flops, bytes_accessed=0, transcendentals=0),
        name=name,
    )


def unit(matrix):
    wide = matrix.astype(f32)
    length = jnp.sqrt(jnp.sum(wide * wide, axis=1, keepdims=True) + tiny_square)
    return wide / length, length


def norm_body(q_hbm, v_hbm, mine_ref, give_ref, pos_ref, q_ref, v_ref, sem):
    copies = [
        pltpu.make_async_copy(q_hbm, q_ref, sem.at[0]),
        pltpu.make_async_copy(v_hbm, v_ref, sem.at[1]),
    ]
    for c in copies:
        c.start()
    core = lax.axis_index("blk")
    copies[0].wait()
    q = unit(q_ref[...])[0].astype(bf16)
    copies[1].wait()
    v = unit(v_ref[...])[0].astype(bf16)
    total = jnp.sum(q.astype(f32) * v.astype(f32)) / sharpness
    pos_ref[...] = jnp.full((8, 128), total, f32)

    @pl.when(core == ITEM)
    def _():
        mine_ref[...] = v
        give_ref[...] = q

    @pl.when(core != ITEM)
    def _():
        mine_ref[...] = q
        give_ref[...] = v


def tile_body(mine_ref, got_ref, out_ref):
    core = lax.axis_index("blk")
    mine, got = mine_ref[...], got_ref[...]
    for k in range(GROUP):
        out_ref[k, core] = mine
        out_ref[k, 1 - core] = got


def score_body(mine_ref, got_ref, pos_ref, e_ref, q_ref, s_ref, u_ref, v_ref):
    core = lax.axis_index("blk")

    @pl.when(core == ITEM)
    def _():
        v_ref[...] = mine_ref[...]
        q_ref[...] = got_ref[:, ITEM]

    @pl.when(core != ITEM)
    def _():
        v_ref[...] = got_ref[...]
        q_ref[...] = mine_ref[:, 1 - ITEM]

    cols = GROUP * ROWS
    q = q_ref[...].reshape(cols, D)
    total = jnp.zeros((1, cols), f32)
    pull = None
    for k in range(GROUP):
        v = v_ref[k].reshape(2 * ROWS, D)
        t = lax.dot_general(v, q, (((1,), (1,)), ((), ())), preferred_element_type=f32)
        e = jnp.exp2(t * (log2_e / sharpness))
        total = total + jnp.sum(e, axis=0, keepdims=True)
        eb = e.astype(bf16)
        e_ref[k] = eb
        part = lax.dot_general(v, eb, (((0,), (0,)), ((), ())), preferred_element_type=f32)
        pull = part if pull is None else pull + part
    for k in range(GROUP):
        cut = slice(k * ROWS, (k + 1) * ROWS)
        rows = slice(k * ROWS, (k + 1) * ROWS)
        u_ref[rows, :ROWS] = pull[:ROWS, cut].astype(bf16)
        u_ref[rows, ROWS:] = pull[ROWS:, cut].astype(bf16)
        for j in range(GROUP):
            s_ref[j, k : k + 1] = total[:, cut]
    for j in range(GROUP):
        s_ref[j, 8:16] = pos_ref[...]


def row_sums(s_ref):
    total = s_ref[0]
    for j in range(1, GROUP):
        total = total + s_ref[j]
    return total


def split(value):
    high = value.astype(bf16)
    low = (value - high.astype(f32)).astype(bf16)
    return jnp.concatenate([high.astype(f32), low.astype(f32)], axis=0).astype(bf16)


def loss_part(sums):
    return jnp.sum(jnp.log(sums[:8])) - jnp.max(sums[8:9])


def weigh_body(first, *refs):
    *u_ref, e_ref, q_ref, s_ref, keep_ref, give_ref = refs
    core = lax.axis_index("blk")
    sums = row_sums(s_ref)
    r = 1.0 / sums[:8]
    q = q_ref[...].reshape(GROUP * ROWS, D)
    for k in range(GROUP // 2):
        parts = [
            (e_ref[first + k, :, j * ROWS : (j + 1) * ROWS].astype(f32) * r[j : j + 1]).astype(bf16)
            for j in range(GROUP)
        ]
        w = jnp.dot(jnp.concatenate(parts, axis=1), q, preferred_element_type=f32)
        keep_ref[k] = w
        give_ref[k * 256 : (k + 1) * 256] = w.astype(bf16)
    if u_ref:
        give_ref[1024:1040] = split(jnp.full((8, D), loss_part(sums), f32))

        @pl.when(core == ITEM)
        def _():
            give_ref[:1024] = u_ref[0][...]


def join_body(keep0_ref, keep1_ref, got0_ref, got1_ref, u_ref, s_ref, out_ref):
    core = lax.axis_index("blk")

    @pl.when(core == ITEM)
    def _():
        for k in range(GROUP):
            keep, got = (keep0_ref, got0_ref) if k < 4 else (keep1_ref, got1_ref)
            i = k % 4
            out_ref[k, :256] = (keep[i] + got[i * 256 : (i + 1) * 256].astype(f32)).astype(bf16)

    @pl.when(core != ITEM)
    def _():
        for k in range(GROUP):
            rows = slice(k * ROWS, (k + 1) * ROWS)
            out_ref[k, (1 - ITEM) * 128 : (2 - ITEM) * 128] = u_ref[rows]
            out_ref[k, ITEM * 128 : (ITEM + 1) * 128] = got0_ref[rows]

    got = got0_ref[1024:1040].astype(f32)
    tail = split(got[:8] + got[8:] + loss_part(row_sums(s_ref)))
    for k in range(GROUP):
        out_ref[k, 256:272] = tail


def sum_body(w_ref, keep_ref, give_ref):
    core = lax.axis_index("blk")

    def summed(first, rows):
        at = pl.ds(first, rows)
        total = w_ref[0, at].astype(f32)
        for k in range(1, GROUP):
            total = total + w_ref[k, at].astype(f32)
        return total

    tail = summed(256, 16)
    tail = tail[:8] + tail[8:]
    keep_ref[:128] = summed(pl.multiple_of(core * 128, 128), 128)
    give_ref[:128] = summed(pl.multiple_of((1 - core) * 128, 128), 128)
    keep_ref[128:136] = tail
    give_ref[128:136] = tail


def slope(pull, hat, direction, length):
    grad = (pull - hat) / sharpness
    along = jnp.sum(direction * grad, axis=1, keepdims=True)
    return (grad - direction * along) / length


def final_body(q_ref, v_ref, keep_ref, got_ref, s_ref, qs_ref, vs_ref, loss_ref):
    first = lax.axis_index("blk") == ITEM
    q, q_len = unit(q_ref[...])
    v, v_len = unit(v_ref[...])
    q_hat, v_hat = q.astype(bf16).astype(f32), v.astype(bf16).astype(f32)
    keep, got = keep_ref[...], got_ref[...]
    w = jnp.where(first, keep, got)
    u = jnp.where(first, got, keep)
    sums = row_sums(s_ref)[:8]
    mine = lax.broadcasted_iota(jnp.int32, sums.shape, 0) == query_index()
    own = jnp.sum(jnp.where(mine, sums, 0.0), axis=0, keepdims=True)
    u = jnp.concatenate([(u[:128, :128] / own).T, (u[:128, 128:] / own).T], axis=1)
    qs_ref[...] = slope(u, v_hat, q, q_len)
    vs_ref[...] = slope(w[:128], q_hat, v, v_len)
    loss_ref[0, 0] = jnp.max(w[128:136]) / (128 * 128)


def per_device(queries, items):
    anyspace = pl.BlockSpec(memory_space=pltpu.HBM)
    rows = (ROWS, D)
    mine, give, pos = call(
        norm_body,
        [(rows, bf16), (rows, bf16), ((8, 128), f32)],
        "norm",
        ins=[anyspace] * 2,
        scratch=[pltpu.VMEM(rows, bf16), pltpu.VMEM(rows, bf16), pltpu.SemaphoreType.DMA((2,))],
    )(*(pltpu.with_memory_space_constraint(a, pltpu.HBM) for a in (queries, items)))
    bulk = (GROUP, 2, ROWS, D)
    (tile,) = call(tile_body, [(bulk, bf16)], "tile")(mine, swap_cores(give))
    block = exchange(tile, BULK)
    flops = 2 * 2048 * 1024 * 256
    e, q, s, u = call(
        score_body,
        [
            ((GROUP, 256, 1024), bf16),
            ((GROUP, ROWS, D), bf16),
            ((GROUP, 16, 128), f32),
            ((GROUP * ROWS, D), bf16),
        ],
        "score",
        2 * flops,
        scratch=[pltpu.VMEM(bulk, bf16)],
    )(block, swap_cores(block), pos)
    sums = exchange(s, QUERY)
    keep, got = [], []
    for half in (0, 1):
        k, g = call(
            functools.partial(weigh_body, half * 4),
            [((4, 256, D), f32), ((1040 - 16 * half, D), bf16)],
            f"weigh{half}",
            flops // 2,
        )(*([u] if half == 0 else []), e, q, sums)
        keep.append(k)
        got.append(swap_cores(g))
    (out,) = call(join_body, [((GROUP, 272, D), bf16)], "join")(*keep, *got, u, sums)
    out = exchange(out, BULK)
    keep, give = call(sum_body, [((136, D), f32), ((136, D), f32)], "sum")(out)
    q_slope, v_slope, loss = call(
        final_body, [(rows, f32), (rows, f32), ((1, 1), f32, pltpu.SMEM)], "final"
    )(queries, items, keep, swap_cores(give), sums)
    return loss.reshape(()), q_slope, v_slope


def solution(mesh):
    split = Mesh(mesh.devices.reshape(2, 4, 4, 4), AXES)
    rows = P(AXES, None)
    return jax.shard_map(
        per_device, mesh=split, in_specs=(rows, rows), out_specs=(P(), rows, rows), check_vma=False
    )
```

```python
import math

import jax
import jax.numpy as jnp
from jax import lax
from jax.experimental import pallas as pl
from jax.experimental.pallas import tpu as pltpu
from jax.sharding import Mesh
from jax.sharding import PartitionSpec as P

AXES = ("blk", "z", "y", "x")
GROUP = 8
ROWS, D = 128, 256
ITEM = 1

sharpness = 0.05
tiny_square = 1e-12
log2_e = math.log2(math.e)
f32, bf16 = jnp.float32, jnp.bfloat16


def device_of(core, z, y, x):
    return ((core * 4 + z) * 4 + y) * 4 + x


def query_groups(core):
    return [[device_of(core, z, y, x) for y in pair for x in range(4)] for z in range(4) for pair in ((0, 1), (2, 3))]


def item_groups(core):
    return [[device_of(core, z, y, x) for y in pair for z in range(4)] for x in range(4) for pair in ((1, 2), (3, 0))]


def query_index():
    return lax.axis_index("y") % 2 * 4 + lax.axis_index("x")


BULK = item_groups(ITEM) + query_groups(1 - ITEM)
QUERY = query_groups(0) + query_groups(1)


def exchange(pieces, groups):
    return lax.all_to_all(pieces, AXES, 0, 0, tiled=True, axis_index_groups=groups)


def swap_cores(value):
    return lax.ppermute(value, "blk", [(0, 1), (1, 0)])


def call(body, outs, name, flops=0, ins=None, scratch=()):
    spec = pl.BlockSpec(memory_space=pltpu.VMEM)
    return pl.pallas_call(
        body,
        out_shape=[jax.ShapeDtypeStruct(s, d) for s, d, *_ in outs],
        out_specs=[pl.BlockSpec(memory_space=o[2]) if len(o) > 2 else spec for o in outs],
        **({"in_specs": ins} if ins else {}),
        scratch_shapes=list(scratch),
        compiler_params=pltpu.CompilerParams(vmem_limit_bytes=24 * 2**20),
        cost_estimate=pl.CostEstimate(flops=flops, bytes_accessed=0, transcendentals=0),
        name=name,
    )


def unit(matrix):
    wide = matrix.astype(f32)
    length = jnp.sqrt(jnp.sum(wide * wide, axis=1, keepdims=True) + tiny_square)
    return wide / length, length


def hat(matrix):
    return unit(matrix)[0].astype(bf16)


def norm_body(q_hbm, v_hbm, mine_ref, pos_ref, q_ref, v_ref, sem):
    copies = [
        pltpu.make_async_copy(q_hbm, q_ref, sem.at[0]),
        pltpu.make_async_copy(v_hbm, v_ref, sem.at[1]),
    ]
    for c in copies:
        c.start()
    core = lax.axis_index("blk")
    for c in copies:
        c.wait()
    q, v = hat(q_ref[...]), hat(v_ref[...])
    total = jnp.sum(q.astype(f32) * v.astype(f32)) / sharpness
    pos_ref[...] = jnp.full((8, 128), total, f32)

    @pl.when(core == ITEM)
    def _():
        mine_ref[...] = v

    @pl.when(core != ITEM)
    def _():
        mine_ref[...] = q


def tile_body(mine_ref, got_q_ref, got_v_ref, out_ref):
    core = lax.axis_index("blk")

    def fill(got_ref):
        mine, got = mine_ref[...], hat(got_ref[...])
        for k in range(GROUP):
            out_ref[k, core] = mine
            out_ref[k, 1 - core] = got

    @pl.when(core == ITEM)
    def _():
        fill(got_v_ref)

    @pl.when(core != ITEM)
    def _():
        fill(got_q_ref)


def score_body(mine_ref, got_ref, pos_ref, e_ref, q_ref, v_ref, s_ref):
    core = lax.axis_index("blk")

    @pl.when(core == ITEM)
    def _():
        v_ref[...] = mine_ref[...]
        q_ref[...] = got_ref[:, ITEM]

    @pl.when(core != ITEM)
    def _():
        v_ref[...] = got_ref[...]
        q_ref[...] = mine_ref[:, 1 - ITEM]

    cols = GROUP * ROWS
    q = q_ref[...].reshape(cols, D)
    total = jnp.zeros((1, cols), f32)
    for k in range(GROUP):
        v = v_ref[k].reshape(2 * ROWS, D)
        t = lax.dot_general(v, q, (((1,), (1,)), ((), ())), preferred_element_type=f32)
        e = jnp.exp2(t * (log2_e / sharpness))
        total = total + jnp.sum(e, axis=0, keepdims=True)
        e_ref[k] = e.astype(bf16)
    for k in range(GROUP):
        for j in range(GROUP):
            s_ref[j, k : k + 1] = total[:, k * ROWS : (k + 1) * ROWS]
    for j in range(GROUP):
        s_ref[j, 8:16] = pos_ref[...]


def row_sums(s_ref):
    total = s_ref[0]
    for j in range(1, GROUP):
        total = total + s_ref[j]
    return total


def split(value):
    high = value.astype(bf16)
    low = (value - high.astype(f32)).astype(bf16)
    return jnp.concatenate([high.astype(f32), low.astype(f32)], axis=0).astype(bf16)


def loss_part(sums):
    return jnp.sum(jnp.log(sums[:8])) - jnp.max(sums[8:9])


def weigh(e_ref, q_ref, r, first, store):
    q = q_ref[...].reshape(GROUP * ROWS, D)
    for k in range(GROUP // 2):
        parts = [
            (e_ref[first + k, :, j * ROWS : (j + 1) * ROWS].astype(f32) * r[j : j + 1]).astype(bf16)
            for j in range(GROUP)
        ]
        store(k, jnp.dot(jnp.concatenate(parts, axis=1), q, preferred_element_type=f32))


def pull(v_ref, e_ref, u_ref):
    total = None
    for k in range(0, GROUP, 2):
        v = v_ref[k : k + 2].reshape(4 * ROWS, D)
        e = e_ref[k : k + 2].reshape(4 * ROWS, GROUP * ROWS)
        part = lax.dot_general(v, e, (((0,), (0,)), ((), ())), preferred_element_type=f32)
        total = part if total is None else total + part
    for k in range(GROUP):
        rows = slice(k * ROWS, (k + 1) * ROWS)
        u_ref[rows, :ROWS] = total[:ROWS, rows].astype(bf16)
        u_ref[rows, ROWS:] = total[ROWS:, rows].astype(bf16)


def first_body(e_ref, q_ref, s_ref, keep_ref, give_ref):
    sums = row_sums(s_ref)

    def store(k, w):
        keep_ref[k] = w
        give_ref[k * 256 : (k + 1) * 256] = w.astype(bf16)

    weigh(e_ref, q_ref, 1.0 / sums[:8], 0, store)
    give_ref[1024:1040] = split(jnp.full((8, D), loss_part(sums), f32))


def second_body(e_ref, q_ref, s_ref, v_ref, give_ref):
    core = lax.axis_index("blk")

    @pl.when(core == ITEM)
    def _():
        pull(v_ref, e_ref, give_ref)

    @pl.when(core != ITEM)
    def _():
        def store(k, w):
            give_ref[k * 256 : (k + 1) * 256] = w.astype(bf16)

        weigh(e_ref, q_ref, 1.0 / row_sums(s_ref)[:8], 4, store)


def third_body(e_ref, q_ref, s_ref, v_ref, keep_ref, u_ref):
    core = lax.axis_index("blk")

    @pl.when(core == ITEM)
    def _():
        def store(k, w):
            keep_ref[k] = w

        weigh(e_ref, q_ref, 1.0 / row_sums(s_ref)[:8], 4, store)

    @pl.when(core != ITEM)
    def _():
        pull(v_ref, e_ref, u_ref)


def join_body(keep0_ref, keep1_ref, got0_ref, got1_ref, u_ref, s_ref, out_ref):
    core = lax.axis_index("blk")

    @pl.when(core == ITEM)
    def _():
        for k in range(GROUP):
            keep, got = (keep0_ref, got0_ref) if k < 4 else (keep1_ref, got1_ref)
            i = k % 4
            out_ref[k, :256] = (keep[i] + got[i * 256 : (i + 1) * 256].astype(f32)).astype(bf16)

    @pl.when(core != ITEM)
    def _():
        for k in range(GROUP):
            rows = slice(k * ROWS, (k + 1) * ROWS)
            out_ref[k, (1 - ITEM) * 128 : (2 - ITEM) * 128] = u_ref[rows]
            out_ref[k, ITEM * 128 : (ITEM + 1) * 128] = got1_ref[rows]

    got = got0_ref[1024:1040].astype(f32)
    tail = split(got[:8] + got[8:] + loss_part(row_sums(s_ref)))
    for k in range(GROUP):
        out_ref[k, 256:272] = tail


def sum_body(w_ref, keep_ref, give_ref):
    core = lax.axis_index("blk")

    def summed(first, rows):
        at = pl.ds(first, rows)
        total = w_ref[0, at].astype(f32)
        for k in range(1, GROUP):
            total = total + w_ref[k, at].astype(f32)
        return total

    tail = summed(256, 16)
    tail = tail[:8] + tail[8:]
    keep_ref[:128] = summed(pl.multiple_of(core * 128, 128), 128)
    give_ref[:128] = summed(pl.multiple_of((1 - core) * 128, 128), 128)
    keep_ref[128:136] = tail
    give_ref[128:136] = tail


def slope(pull, hat, direction, length):
    grad = (pull - hat) / sharpness
    along = jnp.sum(direction * grad, axis=1, keepdims=True)
    return (grad - direction * along) / length


def final_body(q_ref, v_ref, keep_ref, got_ref, s_ref, qs_ref, vs_ref, loss_ref):
    first = lax.axis_index("blk") == ITEM
    q, q_len = unit(q_ref[...])
    v, v_len = unit(v_ref[...])
    q_hat, v_hat = q.astype(bf16).astype(f32), v.astype(bf16).astype(f32)
    keep, got = keep_ref[...], got_ref[...]
    w = jnp.where(first, keep, got)
    u = jnp.where(first, got, keep)
    sums = row_sums(s_ref)[:8]
    mine = lax.broadcasted_iota(jnp.int32, sums.shape, 0) == query_index()
    own = jnp.sum(jnp.where(mine, sums, 0.0), axis=0, keepdims=True)
    u = jnp.concatenate([(u[:128, :128] / own).T, (u[:128, 128:] / own).T], axis=1)
    qs_ref[...] = slope(u, v_hat, q, q_len)
    vs_ref[...] = slope(w[:128], q_hat, v, v_len)
    loss_ref[0, 0] = jnp.max(w[128:136]) / (128 * 128)


def per_device(queries, items):
    rows = (ROWS, D)
    bulk = (GROUP, 2, ROWS, D)
    in_hbm = [pltpu.with_memory_space_constraint(a, pltpu.HBM) for a in (queries, items)]
    mine, pos = call(
        norm_body,
        [(rows, bf16), ((8, 128), f32)],
        "norm",
        10**9,
        ins=[pl.BlockSpec(memory_space=pltpu.HBM)] * 2,
        scratch=[pltpu.VMEM(rows, bf16), pltpu.VMEM(rows, bf16), pltpu.SemaphoreType.DMA((2,))],
    )(*in_hbm)
    (tile,) = call(tile_body, [(bulk, bf16)], "tile")(mine, swap_cores(queries), swap_cores(items))
    block = exchange(tile, BULK)
    flops = 2 * 2048 * 1024 * 256
    e, q, v, s = call(
        score_body,
        [
            ((GROUP, 256, 1024), bf16),
            ((GROUP, ROWS, D), bf16),
            (bulk, bf16),
            ((GROUP, 16, 128), f32),
        ],
        "score",
        flops,
    )(block, swap_cores(block), pos)
    sums = exchange(s, QUERY)
    half, pulled = (4, 256, D), (GROUP * ROWS, D)
    keep0, give = call(first_body, [(half, f32), ((1040, D), bf16)], "first", flops)(e, q, sums)
    got0 = swap_cores(give)
    (give,) = call(second_body, [(pulled, bf16)], "second", flops)(e, q, sums, v)
    got1 = swap_cores(give)
    keep1, u = call(third_body, [(half, f32), (pulled, bf16)], "third", flops)(e, q, sums, v)
    (out,) = call(join_body, [((GROUP, 272, D), bf16)], "join")(keep0, keep1, got0, got1, u, sums)
    out = exchange(out, BULK)
    keep, give = call(sum_body, [((136, D), f32), ((136, D), f32)], "sum")(out)
    q_slope, v_slope, loss = call(
        final_body, [(rows, f32), (rows, f32), ((1, 1), f32, pltpu.SMEM)], "final"
    )(queries, items, keep, swap_cores(give), sums)
    return loss.reshape(()), q_slope, v_slope


def solution(mesh):
    split = Mesh(mesh.devices.reshape(2, 4, 4, 4), AXES)
    rows = P(AXES, None)
    return jax.shard_map(
        per_device, mesh=split, in_specs=(rows, rows), out_specs=(P(), rows, rows), check_vma=False
    )
```

```python
import math

import jax
import jax.numpy as jnp
from jax import lax
from jax.experimental import pallas as pl
from jax.experimental.pallas import tpu as pltpu
from jax.sharding import Mesh
from jax.sharding import PartitionSpec as P

AXES = ("blk", "z", "y", "x")
GROUP = 8
ROWS, D = 128, 256
ITEM = 1

sharpness = 0.05
tiny_square = 1e-12
log2_e = math.log2(math.e)
f32, bf16 = jnp.float32, jnp.bfloat16


def device_of(core, z, y, x):
    return ((core * 4 + z) * 4 + y) * 4 + x


def query_groups(core):
    return [[device_of(core, z, y, x) for y in pair for x in range(4)] for z in range(4) for pair in ((0, 1), (2, 3))]


def item_groups(core):
    return [[device_of(core, z, y, x) for y in pair for z in range(4)] for x in range(4) for pair in ((1, 2), (3, 0))]


def query_index():
    return lax.axis_index("y") % 2 * 4 + lax.axis_index("x")


BULK = item_groups(ITEM) + query_groups(1 - ITEM)
QUERY = query_groups(0) + query_groups(1)


def exchange(pieces, groups):
    return lax.all_to_all(pieces, AXES, 0, 0, tiled=True, axis_index_groups=groups)


def swap_cores(value):
    return lax.ppermute(value, "blk", [(0, 1), (1, 0)])


def call(body, outs, name, flops=0, ins=None, scratch=()):
    spec = pl.BlockSpec(memory_space=pltpu.VMEM)
    return pl.pallas_call(
        body,
        out_shape=[jax.ShapeDtypeStruct(s, d) for s, d, *_ in outs],
        out_specs=[pl.BlockSpec(memory_space=o[2]) if len(o) > 2 else spec for o in outs],
        **({"in_specs": ins} if ins else {}),
        scratch_shapes=list(scratch),
        compiler_params=pltpu.CompilerParams(vmem_limit_bytes=24 * 2**20),
        cost_estimate=pl.CostEstimate(flops=flops, bytes_accessed=0, transcendentals=0),
        name=name,
    )


def unit(matrix):
    wide = matrix.astype(f32)
    length = jnp.sqrt(jnp.sum(wide * wide, axis=1, keepdims=True) + tiny_square)
    return wide / length, length


def hat(matrix):
    return unit(matrix)[0].astype(bf16)


def norm_body(q_hbm, v_hbm, mine_ref, pos_ref, q_ref, v_ref, sem):
    copies = [
        pltpu.make_async_copy(q_hbm, q_ref, sem.at[0]),
        pltpu.make_async_copy(v_hbm, v_ref, sem.at[1]),
    ]
    for c in copies:
        c.start()
    core = lax.axis_index("blk")
    for c in copies:
        c.wait()
    q, v = hat(q_ref[...]), hat(v_ref[...])
    total = jnp.sum(q.astype(f32) * v.astype(f32)) / sharpness
    pos_ref[...] = jnp.full((8, 128), total, f32)

    @pl.when(core == ITEM)
    def _():
        mine_ref[...] = v

    @pl.when(core != ITEM)
    def _():
        mine_ref[...] = q


def tile_body(mine_ref, got_q_ref, got_v_ref, out_ref):
    core = lax.axis_index("blk")

    def fill(got_ref):
        mine, got = mine_ref[...], hat(got_ref[...])
        for k in range(GROUP):
            out_ref[k, core] = mine
            out_ref[k, 1 - core] = got

    @pl.when(core == ITEM)
    def _():
        fill(got_v_ref)

    @pl.when(core != ITEM)
    def _():
        fill(got_q_ref)


def score_body(mine_ref, got_ref, pos_ref, e_ref, q_ref, v_ref, s_ref):
    core = lax.axis_index("blk")

    @pl.when(core == ITEM)
    def _():
        v_ref[...] = mine_ref[...]
        q_ref[...] = got_ref[:, ITEM]

    @pl.when(core != ITEM)
    def _():
        v_ref[...] = got_ref[...]
        q_ref[...] = mine_ref[:, 1 - ITEM]

    cols = GROUP * ROWS
    q = q_ref[...].reshape(cols, D)
    total = jnp.zeros((1, cols), f32)
    for k in range(GROUP):
        v = v_ref[k].reshape(2 * ROWS, D)
        t = lax.dot_general(v, q, (((1,), (1,)), ((), ())), preferred_element_type=f32)
        e = jnp.exp2(t * (log2_e / sharpness))
        total = total + jnp.sum(e, axis=0, keepdims=True)
        e_ref[k] = e.astype(bf16)
    for k in range(GROUP):
        for j in range(GROUP):
            s_ref[j, k : k + 1] = total[:, k * ROWS : (k + 1) * ROWS]
    for j in range(GROUP):
        s_ref[j, 8:16] = pos_ref[...]


def row_sums(s_ref):
    total = s_ref[0]
    for j in range(1, GROUP):
        total = total + s_ref[j]
    return total


def loss_part(sums):
    return jnp.sum(jnp.log(sums[:8])) - jnp.max(sums[8:9])


def split(value):
    high = value.astype(bf16).astype(f32)
    return jnp.concatenate([high, value - high], axis=1).astype(bf16)


def joined(tail):
    tail = tail.astype(f32)
    return tail[:, :128] + tail[:, 128:]


def weigh(e_ref, q_ref, r, first, store):
    q = q_ref[...].reshape(GROUP * ROWS, D)
    for k in range(GROUP // 2):
        parts = [
            (e_ref[first + k, :, j * ROWS : (j + 1) * ROWS].astype(f32) * r[j : j + 1]).astype(bf16)
            for j in range(GROUP)
        ]
        store(k, jnp.dot(jnp.concatenate(parts, axis=1), q, preferred_element_type=f32))


def pull(v_ref, e_ref, u_ref):
    total = None
    for k in range(0, GROUP, 2):
        v = v_ref[k : k + 2].reshape(4 * ROWS, D)
        e = e_ref[k : k + 2].reshape(4 * ROWS, GROUP * ROWS)
        part = lax.dot_general(v, e, (((0,), (0,)), ((), ())), preferred_element_type=f32)
        total = part if total is None else total + part
    for k in range(GROUP):
        rows = slice(k * ROWS, (k + 1) * ROWS)
        u_ref[rows, :ROWS] = total[:ROWS, rows].astype(bf16)
        u_ref[rows, ROWS:] = total[ROWS:, rows].astype(bf16)


def first_body(e_ref, q_ref, s_ref, v_ref, give_ref):
    core = lax.axis_index("blk")
    sums = row_sums(s_ref)
    give_ref[1024:1032] = split(jnp.full((8, 128), loss_part(sums), f32))

    @pl.when(core == ITEM)
    def _():
        pull(v_ref, e_ref, give_ref)

    @pl.when(core != ITEM)
    def _():
        def store(k, w):
            give_ref[k * 256 : (k + 1) * 256] = w.astype(bf16)

        weigh(e_ref, q_ref, 1.0 / sums[:8], 0, store)


def second_body(e_ref, q_ref, s_ref, keep_ref, give_ref):
    core = lax.axis_index("blk")
    r = 1.0 / row_sums(s_ref)[:8]

    @pl.when(core == ITEM)
    def _():
        def store(k, w):
            keep_ref[k] = w

        weigh(e_ref, q_ref, r, 0, store)

    @pl.when(core != ITEM)
    def _():
        def store(k, w):
            give_ref[k * 256 : (k + 1) * 256] = w.astype(bf16)

        weigh(e_ref, q_ref, r, 4, store)


def third_body(e_ref, q_ref, s_ref, v_ref, keep_ref, u_ref):
    core = lax.axis_index("blk")

    @pl.when(core == ITEM)
    def _():
        def store(k, w):
            keep_ref[k] = w

        weigh(e_ref, q_ref, 1.0 / row_sums(s_ref)[:8], 4, store)

    @pl.when(core != ITEM)
    def _():
        pull(v_ref, e_ref, u_ref)


def join_body(keep0_ref, keep1_ref, got0_ref, got1_ref, u_ref, s_ref, out_ref):
    core = lax.axis_index("blk")

    @pl.when(core == ITEM)
    def _():
        for k in range(GROUP):
            keep, got = (keep0_ref, got0_ref) if k < 4 else (keep1_ref, got1_ref)
            i = k % 4
            out_ref[k, :256] = (keep[i] + got[i * 256 : (i + 1) * 256].astype(f32)).astype(bf16)

    @pl.when(core != ITEM)
    def _():
        for k in range(GROUP):
            rows = slice(k * ROWS, (k + 1) * ROWS)
            out_ref[k, (1 - ITEM) * 128 : (2 - ITEM) * 128] = u_ref[rows]
            out_ref[k, ITEM * 128 : (ITEM + 1) * 128] = got0_ref[rows]

    tail = split(joined(got0_ref[1024:1032]) + loss_part(row_sums(s_ref)))
    for k in range(GROUP):
        out_ref[k, 256:264] = tail


def sum_body(w_ref, keep_ref, give_ref):
    core = lax.axis_index("blk")

    def summed(first, rows):
        at = pl.ds(first, rows)
        total = w_ref[0, at].astype(f32)
        for k in range(1, GROUP):
            total = total + w_ref[k, at].astype(f32)
        return total

    tail = jnp.concatenate([joined(summed(256, 8))] * 2, axis=1)
    keep_ref[:128] = summed(pl.multiple_of(core * 128, 128), 128)
    give_ref[:128] = summed(pl.multiple_of((1 - core) * 128, 128), 128)
    keep_ref[128:136] = tail
    give_ref[128:136] = tail


def slope(pull, hat, direction, length):
    grad = (pull - hat) / sharpness
    along = jnp.sum(direction * grad, axis=1, keepdims=True)
    return (grad - direction * along) / length


def final_body(q_ref, v_ref, keep_ref, got_ref, s_ref, qs_ref, vs_ref, loss_ref):
    first = lax.axis_index("blk") == ITEM
    q, q_len = unit(q_ref[...])
    v, v_len = unit(v_ref[...])
    q_hat, v_hat = q.astype(bf16).astype(f32), v.astype(bf16).astype(f32)
    keep, got = keep_ref[...], got_ref[...]
    w = jnp.where(first, keep, got)
    u = jnp.where(first, got, keep)
    sums = row_sums(s_ref)[:8]
    mine = lax.broadcasted_iota(jnp.int32, sums.shape, 0) == query_index()
    own = jnp.sum(jnp.where(mine, sums, 0.0), axis=0, keepdims=True)
    u = jnp.concatenate([(u[:128, :128] / own).T, (u[:128, 128:] / own).T], axis=1)
    qs_ref[...] = slope(u, v_hat, q, q_len)
    vs_ref[...] = slope(w[:128], q_hat, v, v_len)
    loss_ref[0, 0] = jnp.max(w[128:136]) / (128 * 128)


def per_device(queries, items):
    rows = (ROWS, D)
    bulk = (GROUP, 2, ROWS, D)
    in_hbm = [pltpu.with_memory_space_constraint(a, pltpu.HBM) for a in (queries, items)]
    mine, pos = call(
        norm_body,
        [(rows, bf16), ((8, 128), f32)],
        "norm",
        10**9,
        ins=[pl.BlockSpec(memory_space=pltpu.HBM)] * 2,
        scratch=[pltpu.VMEM(rows, bf16), pltpu.VMEM(rows, bf16), pltpu.SemaphoreType.DMA((2,))],
    )(*in_hbm)
    (tile,) = call(tile_body, [(bulk, bf16)], "tile")(mine, swap_cores(queries), swap_cores(items))
    block = exchange(tile, BULK)
    flops = 2 * 2048 * 1024 * 256
    e, q, v, s = call(
        score_body,
        [
            ((GROUP, 256, 1024), bf16),
            ((GROUP, ROWS, D), bf16),
            (bulk, bf16),
            ((GROUP, 16, 128), f32),
        ],
        "score",
        flops,
    )(block, swap_cores(block), pos)
    sums = exchange(s, QUERY)
    half, pulled = (4, 256, D), (GROUP * ROWS, D)
    (give,) = call(first_body, [((1032, D), bf16)], "first", flops)(e, q, sums, v)
    got0 = swap_cores(give)
    keep0, give = call(second_body, [(half, f32), (pulled, bf16)], "second", flops)(e, q, sums)
    got1 = swap_cores(give)
    keep1, u = call(third_body, [(half, f32), (pulled, bf16)], "third", flops)(e, q, sums, v)
    (out,) = call(join_body, [((GROUP, 264, D), bf16)], "join")(keep0, keep1, got0, got1, u, sums)
    out = exchange(out, BULK)
    keep, give = call(sum_body, [((136, D), f32), ((136, D), f32)], "sum")(out)
    q_slope, v_slope, loss = call(
        final_body, [(rows, f32), (rows, f32), ((1, 1), f32, pltpu.SMEM)], "final"
    )(queries, items, keep, swap_cores(give), sums)
    return loss.reshape(()), q_slope, v_slope


def solution(mesh):
    split = Mesh(mesh.devices.reshape(2, 4, 4, 4), AXES)
    rows = P(AXES, None)
    return jax.shard_map(
        per_device, mesh=split, in_specs=(rows, rows), out_specs=(P(), rows, rows), check_vma=False
    )
```

```python
import math

import jax
import jax.numpy as jnp
from jax import lax
from jax.experimental import pallas as pl
from jax.experimental.pallas import tpu as pltpu
from jax.sharding import Mesh
from jax.sharding import PartitionSpec as P

AXES = ("blk", "z", "y", "x")
GROUP = 8
ROWS, D = 128, 256
ITEM = 1

sharpness = 0.05
tiny_square = 1e-12
log2_e = math.log2(math.e)
f32, bf16 = jnp.float32, jnp.bfloat16


def device_of(core, z, y, x):
    return ((core * 4 + z) * 4 + y) * 4 + x


def query_groups(core):
    return [[device_of(core, z, y, x) for y in pair for x in range(4)] for z in range(4) for pair in ((0, 1), (2, 3))]


def item_groups(core):
    return [[device_of(core, z, y, x) for y in pair for z in range(4)] for x in range(4) for pair in ((1, 2), (3, 0))]


def query_index():
    return lax.axis_index("y") % 2 * 4 + lax.axis_index("x")


BULK = item_groups(ITEM) + query_groups(1 - ITEM)
QUERY = query_groups(0) + query_groups(1)


def exchange(pieces, groups):
    return lax.all_to_all(pieces, AXES, 0, 0, tiled=True, axis_index_groups=groups)


def swap_cores(value):
    return lax.ppermute(value, "blk", [(0, 1), (1, 0)])


def call(body, outs, name, flops=0, ins=None, scratch=()):
    spec = pl.BlockSpec(memory_space=pltpu.VMEM)
    return pl.pallas_call(
        body,
        out_shape=[jax.ShapeDtypeStruct(s, d) for s, d, *_ in outs],
        out_specs=[pl.BlockSpec(memory_space=o[2]) if len(o) > 2 else spec for o in outs],
        **({"in_specs": ins} if ins else {}),
        scratch_shapes=list(scratch),
        compiler_params=pltpu.CompilerParams(vmem_limit_bytes=24 * 2**20),
        cost_estimate=pl.CostEstimate(flops=flops, bytes_accessed=0, transcendentals=0),
        name=name,
    )


def unit(matrix):
    wide = matrix.astype(f32)
    length = jnp.sqrt(jnp.sum(wide * wide, axis=1, keepdims=True) + tiny_square)
    return wide / length, length


def hat(matrix):
    return unit(matrix)[0].astype(bf16)


def norm_body(q_hbm, v_hbm, mine_ref, pos_ref, q_ref, v_ref, sem):
    copies = [
        pltpu.make_async_copy(q_hbm, q_ref, sem.at[0]),
        pltpu.make_async_copy(v_hbm, v_ref, sem.at[1]),
    ]
    for c in copies:
        c.start()
    core = lax.axis_index("blk")
    for c in copies:
        c.wait()
    q, v = hat(q_ref[...]), hat(v_ref[...])
    total = jnp.sum(q.astype(f32) * v.astype(f32)) / sharpness
    pos_ref[...] = jnp.full((8, 128), total, f32)

    @pl.when(core == ITEM)
    def _():
        mine_ref[...] = v

    @pl.when(core != ITEM)
    def _():
        mine_ref[...] = q


def tile_body(mine_ref, got_q_ref, got_v_ref, out_ref):
    core = lax.axis_index("blk")

    def fill(got_ref):
        mine, got = mine_ref[...], hat(got_ref[...])
        for k in range(GROUP):
            out_ref[k, core] = mine
            out_ref[k, 1 - core] = got

    @pl.when(core == ITEM)
    def _():
        fill(got_v_ref)

    @pl.when(core != ITEM)
    def _():
        fill(got_q_ref)


def half_body(block_ref, out_ref):
    core = lax.axis_index("blk")

    @pl.when(core == ITEM)
    def _():
        out_ref[...] = block_ref[:4].reshape(GROUP, ROWS, D)

    @pl.when(core != ITEM)
    def _():
        out_ref[...] = block_ref[:, ITEM]


def rest_body(block_ref, out_ref):
    out_ref[...] = block_ref[4:].reshape(GROUP, ROWS, D)


def scores(v_ref, q_ref, e_ref):
    q = q_ref[...].reshape(GROUP * ROWS, D)
    total = jnp.zeros((1, GROUP * ROWS), f32)
    for k in range(4):
        v = v_ref[k].reshape(2 * ROWS, D)
        t = lax.dot_general(v, q, (((1,), (1,)), ((), ())), preferred_element_type=f32)
        e = jnp.exp2(t * (log2_e / sharpness))
        total = total + jnp.sum(e, axis=0, keepdims=True)
        e_ref[k] = e.astype(bf16)
    return total


def score0_body(block_ref, got_ref, e_ref, q_ref, v_ref, t_ref):
    core = lax.axis_index("blk")

    @pl.when(core == ITEM)
    def _():
        v_ref[...] = block_ref[:4]
        q_ref[...] = got_ref[...]

    @pl.when(core != ITEM)
    def _():
        v_ref[...] = got_ref[...].reshape(4, 2, ROWS, D)
        q_ref[...] = block_ref[:, 1 - ITEM]

    t_ref[...] = jnp.broadcast_to(scores(v_ref, q_ref, e_ref), t_ref.shape)


def score1_body(block_ref, got_ref, q_ref, t_ref, pos_ref, e_ref, v_ref, s_ref):
    core = lax.axis_index("blk")

    @pl.when(core == ITEM)
    def _():
        v_ref[...] = block_ref[4:]

    @pl.when(core != ITEM)
    def _():
        v_ref[...] = got_ref[...].reshape(4, 2, ROWS, D)

    total = t_ref[:1] + scores(v_ref, q_ref, e_ref)
    for k in range(GROUP):
        for j in range(GROUP):
            s_ref[j, k : k + 1] = total[:, k * ROWS : (k + 1) * ROWS]
    for j in range(GROUP):
        s_ref[j, 8:16] = pos_ref[...]


def row_sums(s_ref):
    total = s_ref[0]
    for j in range(1, GROUP):
        total = total + s_ref[j]
    return total


def loss_part(sums):
    return jnp.sum(jnp.log(sums[:8])) - jnp.max(sums[8:9])


def split(value):
    high = value.astype(bf16).astype(f32)
    return jnp.concatenate([high, value - high], axis=1).astype(bf16)


def joined(tail):
    tail = tail.astype(f32)
    return tail[:, :128] + tail[:, 128:]


def weigh(e_ref, q_ref, r, store):
    q = q_ref[...].reshape(GROUP * ROWS, D)
    for k in range(4):
        parts = [
            (e_ref[k, :, j * ROWS : (j + 1) * ROWS].astype(f32) * r[j : j + 1]).astype(bf16)
            for j in range(GROUP)
        ]
        store(k, jnp.dot(jnp.concatenate(parts, axis=1), q, preferred_element_type=f32))


def pull(v_refs, e_refs, u_ref):
    total = None
    for v_ref, e_ref in zip(v_refs, e_refs):
        for k in (0, 2):
            v = v_ref[k : k + 2].reshape(4 * ROWS, D)
            e = e_ref[k : k + 2].reshape(4 * ROWS, GROUP * ROWS)
            part = lax.dot_general(v, e, (((0,), (0,)), ((), ())), preferred_element_type=f32)
            total = part if total is None else total + part
    for k in range(GROUP):
        rows = slice(k * ROWS, (k + 1) * ROWS)
        u_ref[rows, :ROWS] = total[:ROWS, rows].astype(bf16)
        u_ref[rows, ROWS:] = total[ROWS:, rows].astype(bf16)


def into(ref):
    def store(k, w):
        ref[k * 256 : (k + 1) * 256] = w.astype(bf16)

    return store


def first_body(e0_ref, e1_ref, v0_ref, v1_ref, q_ref, s_ref, give_ref):
    core = lax.axis_index("blk")
    sums = row_sums(s_ref)
    give_ref[1024:1032] = split(jnp.full((8, 128), loss_part(sums), f32))

    @pl.when(core == ITEM)
    def _():
        pull((v0_ref, v1_ref), (e0_ref, e1_ref), give_ref)

    @pl.when(core != ITEM)
    def _():
        weigh(e0_ref, q_ref, 1.0 / sums[:8], into(give_ref))


def second_body(e1_ref, q_ref, s_ref, give_ref):
    @pl.when(lax.axis_index("blk") != ITEM)
    def _():
        weigh(e1_ref, q_ref, 1.0 / row_sums(s_ref)[:8], into(give_ref))


def third_body(e0_ref, e1_ref, v0_ref, v1_ref, q_ref, s_ref, keep_ref, u_ref):
    core = lax.axis_index("blk")

    @pl.when(core == ITEM)
    def _():
        r = 1.0 / row_sums(s_ref)[:8]
        for first, e_ref in ((0, e0_ref), (4, e1_ref)):

            def store(k, w):
                keep_ref[first + k] = w

            weigh(e_ref, q_ref, r, store)

    @pl.when(core != ITEM)
    def _():
        pull((v0_ref, v1_ref), (e0_ref, e1_ref), u_ref)


def merge_body(keep_ref, u_ref, got_ref, s_ref, out_ref):
    core = lax.axis_index("blk")

    @pl.when(core == ITEM)
    def _():
        for k in range(4):
            got = got_ref[k * 256 : (k + 1) * 256].astype(f32)
            out_ref[k, :256] = (keep_ref[k] + got).astype(bf16)

    @pl.when(core != ITEM)
    def _():
        for k in range(GROUP):
            rows = slice(k * ROWS, (k + 1) * ROWS)
            out_ref[k, (1 - ITEM) * 128 : (2 - ITEM) * 128] = u_ref[rows]
            out_ref[k, ITEM * 128 : (ITEM + 1) * 128] = got_ref[rows]

    tail = split(joined(got_ref[1024:1032]) + loss_part(row_sums(s_ref)))
    for k in range(GROUP):
        out_ref[k, 256:264] = tail


def join_body(part_ref, keep_ref, got_ref, out_ref):
    core = lax.axis_index("blk")
    out_ref[:4] = part_ref[:4]
    out_ref[4:, 256:264] = part_ref[4:, 256:264]

    @pl.when(core == ITEM)
    def _():
        for k in range(4):
            got = got_ref[k * 256 : (k + 1) * 256].astype(f32)
            out_ref[4 + k, :256] = (keep_ref[4 + k] + got).astype(bf16)

    @pl.when(core != ITEM)
    def _():
        out_ref[4:, :256] = part_ref[4:, :256]


def summed(w_ref, first, rows):
    at = pl.ds(first, rows)
    total = w_ref[0, at].astype(f32)
    for k in range(1, GROUP):
        total = total + w_ref[k, at].astype(f32)
    return total


def give_body(w_ref, give_ref):
    core = lax.axis_index("blk")
    give_ref[:128] = summed(w_ref, pl.multiple_of((1 - core) * 128, 128), 128)
    give_ref[128:136] = jnp.concatenate([joined(summed(w_ref, 256, 8))] * 2, axis=1)


def slope(pull, hat, direction, length):
    grad = (pull - hat) / sharpness
    along = jnp.sum(direction * grad, axis=1, keepdims=True)
    return (grad - direction * along) / length


def query_slope(u, q_ref, v_ref, s_ref):
    q, q_len = unit(q_ref[...])
    sums = row_sums(s_ref)[:8]
    mine = lax.broadcasted_iota(jnp.int32, sums.shape, 0) == query_index()
    own = jnp.sum(jnp.where(mine, sums, 0.0), axis=0, keepdims=True)
    u = jnp.concatenate([(u[:, :128] / own).T, (u[:, 128:] / own).T], axis=1)
    return slope(u, hat(v_ref[...]).astype(f32), q, q_len)


def item_slope(w, q_ref, v_ref):
    v, v_len = unit(v_ref[...])
    return slope(w, hat(q_ref[...]).astype(f32), v, v_len)


def own_body(w_ref, q_ref, v_ref, s_ref, own_ref):
    core = lax.axis_index("blk")
    own = summed(w_ref, pl.multiple_of(core * 128, 128), 128)

    @pl.when(core == ITEM)
    def _():
        own_ref[...] = item_slope(own, q_ref, v_ref)

    @pl.when(core != ITEM)
    def _():
        own_ref[...] = query_slope(own, q_ref, v_ref, s_ref)


def final_body(q_ref, v_ref, own_ref, give_ref, got_ref, s_ref, qs_ref, vs_ref, loss_ref):
    core = lax.axis_index("blk")

    @pl.when(core == ITEM)
    def _():
        vs_ref[...] = own_ref[...]
        qs_ref[...] = query_slope(got_ref[:128], q_ref, v_ref, s_ref)
        loss_ref[0, 0] = jnp.max(give_ref[128:136]) / (128 * 128)

    @pl.when(core != ITEM)
    def _():
        qs_ref[...] = own_ref[...]
        vs_ref[...] = item_slope(got_ref[:128], q_ref, v_ref)
        loss_ref[0, 0] = jnp.max(got_ref[128:136]) / (128 * 128)


def per_device(queries, items):
    rows = (ROWS, D)
    bulk = (GROUP, 2, ROWS, D)
    in_hbm = [pltpu.with_memory_space_constraint(a, pltpu.HBM) for a in (queries, items)]
    mine, pos = call(
        norm_body,
        [(rows, bf16), ((8, 128), f32)],
        "norm",
        10**9,
        ins=[pl.BlockSpec(memory_space=pltpu.HBM)] * 2,
        scratch=[pltpu.VMEM(rows, bf16), pltpu.VMEM(rows, bf16), pltpu.SemaphoreType.DMA((2,))],
    )(*in_hbm)
    (tile,) = call(tile_body, [(bulk, bf16)], "tile")(mine, swap_cores(queries), swap_cores(items))
    block = exchange(tile, BULK)
    flops = 2 * 2048 * 1024 * 256
    cut = (GROUP, ROWS, D)
    (a,) = call(half_body, [(cut, bf16)], "half")(block)
    got_a = swap_cores(a)
    (b,) = call(rest_body, [(cut, bf16)], "rest")(block)
    got_b = swap_cores(b)
    scored = ((4, 256, 1024), bf16)
    v_half = ((4, 2, ROWS, D), bf16)
    e0, q, v0, t = call(
        score0_body, [scored, (cut, bf16), v_half, ((8, GROUP * ROWS), f32)], "score0", flops
    )(block, got_a)
    e1, v1, s = call(
        score1_body, [scored, v_half, ((GROUP, 16, 128), f32)], "score1", flops
    )(block, got_b, q, t, pos)
    sums = exchange(s, QUERY)
    pulled = (GROUP * ROWS, D)
    (give,) = call(first_body, [((1032, D), bf16)], "first", flops)(e0, e1, v0, v1, q, sums)
    got0 = swap_cores(give)
    (give,) = call(second_body, [(pulled, bf16)], "second", flops)(e1, q, sums)
    got1 = swap_cores(give)
    keep, u = call(
        third_body, [((GROUP, 256, D), f32), (pulled, bf16)], "third", flops
    )(e0, e1, v0, v1, q, sums)
    packed = (GROUP, 264, D)
    (part,) = call(merge_body, [(packed, bf16)], "merge", flops)(keep, u, got0, sums)
    (out,) = call(join_body, [(packed, bf16)], "join")(part, keep, got1)
    out = exchange(out, BULK)
    (give,) = call(give_body, [((136, D), f32)], "give")(out)
    got = swap_cores(give)
    (own,) = call(own_body, [(rows, f32)], "own", flops)(out, queries, items, sums)
    q_slope, v_slope, loss = call(
        final_body, [(rows, f32), (rows, f32), ((1, 1), f32, pltpu.SMEM)], "final"
    )(queries, items, own, give, got, sums)
    return loss.reshape(()), q_slope, v_slope


def solution(mesh):
    split = Mesh(mesh.devices.reshape(2, 4, 4, 4), AXES)
    rows = P(AXES, None)
    return jax.shard_map(
        per_device, mesh=split, in_specs=(rows, rows), out_specs=(P(), rows, rows), check_vma=False
    )
```

```python
import math

import jax
import jax.numpy as jnp
from jax import lax
from jax.experimental import pallas as pl
from jax.experimental.pallas import tpu as pltpu
from jax.sharding import Mesh
from jax.sharding import PartitionSpec as P

AXES = ("blk", "z", "y", "x")
GROUP = 8
ROWS, D = 128, 256
ITEM = 1

sharpness = 0.05
tiny_square = 1e-12
log2_e = math.log2(math.e)
f32, bf16 = jnp.float32, jnp.bfloat16


def device_of(core, z, y, x):
    return ((core * 4 + z) * 4 + y) * 4 + x


def query_groups(core):
    return [[device_of(core, z, y, x) for y in pair for x in range(4)] for z in range(4) for pair in ((0, 1), (2, 3))]


def item_groups(core):
    return [[device_of(core, z, y, x) for y in pair for z in range(4)] for x in range(4) for pair in ((1, 2), (3, 0))]


def query_index():
    return lax.axis_index("y") % 2 * 4 + lax.axis_index("x")


BULK = item_groups(ITEM) + query_groups(1 - ITEM)
QUERY = query_groups(0) + query_groups(1)


def exchange(pieces, groups):
    return lax.all_to_all(pieces, AXES, 0, 0, tiled=True, axis_index_groups=groups)


def swap_cores(value):
    return lax.ppermute(value, "blk", [(0, 1), (1, 0)])


def call(body, outs, name, flops=0, ins=None, scratch=()):
    spec = pl.BlockSpec(memory_space=pltpu.VMEM)
    return pl.pallas_call(
        body,
        out_shape=[jax.ShapeDtypeStruct(s, d) for s, d, *_ in outs],
        out_specs=[pl.BlockSpec(memory_space=o[2]) if len(o) > 2 else spec for o in outs],
        **({"in_specs": ins} if ins else {}),
        scratch_shapes=list(scratch),
        compiler_params=pltpu.CompilerParams(vmem_limit_bytes=24 * 2**20),
        cost_estimate=pl.CostEstimate(flops=flops, bytes_accessed=0, transcendentals=0),
        name=name,
    )


def unit(matrix):
    wide = matrix.astype(f32)
    length = jnp.sqrt(jnp.sum(wide * wide, axis=1, keepdims=True) + tiny_square)
    return wide / length, length


def hat(matrix):
    return unit(matrix)[0].astype(bf16)


def norm_body(q_hbm, v_hbm, mine_ref, pos_ref, q_ref, v_ref, sem):
    copies = [
        pltpu.make_async_copy(q_hbm, q_ref, sem.at[0]),
        pltpu.make_async_copy(v_hbm, v_ref, sem.at[1]),
    ]
    for c in copies:
        c.start()
    core = lax.axis_index("blk")
    for c in copies:
        c.wait()
    q, v = hat(q_ref[...]), hat(v_ref[...])
    total = jnp.sum(q.astype(f32) * v.astype(f32)) / sharpness
    pos_ref[...] = jnp.full((8, 128), total, f32)

    @pl.when(core == ITEM)
    def _():
        mine_ref[...] = v

    @pl.when(core != ITEM)
    def _():
        mine_ref[...] = q


def tile_body(mine_ref, got_q_ref, got_v_ref, out_ref):
    core = lax.axis_index("blk")

    def fill(got_ref):
        mine, got = mine_ref[...], hat(got_ref[...])
        for k in range(GROUP):
            out_ref[k, core] = mine
            out_ref[k, 1 - core] = got

    @pl.when(core == ITEM)
    def _():
        fill(got_v_ref)

    @pl.when(core != ITEM)
    def _():
        fill(got_q_ref)


def half_body(block_ref, out_ref):
    core = lax.axis_index("blk")

    @pl.when(core == ITEM)
    def _():
        out_ref[...] = block_ref[:4].reshape(GROUP, ROWS, D)

    @pl.when(core != ITEM)
    def _():
        out_ref[...] = block_ref[:, ITEM]


def rest_body(block_ref, out_ref):
    out_ref[...] = block_ref[4:].reshape(GROUP, ROWS, D)


def by_role(item, query):
    core = lax.axis_index("blk")
    pl.when(core == ITEM)(item)
    pl.when(core != ITEM)(query)


def rows_of(ref):
    return ref[...].reshape(-1, D)


def own_queries(block_ref):
    return block_ref[:, 1 - ITEM].reshape(GROUP * ROWS, D)


def item_parts(block_ref):
    return [lambda k=k: block_ref[k].reshape(2 * ROWS, D) for k in range(GROUP)]


def got_parts(*refs):
    return [lambda ref=ref, k=k: ref[2 * k : 2 * k + 2].reshape(2 * ROWS, D) for ref in refs for k in range(4)]


def scores(parts, q, e_ref):
    total = jnp.zeros((1, GROUP * ROWS), f32)
    for k, part in enumerate(parts):
        t = lax.dot_general(part(), q, (((1,), (1,)), ((), ())), preferred_element_type=f32)
        e = jnp.exp2(t * (log2_e / sharpness))
        total = total + jnp.sum(e, axis=0, keepdims=True)
        e_ref[k] = e.astype(bf16)
    return total


def score0_body(block_ref, got_ref, e_ref, t_ref):
    def item():
        t_ref[:1] = scores(item_parts(block_ref)[:4], rows_of(got_ref), e_ref)

    def query():
        t_ref[:1] = scores(got_parts(got_ref), own_queries(block_ref), e_ref)

    by_role(item, query)


def score1_body(block_ref, got_a_ref, got_b_ref, t_ref, pos_ref, e_ref, s_ref):
    def send(total):
        total = total + t_ref[:1]
        total = jnp.concatenate([total[:, k * ROWS : (k + 1) * ROWS] for k in range(GROUP)], axis=0)
        for j in range(GROUP):
            s_ref[j, :8] = total

    def item():
        send(scores(item_parts(block_ref)[4:], rows_of(got_a_ref), e_ref))

    def query():
        send(scores(got_parts(got_b_ref), own_queries(block_ref), e_ref))

    by_role(item, query)
    for j in range(GROUP):
        s_ref[j, 8:16] = pos_ref[...]


def row_sums(s_ref):
    total = s_ref[0]
    for j in range(1, GROUP):
        total = total + s_ref[j]
    return total


def loss_part(sums, pos):
    return jnp.sum(jnp.log(sums)) - jnp.max(pos[:1])


def split(value):
    high = value.astype(bf16).astype(f32)
    return jnp.concatenate([high, value - high], axis=1).astype(bf16)


def joined(tail):
    tail = tail.astype(f32)
    return tail[:, :128] + tail[:, 128:]


def weigh(e_ref, q, r, store, ks=range(4)):
    for k in ks:
        parts = [
            (e_ref[k, :, j * ROWS : (j + 1) * ROWS].astype(f32) * r[j : j + 1]).astype(bf16)
            for j in range(GROUP)
        ]
        store(k, jnp.dot(jnp.concatenate(parts, axis=1), q, preferred_element_type=f32))


def pull(parts, e_refs, u_ref):
    total = None
    for i in range(0, GROUP, 2):
        v = jnp.concatenate([parts[i](), parts[i + 1]()], axis=0)
        k = i % 4
        e = e_refs[i // 4][k : k + 2].reshape(4 * ROWS, GROUP * ROWS)
        part = lax.dot_general(v, e, (((0,), (0,)), ((), ())), preferred_element_type=f32)
        total = part if total is None else total + part
    for k in range(GROUP):
        rows = slice(k * ROWS, (k + 1) * ROWS)
        u_ref[rows, :ROWS] = total[:ROWS, rows].astype(bf16)
        u_ref[rows, ROWS:] = total[ROWS:, rows].astype(bf16)


def into(ref):
    def store(k, w):
        ref[k * 256 : (k + 1) * 256] = w.astype(bf16)

    return store


def keeping(ref):
    def store(k, w):
        ref[k] = w

    return store


def first_body(e0_ref, e1_ref, block_ref, s_ref, give_ref):
    sums = row_sums(s_ref)
    give_ref[1024:1032] = split(sums[:8])
    give_ref[1032:1040] = split(sums[8:])

    def item():
        pull(item_parts(block_ref), (e0_ref, e1_ref), give_ref)

    def query():
        weigh(e0_ref, own_queries(block_ref), 1.0 / sums[:8], into(give_ref))

    by_role(item, query)


def second_body(e0_ref, e1_ref, block_ref, got_a_ref, s_ref, keep_ref, give_ref):
    r = 1.0 / row_sums(s_ref)[:8]

    def item():
        weigh(e0_ref, rows_of(got_a_ref), r, keeping(keep_ref), range(2))

    def query():
        weigh(e1_ref, own_queries(block_ref), r, into(give_ref))

    by_role(item, query)


def third_body(e0_ref, e1_ref, got_a_ref, got_b_ref, s_ref, keep0_ref, keep1_ref, u_ref):
    def item():
        r, q = 1.0 / row_sums(s_ref)[:8], rows_of(got_a_ref)
        weigh(e0_ref, q, r, lambda k, w: keeping(keep0_ref)(k - 2, w), range(2, 4))
        weigh(e1_ref, q, r, keeping(keep1_ref))

    def query():
        pull(got_parts(got_a_ref, got_b_ref), (e0_ref, e1_ref), u_ref)

    by_role(item, query)


def merge_body(keep0_ref, keep1_ref, u_ref, got_ref, s_ref, out_ref):
    def item():
        for k in range(4):
            keep = keep0_ref[k] if k < 2 else keep1_ref[k - 2]
            got = got_ref[k * 256 : (k + 1) * 256].astype(f32)
            out_ref[k, :256] = (keep + got).astype(bf16)
        sums = row_sums(s_ref)
        loss = loss_part(sums[:8], sums[8:])
        loss = loss + loss_part(joined(got_ref[1024:1032]), joined(got_ref[1032:1040]))
        tail = split(jnp.full((8, 128), loss, f32))
        for k in range(GROUP):
            out_ref[k, 256:264] = tail

    def query():
        for k in range(GROUP):
            rows = slice(k * ROWS, (k + 1) * ROWS)
            out_ref[k, (1 - ITEM) * 128 : (2 - ITEM) * 128] = u_ref[rows]
            out_ref[k, ITEM * 128 : (ITEM + 1) * 128] = got_ref[rows]
            out_ref[k, 256:264] = jnp.zeros((8, D), bf16)

    by_role(item, query)


def join_body(part_ref, keep_ref, got_ref, out_ref):
    out_ref[:4] = part_ref[:4]
    out_ref[4:, 256:264] = part_ref[4:, 256:264]

    def item():
        for k in range(4):
            got = got_ref[k * 256 : (k + 1) * 256].astype(f32)
            out_ref[4 + k, :256] = (keep_ref[k] + got).astype(bf16)

    def query():
        out_ref[4:, :256] = part_ref[4:, :256]

    by_role(item, query)


def summed(w_ref, first, rows):
    at = pl.ds(first, rows)
    total = w_ref[0, at].astype(f32)
    for k in range(1, GROUP):
        total = total + w_ref[k, at].astype(f32)
    return total


def give_body(w_ref, give_ref):
    core = lax.axis_index("blk")
    give_ref[:128] = summed(w_ref, pl.multiple_of((1 - core) * 128, 128), 128)
    give_ref[128:136] = jnp.concatenate([joined(summed(w_ref, 256, 8))] * 2, axis=1)


def slope(pull, hat, direction, length):
    grad = (pull - hat) / sharpness
    along = jnp.sum(direction * grad, axis=1, keepdims=True)
    return (grad - direction * along) / length


def query_slope(u, q_ref, v_ref, s_ref):
    q, q_len = unit(q_ref[...])
    sums = row_sums(s_ref)[:8]
    mine = lax.broadcasted_iota(jnp.int32, sums.shape, 0) == query_index()
    own = jnp.sum(jnp.where(mine, sums, 0.0), axis=0, keepdims=True)
    u = jnp.concatenate([(u[:, :128] / own).T, (u[:, 128:] / own).T], axis=1)
    return slope(u, hat(v_ref[...]).astype(f32), q, q_len)


def item_slope(w, q_ref, v_ref):
    v, v_len = unit(v_ref[...])
    return slope(w, hat(q_ref[...]).astype(f32), v, v_len)


def own_body(w_ref, q_ref, v_ref, s_ref, own_ref):
    core = lax.axis_index("blk")
    own = summed(w_ref, pl.multiple_of(core * 128, 128), 128)

    @pl.when(core == ITEM)
    def _():
        own_ref[...] = item_slope(own, q_ref, v_ref)

    @pl.when(core != ITEM)
    def _():
        own_ref[...] = query_slope(own, q_ref, v_ref, s_ref)


def final_body(q_ref, v_ref, own_ref, give_ref, got_ref, s_ref, qs_ref, vs_ref, loss_ref):
    core = lax.axis_index("blk")

    @pl.when(core == ITEM)
    def _():
        vs_ref[...] = own_ref[...]
        qs_ref[...] = query_slope(got_ref[:128], q_ref, v_ref, s_ref)
        loss_ref[0, 0] = jnp.max(give_ref[128:136]) / (128 * 128)

    @pl.when(core != ITEM)
    def _():
        qs_ref[...] = own_ref[...]
        vs_ref[...] = item_slope(got_ref[:128], q_ref, v_ref)
        loss_ref[0, 0] = jnp.max(got_ref[128:136]) / (128 * 128)


def per_device(queries, items):
    rows = (ROWS, D)
    bulk = (GROUP, 2, ROWS, D)
    in_hbm = [pltpu.with_memory_space_constraint(a, pltpu.HBM) for a in (queries, items)]
    mine, pos = call(
        norm_body,
        [(rows, bf16), ((8, 128), f32)],
        "norm",
        10**9,
        ins=[pl.BlockSpec(memory_space=pltpu.HBM)] * 2,
        scratch=[pltpu.VMEM(rows, bf16), pltpu.VMEM(rows, bf16), pltpu.SemaphoreType.DMA((2,))],
    )(*in_hbm)
    (tile,) = call(tile_body, [(bulk, bf16)], "tile")(mine, swap_cores(queries), swap_cores(items))
    block = exchange(tile, BULK)
    flops = 2 * 2048 * 1024 * 256
    cut = (GROUP, ROWS, D)
    (a,) = call(half_body, [(cut, bf16)], "half")(block)
    got_a = swap_cores(a)
    (b,) = call(rest_body, [(cut, bf16)], "rest")(block)
    got_b = swap_cores(b)
    scored = ((4, 256, 1024), bf16)
    e0, t = call(score0_body, [scored, ((8, GROUP * ROWS), f32)], "score0", flops)(block, got_a)
    e1, s = call(
        score1_body, [scored, ((GROUP, 16, 128), f32)], "score1", flops
    )(block, got_a, got_b, t, pos)
    sums = exchange(s, QUERY)
    pulled = (GROUP * ROWS, D)
    (give,) = call(first_body, [((1040, D), bf16)], "first", flops)(e0, e1, block, sums)
    got0 = swap_cores(give)
    keep0, give = call(
        second_body, [((2, 256, D), f32), (pulled, bf16)], "second", flops
    )(e0, e1, block, got_a, sums)
    got1 = swap_cores(give)
    keep1, keep2, u = call(
        third_body, [((2, 256, D), f32), ((4, 256, D), f32), (pulled, bf16)], "third", flops
    )(e0, e1, got_a, got_b, sums)
    packed = (GROUP, 264, D)
    (part,) = call(merge_body, [(packed, bf16)], "merge", flops)(keep0, keep1, u, got0, sums)
    (out,) = call(join_body, [(packed, bf16)], "join")(part, keep2, got1)
    out = exchange(out, BULK)
    (give,) = call(give_body, [((136, D), f32)], "give")(out)
    got = swap_cores(give)
    (own,) = call(own_body, [(rows, f32)], "own", flops)(out, queries, items, sums)
    q_slope, v_slope, loss = call(
        final_body, [(rows, f32), (rows, f32), ((1, 1), f32, pltpu.SMEM)], "final"
    )(queries, items, own, give, got, sums)
    return loss.reshape(()), q_slope, v_slope


def solution(mesh):
    split = Mesh(mesh.devices.reshape(2, 4, 4, 4), AXES)
    rows = P(AXES, None)
    return jax.shard_map(
        per_device, mesh=split, in_specs=(rows, rows), out_specs=(P(), rows, rows), check_vma=False
    )
```

```python
import math

import jax
import jax.numpy as jnp
from jax import lax
from jax.experimental import pallas as pl
from jax.experimental.pallas import tpu as pltpu
from jax.sharding import Mesh
from jax.sharding import PartitionSpec as P

AXES = ("blk", "z", "y", "x")
GROUP = 8
ROWS, D = 128, 256
ITEM = 1

sharpness = 0.05
tiny_square = 1e-12
log2_e = math.log2(math.e)
f32, bf16 = jnp.float32, jnp.bfloat16


def device_of(core, z, y, x):
    return ((core * 4 + z) * 4 + y) * 4 + x


def query_groups(core):
    return [[device_of(core, z, y, x) for y in pair for x in range(4)] for z in range(4) for pair in ((0, 1), (2, 3))]


def item_groups(core):
    return [[device_of(core, z, y, x) for y in pair for z in range(4)] for x in range(4) for pair in ((1, 2), (3, 0))]


def query_index():
    return lax.axis_index("y") % 2 * 4 + lax.axis_index("x")


BULK = item_groups(ITEM) + query_groups(1 - ITEM)
QUERY = query_groups(0) + query_groups(1)


def exchange(pieces, groups):
    return lax.all_to_all(pieces, AXES, 0, 0, tiled=True, axis_index_groups=groups)


def swap_cores(value):
    return lax.ppermute(value, "blk", [(0, 1), (1, 0)])


def call(body, outs, name, flops=0, ins=None, scratch=()):
    spec = pl.BlockSpec(memory_space=pltpu.VMEM)
    return pl.pallas_call(
        body,
        out_shape=[jax.ShapeDtypeStruct(s, d) for s, d, *_ in outs],
        out_specs=[pl.BlockSpec(memory_space=o[2]) if len(o) > 2 else spec for o in outs],
        **({"in_specs": ins} if ins else {}),
        scratch_shapes=list(scratch),
        compiler_params=pltpu.CompilerParams(vmem_limit_bytes=24 * 2**20),
        cost_estimate=pl.CostEstimate(flops=flops, bytes_accessed=0, transcendentals=0),
        name=name,
    )


def unit(matrix):
    wide = matrix.astype(f32)
    length = jnp.sqrt(jnp.sum(wide * wide, axis=1, keepdims=True) + tiny_square)
    return wide / length, length


def hat(matrix):
    return unit(matrix)[0].astype(bf16)


def norm_body(q_hbm, v_hbm, mine_ref, pos_ref, q_ref, v_ref, sem):
    copies = [
        pltpu.make_async_copy(q_hbm, q_ref, sem.at[0]),
        pltpu.make_async_copy(v_hbm, v_ref, sem.at[1]),
    ]
    for c in copies:
        c.start()
    core = lax.axis_index("blk")
    for c in copies:
        c.wait()
    q, v = hat(q_ref[...]), hat(v_ref[...])
    total = jnp.sum(q.astype(f32) * v.astype(f32)) / sharpness
    pos_ref[...] = jnp.full((8, 128), total, f32)

    @pl.when(core == ITEM)
    def _():
        mine_ref[...] = v

    @pl.when(core != ITEM)
    def _():
        mine_ref[...] = q


def tile_body(mine_ref, got_q_ref, got_v_ref, out_ref):
    core = lax.axis_index("blk")

    def fill(got_ref):
        mine, got = mine_ref[...], hat(got_ref[...])
        for k in range(GROUP):
            out_ref[k, core] = mine
            out_ref[k, 1 - core] = got

    @pl.when(core == ITEM)
    def _():
        fill(got_v_ref)

    @pl.when(core != ITEM)
    def _():
        fill(got_q_ref)


def half_body(block_ref, out_ref):
    core = lax.axis_index("blk")

    @pl.when(core == ITEM)
    def _():
        out_ref[...] = block_ref[:4].reshape(GROUP, ROWS, D)

    @pl.when(core != ITEM)
    def _():
        out_ref[...] = block_ref[:, ITEM]


def rest_body(block_ref, out_ref):
    out_ref[...] = block_ref[4:].reshape(GROUP, ROWS, D)


def by_role(item, query):
    core = lax.axis_index("blk")
    pl.when(core == ITEM)(item)
    pl.when(core != ITEM)(query)


def rows_of(ref):
    return ref[...].reshape(-1, D)


def own_queries(block_ref):
    return block_ref[:, 1 - ITEM].reshape(GROUP * ROWS, D)


def item_parts(block_ref):
    return [lambda k=k: block_ref[k].reshape(2 * ROWS, D) for k in range(GROUP)]


def got_parts(*refs):
    return [lambda ref=ref, k=k: ref[2 * k : 2 * k + 2].reshape(2 * ROWS, D) for ref in refs for k in range(4)]


def scores(parts, q, e_ref):
    total = jnp.zeros((1, GROUP * ROWS), f32)
    for k, part in enumerate(parts):
        t = lax.dot_general(part(), q, (((1,), (1,)), ((), ())), preferred_element_type=f32)
        e = jnp.exp2(t * (log2_e / sharpness))
        total = total + jnp.sum(e, axis=0, keepdims=True)
        e_ref[k] = e.astype(bf16)
    return total


def score0_body(block_ref, got_ref, e_ref, t_ref):
    def item():
        t_ref[:1] = scores(item_parts(block_ref)[:4], rows_of(got_ref), e_ref)

    def query():
        t_ref[:1] = scores(got_parts(got_ref), own_queries(block_ref), e_ref)

    by_role(item, query)


def score1_body(block_ref, got_a_ref, got_b_ref, t_ref, pos_ref, e_ref, s_ref):
    def send(total):
        total = total + t_ref[:1]
        total = jnp.concatenate([total[:, k * ROWS : (k + 1) * ROWS] for k in range(GROUP)], axis=0)
        for j in range(GROUP):
            s_ref[j, :8] = total

    def item():
        send(scores(item_parts(block_ref)[4:], rows_of(got_a_ref), e_ref))

    def query():
        send(scores(got_parts(got_b_ref), own_queries(block_ref), e_ref))

    by_role(item, query)
    for j in range(GROUP):
        s_ref[j, 8:16] = pos_ref[...]


def row_sums(s_ref):
    total = s_ref[0]
    for j in range(1, GROUP):
        total = total + s_ref[j]
    return total


def loss_part(sums, pos):
    return jnp.sum(jnp.log(sums)) - jnp.max(pos[:1])


def split(value):
    high = value.astype(bf16).astype(f32)
    return jnp.concatenate([high, value - high], axis=1).astype(bf16)


def joined(tail):
    tail = tail.astype(f32)
    return tail[:, :128] + tail[:, 128:]


def weigh(e_ref, q, r, store, ks=range(4)):
    for k in ks:
        parts = [
            (e_ref[k, :, j * ROWS : (j + 1) * ROWS].astype(f32) * r[j : j + 1]).astype(bf16)
            for j in range(GROUP)
        ]
        store(k, jnp.dot(jnp.concatenate(parts, axis=1), q, preferred_element_type=f32))


def pull(parts, e_refs, u_ref):
    total = None
    for i in range(0, GROUP, 2):
        v = jnp.concatenate([parts[i](), parts[i + 1]()], axis=0)
        k = i % 4
        e = e_refs[i // 4][k : k + 2].reshape(4 * ROWS, GROUP * ROWS)
        part = lax.dot_general(v, e, (((0,), (0,)), ((), ())), preferred_element_type=f32)
        total = part if total is None else total + part
    for k in range(GROUP):
        rows = slice(k * ROWS, (k + 1) * ROWS)
        u_ref[rows, :ROWS] = total[:ROWS, rows].astype(bf16)
        u_ref[rows, ROWS:] = total[ROWS:, rows].astype(bf16)


def into(ref):
    def store(k, w):
        ref[k * 256 : (k + 1) * 256] = w.astype(bf16)

    return store


def keeping(ref):
    def store(k, w):
        ref[k] = w

    return store


def first_body(e0_ref, e1_ref, block_ref, s_ref, give_ref):
    sums = row_sums(s_ref)
    give_ref[1024:1032] = split(sums[:8])
    give_ref[1032:1040] = split(sums[8:])

    def item():
        pull(item_parts(block_ref), (e0_ref, e1_ref), give_ref)

    def query():
        weigh(e0_ref, own_queries(block_ref), 1.0 / sums[:8], into(give_ref))

    by_role(item, query)


def second_body(e0_ref, e1_ref, block_ref, got_a_ref, s_ref, keep_ref, give_ref):
    r = 1.0 / row_sums(s_ref)[:8]

    def item():
        weigh(e0_ref, rows_of(got_a_ref), r, keeping(keep_ref), range(2))

    def query():
        weigh(e1_ref, own_queries(block_ref), r, into(give_ref))

    by_role(item, query)


def third_body(e0_ref, e1_ref, got_a_ref, got_b_ref, s_ref, keep0_ref, keep1_ref, u_ref):
    def item():
        r, q = 1.0 / row_sums(s_ref)[:8], rows_of(got_a_ref)
        weigh(e0_ref, q, r, lambda k, w: keeping(keep0_ref)(k - 2, w), range(2, 4))
        weigh(e1_ref, q, r, keeping(keep1_ref))

    def query():
        pull(got_parts(got_a_ref, got_b_ref), (e0_ref, e1_ref), u_ref)

    by_role(item, query)


def merge_body(keep0_ref, keep1_ref, u_ref, got_ref, s_ref, out_ref):
    def item():
        for k in range(4):
            keep = keep0_ref[k] if k < 2 else keep1_ref[k - 2]
            got = got_ref[k * 256 : (k + 1) * 256].astype(f32)
            out_ref[k, :256] = (keep + got).astype(bf16)
        sums = row_sums(s_ref)
        loss = loss_part(sums[:8], sums[8:])
        loss = loss + loss_part(joined(got_ref[1024:1032]), joined(got_ref[1032:1040]))
        tail = split(jnp.full((8, 128), loss, f32))
        for k in range(GROUP):
            out_ref[k, 256:264] = tail

    def query():
        for k in range(GROUP):
            rows = slice(k * ROWS, (k + 1) * ROWS)
            out_ref[k, (1 - ITEM) * 128 : (2 - ITEM) * 128] = u_ref[rows]
            out_ref[k, ITEM * 128 : (ITEM + 1) * 128] = got_ref[rows]
            out_ref[k, 256:264] = jnp.zeros((8, D), bf16)

    by_role(item, query)


def join_body(part_ref, keep_ref, got_ref, out_ref):
    out_ref[:4] = part_ref[:4]
    out_ref[4:, 256:264] = part_ref[4:, 256:264]

    def item():
        for k in range(4):
            got = got_ref[k * 256 : (k + 1) * 256].astype(f32)
            out_ref[4 + k, :256] = (keep_ref[k] + got).astype(bf16)

    def query():
        out_ref[4:, :256] = part_ref[4:, :256]

    by_role(item, query)


def summed(w_ref, first, rows):
    at = pl.ds(first, rows)
    total = w_ref[0, at].astype(f32)
    for k in range(1, GROUP):
        total = total + w_ref[k, at].astype(f32)
    return total


def give_body(w_ref, give_ref):
    core = lax.axis_index("blk")
    give_ref[:128] = summed(w_ref, pl.multiple_of((1 - core) * 128, 128), 128)
    give_ref[128:136] = jnp.concatenate([joined(summed(w_ref, 256, 8))] * 2, axis=1)


def slope(pull, hat, direction, length):
    grad = (pull - hat) / sharpness
    along = jnp.sum(direction * grad, axis=1, keepdims=True)
    return (grad - direction * along) / length


def query_slope(u, q_ref, v_ref, s_ref):
    q, q_len = unit(q_ref[...])
    sums = row_sums(s_ref)[:8]
    mine = lax.broadcasted_iota(jnp.int32, sums.shape, 0) == query_index()
    own = jnp.sum(jnp.where(mine, sums, 0.0), axis=0, keepdims=True)
    u = jnp.concatenate([(u[:, :128] / own).T, (u[:, 128:] / own).T], axis=1)
    return slope(u, hat(v_ref[...]).astype(f32), q, q_len)


def item_slope(w, q_ref, v_ref):
    v, v_len = unit(v_ref[...])
    return slope(w, hat(q_ref[...]).astype(f32), v, v_len)


def own_body(w_ref, q_ref, v_ref, s_ref, own_ref):
    core = lax.axis_index("blk")
    own = summed(w_ref, pl.multiple_of(core * 128, 128), 128)

    @pl.when(core == ITEM)
    def _():
        own_ref[...] = item_slope(own, q_ref, v_ref)

    @pl.when(core != ITEM)
    def _():
        own_ref[...] = query_slope(own, q_ref, v_ref, s_ref)


def final_body(q_ref, v_ref, own_ref, give_ref, got_ref, s_ref, qs_hbm, vs_hbm, loss_ref, new_ref, sem):
    def finish(own_hbm, other_hbm, other, total):
        first = pltpu.make_async_copy(own_ref, own_hbm, sem.at[0])
        first.start()
        new_ref[...] = other()
        second = pltpu.make_async_copy(new_ref, other_hbm, sem.at[1])
        second.start()
        loss_ref[0, 0] = jnp.max(total[128:136]) / (128 * 128)
        first.wait()
        second.wait()

    def item():
        finish(vs_hbm, qs_hbm, lambda: query_slope(got_ref[:128], q_ref, v_ref, s_ref), give_ref)

    def query():
        finish(qs_hbm, vs_hbm, lambda: item_slope(got_ref[:128], q_ref, v_ref), got_ref)

    by_role(item, query)


def per_device(queries, items):
    rows = (ROWS, D)
    bulk = (GROUP, 2, ROWS, D)
    in_hbm = [pltpu.with_memory_space_constraint(a, pltpu.HBM) for a in (queries, items)]
    mine, pos, q_raw, v_raw = call(
        norm_body,
        [(rows, bf16), ((8, 128), f32), (rows, bf16), (rows, bf16)],
        "norm",
        10**9,
        ins=[pl.BlockSpec(memory_space=pltpu.HBM)] * 2,
        scratch=[pltpu.SemaphoreType.DMA((2,))],
    )(*in_hbm)
    (tile,) = call(tile_body, [(bulk, bf16)], "tile")(mine, swap_cores(queries), swap_cores(items))
    block = exchange(tile, BULK)
    flops = 2 * 2048 * 1024 * 256
    cut = (GROUP, ROWS, D)
    (a,) = call(half_body, [(cut, bf16)], "half")(block)
    got_a = swap_cores(a)
    (b,) = call(rest_body, [(cut, bf16)], "rest")(block)
    got_b = swap_cores(b)
    scored = ((4, 256, 1024), bf16)
    e0, t = call(score0_body, [scored, ((8, GROUP * ROWS), f32)], "score0", flops)(block, got_a)
    e1, s = call(
        score1_body, [scored, ((GROUP, 16, 128), f32)], "score1", flops
    )(block, got_a, got_b, t, pos)
    sums = exchange(s, QUERY)
    pulled = (GROUP * ROWS, D)
    (give,) = call(first_body, [((1040, D), bf16)], "first", flops)(e0, e1, block, sums)
    got0 = swap_cores(give)
    keep0, give = call(
        second_body, [((2, 256, D), f32), (pulled, bf16)], "second", flops
    )(e0, e1, block, got_a, sums)
    got1 = swap_cores(give)
    keep1, keep2, u = call(
        third_body, [((2, 256, D), f32), ((4, 256, D), f32), (pulled, bf16)], "third", flops
    )(e0, e1, got_a, got_b, sums)
    packed = (GROUP, 264, D)
    (part,) = call(merge_body, [(packed, bf16)], "merge", flops)(keep0, keep1, u, got0, sums)
    (out,) = call(join_body, [(packed, bf16)], "join")(part, keep2, got1)
    out = exchange(out, BULK)
    (give,) = call(give_body, [((136, D), f32)], "give")(out)
    got = swap_cores(give)
    (own,) = call(own_body, [(rows, f32)], "own", flops)(out, q_raw, v_raw, sums)
    q_slope, v_slope, loss = call(
        final_body,
        [(rows, f32, pltpu.HBM), (rows, f32, pltpu.HBM), ((1, 1), f32, pltpu.SMEM)],
        "final",
        scratch=[pltpu.VMEM(rows, f32), pltpu.SemaphoreType.DMA((2,))],
    )(q_raw, v_raw, own, give, got, sums)
    return loss.reshape(()), q_slope, v_slope


def solution(mesh):
    split = Mesh(mesh.devices.reshape(2, 4, 4, 4), AXES)
    rows = P(AXES, None)
    return jax.shard_map(
        per_device, mesh=split, in_specs=(rows, rows), out_specs=(P(), rows, rows), check_vma=False
    )
```

```python
import math

import jax
import jax.numpy as jnp
from jax import lax
from jax.experimental import pallas as pl
from jax.experimental.pallas import tpu as pltpu
from jax.sharding import Mesh
from jax.sharding import PartitionSpec as P

AXES = ("blk", "z", "y", "x")
GROUP = 8
ROWS, D = 128, 256
ITEM = 1
RING_Q, RING_V, PAIR = "z", "y", "x"
NEAR, CROSS = ((0, 1), (2, 3)), ((1, 2), (3, 0))

sharpness = 0.05
tiny_square = 1e-12
log2_e = math.log2(math.e)
f32, bf16 = jnp.float32, jnp.bfloat16


def groups(core, ring, pairs, fixed, order):
    def device(at):
        return ((core * 4 + at["z"]) * 4 + at["y"]) * 4 + at["x"]

    return [
        [device({fixed: f, PAIR: p, ring: r}) for p in pair for r in order] for f in range(4) for pair in pairs
    ]


def query_groups(core, order):
    return groups(core, RING_Q, NEAR, RING_V, order)


def item_groups(core, order):
    return groups(core, RING_V, CROSS, RING_Q, order)


def query_index():
    return lax.axis_index(PAIR) % 2 * 4 + 3 - lax.axis_index(RING_Q)


BULK = item_groups(ITEM, (2, 1, 0, 3)) + query_groups(1 - ITEM, (3, 2, 1, 0))
QUERY = query_groups(0, (3, 1, 0, 2)) + query_groups(1, (3, 1, 0, 2))


def exchange(pieces, groups):
    return lax.all_to_all(pieces, AXES, 0, 0, tiled=True, axis_index_groups=groups)


def swap_cores(value):
    return lax.ppermute(value, "blk", [(0, 1), (1, 0)])


def call(body, outs, name, flops=0, ins=None, scratch=()):
    spec = pl.BlockSpec(memory_space=pltpu.VMEM)
    return pl.pallas_call(
        body,
        out_shape=[jax.ShapeDtypeStruct(s, d) for s, d, *_ in outs],
        out_specs=[pl.BlockSpec(memory_space=o[2]) if len(o) > 2 else spec for o in outs],
        **({"in_specs": ins} if ins else {}),
        scratch_shapes=list(scratch),
        compiler_params=pltpu.CompilerParams(vmem_limit_bytes=24 * 2**20),
        cost_estimate=pl.CostEstimate(flops=flops, bytes_accessed=0, transcendentals=0),
        name=name,
    )


def unit(matrix):
    wide = matrix.astype(f32)
    length = jnp.sqrt(jnp.sum(wide * wide, axis=1, keepdims=True) + tiny_square)
    return wide / length, length


def hat(matrix):
    return unit(matrix)[0].astype(bf16)


def norm_body(q_hbm, v_hbm, mine_ref, pos_ref, q_ref, v_ref, sem):
    copies = [
        pltpu.make_async_copy(q_hbm, q_ref, sem.at[0]),
        pltpu.make_async_copy(v_hbm, v_ref, sem.at[1]),
    ]
    for c in copies:
        c.start()
    core = lax.axis_index("blk")
    for c in copies:
        c.wait()
    q, v = hat(q_ref[...]), hat(v_ref[...])
    total = jnp.sum(q.astype(f32) * v.astype(f32)) / sharpness
    pos_ref[...] = jnp.full((8, 128), total, f32)

    @pl.when(core == ITEM)
    def _():
        mine_ref[...] = v

    @pl.when(core != ITEM)
    def _():
        mine_ref[...] = q


def tile_body(mine_ref, got_q_ref, got_v_ref, out_ref):
    core = lax.axis_index("blk")

    def fill(got_ref):
        mine, got = mine_ref[...], hat(got_ref[...])
        for k in range(GROUP):
            out_ref[k, core] = mine
            out_ref[k, 1 - core] = got

    @pl.when(core == ITEM)
    def _():
        fill(got_v_ref)

    @pl.when(core != ITEM)
    def _():
        fill(got_q_ref)


def half_body(block_ref, out_ref):
    core = lax.axis_index("blk")

    @pl.when(core == ITEM)
    def _():
        out_ref[...] = block_ref[:4].reshape(GROUP, ROWS, D)

    @pl.when(core != ITEM)
    def _():
        out_ref[...] = block_ref[:, ITEM]


def rest_body(block_ref, out_ref):
    out_ref[...] = block_ref[4:].reshape(GROUP, ROWS, D)


def by_role(item, query):
    core = lax.axis_index("blk")
    pl.when(core == ITEM)(item)
    pl.when(core != ITEM)(query)


def rows_of(ref):
    return ref[...].reshape(-1, D)


def own_queries(block_ref):
    return block_ref[:, 1 - ITEM].reshape(GROUP * ROWS, D)


def item_parts(block_ref):
    return [lambda k=k: block_ref[k].reshape(2 * ROWS, D) for k in range(GROUP)]


def got_parts(*refs):
    return [lambda ref=ref, k=k: ref[2 * k : 2 * k + 2].reshape(2 * ROWS, D) for ref in refs for k in range(4)]


def scores(parts, q, e_ref):
    total = jnp.zeros((1, GROUP * ROWS), f32)
    for k, part in enumerate(parts):
        t = lax.dot_general(part(), q, (((1,), (1,)), ((), ())), preferred_element_type=f32)
        e = jnp.exp2(t * (log2_e / sharpness))
        total = total + jnp.sum(e, axis=0, keepdims=True)
        e_ref[k] = e.astype(bf16)
    return total


def score0_body(block_ref, got_ref, e_ref, t_ref):
    def item():
        t_ref[:1] = scores(item_parts(block_ref)[:4], rows_of(got_ref), e_ref)

    def query():
        t_ref[:1] = scores(got_parts(got_ref), own_queries(block_ref), e_ref)

    by_role(item, query)


def score1_body(block_ref, got_a_ref, got_b_ref, t_ref, pos_ref, e_ref, s_ref):
    def send(total):
        total = total + t_ref[:1]
        total = jnp.concatenate([total[:, k * ROWS : (k + 1) * ROWS] for k in range(GROUP)], axis=0)
        for j in range(GROUP):
            s_ref[j, :8] = total

    def item():
        send(scores(item_parts(block_ref)[4:], rows_of(got_a_ref), e_ref))

    def query():
        send(scores(got_parts(got_b_ref), own_queries(block_ref), e_ref))

    by_role(item, query)
    for j in range(GROUP):
        s_ref[j, 8:16] = pos_ref[...]


def row_sums(s_ref):
    total = s_ref[0]
    for j in range(1, GROUP):
        total = total + s_ref[j]
    return total


def loss_part(sums, pos):
    return jnp.sum(jnp.log(sums)) - jnp.max(pos[:1])


def split(value):
    high = value.astype(bf16).astype(f32)
    return jnp.concatenate([high, value - high], axis=1).astype(bf16)


def joined(tail):
    tail = tail.astype(f32)
    return tail[:, :128] + tail[:, 128:]


def weigh(e_ref, q, r, store, ks=range(4)):
    for k in ks:
        parts = [
            (e_ref[k, :, j * ROWS : (j + 1) * ROWS].astype(f32) * r[j : j + 1]).astype(bf16)
            for j in range(GROUP)
        ]
        store(k, jnp.dot(jnp.concatenate(parts, axis=1), q, preferred_element_type=f32))


def pull(parts, e_refs, u_ref):
    total = None
    for i in range(0, GROUP, 2):
        v = jnp.concatenate([parts[i](), parts[i + 1]()], axis=0)
        k = i % 4
        e = e_refs[i // 4][k : k + 2].reshape(4 * ROWS, GROUP * ROWS)
        part = lax.dot_general(v, e, (((0,), (0,)), ((), ())), preferred_element_type=f32)
        total = part if total is None else total + part
    for k in range(GROUP):
        rows = slice(k * ROWS, (k + 1) * ROWS)
        u_ref[rows, :ROWS] = total[:ROWS, rows].astype(bf16)
        u_ref[rows, ROWS:] = total[ROWS:, rows].astype(bf16)


def into(ref):
    def store(k, w):
        ref[k * 256 : (k + 1) * 256] = w.astype(bf16)

    return store


def keeping(ref):
    def store(k, w):
        ref[k] = w

    return store


def first_body(e0_ref, e1_ref, block_ref, s_ref, give_ref):
    sums = row_sums(s_ref)
    give_ref[1024:1032] = split(sums[:8])
    give_ref[1032:1040] = split(sums[8:])

    def item():
        pull(item_parts(block_ref), (e0_ref, e1_ref), give_ref)

    def query():
        weigh(e0_ref, own_queries(block_ref), 1.0 / sums[:8], into(give_ref))

    by_role(item, query)


def second_body(e0_ref, e1_ref, block_ref, got_a_ref, s_ref, keep_ref, give_ref):
    r = 1.0 / row_sums(s_ref)[:8]

    def item():
        weigh(e0_ref, rows_of(got_a_ref), r, keeping(keep_ref), range(2))

    def query():
        weigh(e1_ref, own_queries(block_ref), r, into(give_ref))

    by_role(item, query)


def third_body(e0_ref, e1_ref, got_a_ref, got_b_ref, s_ref, keep0_ref, keep1_ref, u_ref):
    def item():
        r, q = 1.0 / row_sums(s_ref)[:8], rows_of(got_a_ref)
        weigh(e0_ref, q, r, lambda k, w: keeping(keep0_ref)(k - 2, w), range(2, 4))
        weigh(e1_ref, q, r, keeping(keep1_ref))

    def query():
        pull(got_parts(got_a_ref, got_b_ref), (e0_ref, e1_ref), u_ref)

    by_role(item, query)


def merge_body(keep0_ref, keep1_ref, u_ref, got_ref, s_ref, out_ref):
    def item():
        for k in range(4):
            keep = keep0_ref[k] if k < 2 else keep1_ref[k - 2]
            got = got_ref[k * 256 : (k + 1) * 256].astype(f32)
            out_ref[k, :256] = (keep + got).astype(bf16)
        sums = row_sums(s_ref)
        loss = loss_part(sums[:8], sums[8:])
        loss = loss + loss_part(joined(got_ref[1024:1032]), joined(got_ref[1032:1040]))
        tail = split(jnp.full((8, 128), loss, f32))
        for k in range(GROUP):
            out_ref[k, 256:264] = tail

    def query():
        for k in range(GROUP):
            rows = slice(k * ROWS, (k + 1) * ROWS)
            out_ref[k, (1 - ITEM) * 128 : (2 - ITEM) * 128] = u_ref[rows]
            out_ref[k, ITEM * 128 : (ITEM + 1) * 128] = got_ref[rows]
            out_ref[k, 256:264] = jnp.zeros((8, D), bf16)

    by_role(item, query)


def join_body(part_ref, keep_ref, got_ref, out_ref):
    out_ref[:4] = part_ref[:4]
    out_ref[4:, 256:264] = part_ref[4:, 256:264]

    def item():
        for k in range(4):
            got = got_ref[k * 256 : (k + 1) * 256].astype(f32)
            out_ref[4 + k, :256] = (keep_ref[k] + got).astype(bf16)

    def query():
        out_ref[4:, :256] = part_ref[4:, :256]

    by_role(item, query)


def summed(w_ref, first, rows):
    at = pl.ds(first, rows)
    total = w_ref[0, at].astype(f32)
    for k in range(1, GROUP):
        total = total + w_ref[k, at].astype(f32)
    return total


def give_body(w_ref, give_ref):
    core = lax.axis_index("blk")
    give_ref[:128] = summed(w_ref, pl.multiple_of((1 - core) * 128, 128), 128)
    give_ref[128:136] = jnp.concatenate([joined(summed(w_ref, 256, 8))] * 2, axis=1)


def slope(pull, hat, direction, length):
    grad = (pull - hat) / sharpness
    along = jnp.sum(direction * grad, axis=1, keepdims=True)
    return (grad - direction * along) / length


def query_slope(u, q_ref, v_ref, s_ref):
    q, q_len = unit(q_ref[...])
    sums = row_sums(s_ref)[:8]
    mine = lax.broadcasted_iota(jnp.int32, sums.shape, 0) == query_index()
    own = jnp.sum(jnp.where(mine, sums, 0.0), axis=0, keepdims=True)
    u = jnp.concatenate([(u[:, :128] / own).T, (u[:, 128:] / own).T], axis=1)
    return slope(u, hat(v_ref[...]).astype(f32), q, q_len)


def item_slope(w, q_ref, v_ref):
    v, v_len = unit(v_ref[...])
    return slope(w, hat(q_ref[...]).astype(f32), v, v_len)


def own_body(w_ref, q_ref, v_ref, s_ref, own_ref):
    core = lax.axis_index("blk")
    own = summed(w_ref, pl.multiple_of(core * 128, 128), 128)

    @pl.when(core == ITEM)
    def _():
        own_ref[...] = item_slope(own, q_ref, v_ref)

    @pl.when(core != ITEM)
    def _():
        own_ref[...] = query_slope(own, q_ref, v_ref, s_ref)


def final_body(q_ref, v_ref, own_ref, give_ref, got_ref, s_ref, qs_ref, vs_ref, loss_ref):
    core = lax.axis_index("blk")

    @pl.when(core == ITEM)
    def _():
        vs_ref[...] = own_ref[...]
        qs_ref[...] = query_slope(got_ref[:128], q_ref, v_ref, s_ref)
        loss_ref[0, 0] = jnp.max(give_ref[128:136]) / (128 * 128)

    @pl.when(core != ITEM)
    def _():
        qs_ref[...] = own_ref[...]
        vs_ref[...] = item_slope(got_ref[:128], q_ref, v_ref)
        loss_ref[0, 0] = jnp.max(got_ref[128:136]) / (128 * 128)


def per_device(queries, items):
    rows = (ROWS, D)
    bulk = (GROUP, 2, ROWS, D)
    in_hbm = [pltpu.with_memory_space_constraint(a, pltpu.HBM) for a in (queries, items)]
    mine, pos, q_raw, v_raw = call(
        norm_body,
        [(rows, bf16), ((8, 128), f32), (rows, bf16), (rows, bf16)],
        "norm",
        10**9,
        ins=[pl.BlockSpec(memory_space=pltpu.HBM)] * 2,
        scratch=[pltpu.SemaphoreType.DMA((2,))],
    )(*in_hbm)
    (tile,) = call(tile_body, [(bulk, bf16)], "tile")(mine, swap_cores(queries), swap_cores(items))
    block = exchange(tile, BULK)
    flops = 2 * 2048 * 1024 * 256
    cut = (GROUP, ROWS, D)
    (a,) = call(half_body, [(cut, bf16)], "half")(block)
    got_a = swap_cores(a)
    (b,) = call(rest_body, [(cut, bf16)], "rest")(block)
    got_b = swap_cores(b)
    scored = ((4, 256, 1024), bf16)
    e0, t = call(score0_body, [scored, ((8, GROUP * ROWS), f32)], "score0", flops)(block, got_a)
    e1, s = call(
        score1_body, [scored, ((GROUP, 16, 128), f32)], "score1", flops
    )(block, got_a, got_b, t, pos)
    sums = exchange(s, QUERY)
    pulled = (GROUP * ROWS, D)
    (give,) = call(first_body, [((1040, D), bf16)], "first", flops)(e0, e1, block, sums)
    got0 = swap_cores(give)
    keep0, give = call(
        second_body, [((2, 256, D), f32), (pulled, bf16)], "second", flops
    )(e0, e1, block, got_a, sums)
    got1 = swap_cores(give)
    keep1, keep2, u = call(
        third_body, [((2, 256, D), f32), ((4, 256, D), f32), (pulled, bf16)], "third", flops
    )(e0, e1, got_a, got_b, sums)
    packed = (GROUP, 264, D)
    (part,) = call(merge_body, [(packed, bf16)], "merge", flops)(keep0, keep1, u, got0, sums)
    (out,) = call(join_body, [(packed, bf16)], "join")(part, keep2, got1)
    out = exchange(out, BULK)
    (give,) = call(give_body, [((136, D), f32)], "give")(out)
    got = swap_cores(give)
    (own,) = call(own_body, [(rows, f32)], "own", flops)(out, q_raw, v_raw, sums)
    q_slope, v_slope, loss = call(
        final_body, [(rows, f32), (rows, f32), ((1, 1), f32, pltpu.SMEM)], "final"
    )(q_raw, v_raw, own, give, got, sums)
    return loss.reshape(()), q_slope, v_slope


def solution(mesh):
    split = Mesh(mesh.devices.reshape(2, 4, 4, 4), AXES)
    rows = P(AXES, None)
    return jax.shard_map(
        per_device, mesh=split, in_specs=(rows, rows), out_specs=(P(), rows, rows), check_vma=False
    )
```

```python
import math

import jax
import jax.numpy as jnp
from jax import lax
from jax.experimental import pallas as pl
from jax.experimental.pallas import tpu as pltpu
from jax.sharding import Mesh
from jax.sharding import PartitionSpec as P

AXES = ("blk", "z", "y", "x")
GROUP = 8
ROWS, D = 128, 256
ITEM = 1
RING_Q, RING_V, PAIR = "z", "y", "x"
NEAR, CROSS = ((0, 1), (2, 3)), ((1, 2), (3, 0))

sharpness = 0.05
tiny_square = 1e-12
log2_e = math.log2(math.e)
f32, bf16 = jnp.float32, jnp.bfloat16


ITEM_ORDER = ((7, 1, 0, 2, 6, 5, 4, 3), (2, 1, 0, 3, 4, 5, 6, 7))
QUERY_ORDER = ((3, 2, 7, 0, 1, 6, 5, 4), (3, 4, 1, 0, 7, 6, 5, 2))
SUM_ORDER = ((3, 1, 0, 2, 7, 5, 4, 6),) * 2


def groups(core, ring, pairs, fixed, orders):
    def device(at):
        return ((core * 4 + at["z"]) * 4 + at["y"]) * 4 + at["x"]

    return [
        [device({fixed: f, PAIR: pair[m // 4], ring: m % 4}) for m in order]
        for f in range(4)
        for pair, order in zip(pairs, orders)
    ]


def query_groups(core, orders):
    return groups(core, RING_Q, NEAR, RING_V, orders)


def item_groups(core, orders):
    return groups(core, RING_V, CROSS, RING_Q, orders)


def query_index():
    at = lax.axis_index(PAIR)
    member = at % 2 * 4 + lax.axis_index(RING_Q)
    index = jnp.int32(0)
    for k, (m0, m1) in enumerate(zip(*QUERY_ORDER)):
        index = jnp.where(member == jnp.where(at < 2, m0, m1), k, index)
    return index


BULK = item_groups(ITEM, ITEM_ORDER) + query_groups(1 - ITEM, QUERY_ORDER)
QUERY = query_groups(0, SUM_ORDER) + query_groups(1, SUM_ORDER)


def exchange(pieces, groups):
    return lax.all_to_all(pieces, AXES, 0, 0, tiled=True, axis_index_groups=groups)


def swap_cores(value):
    return lax.ppermute(value, "blk", [(0, 1), (1, 0)])


def call(body, outs, name, flops=0, ins=None, scratch=()):
    spec = pl.BlockSpec(memory_space=pltpu.VMEM)
    return pl.pallas_call(
        body,
        out_shape=[jax.ShapeDtypeStruct(s, d) for s, d, *_ in outs],
        out_specs=[pl.BlockSpec(memory_space=o[2]) if len(o) > 2 else spec for o in outs],
        **({"in_specs": ins} if ins else {}),
        scratch_shapes=list(scratch),
        compiler_params=pltpu.CompilerParams(vmem_limit_bytes=24 * 2**20),
        cost_estimate=pl.CostEstimate(flops=flops, bytes_accessed=0, transcendentals=0),
        name=name,
    )


def unit(matrix):
    wide = matrix.astype(f32)
    length = jnp.sqrt(jnp.sum(wide * wide, axis=1, keepdims=True) + tiny_square)
    return wide / length, length


def hat(matrix):
    return unit(matrix)[0].astype(bf16)


def norm_body(q_hbm, v_hbm, mine_ref, pos_ref, q_ref, v_ref, sem):
    copies = [
        pltpu.make_async_copy(q_hbm, q_ref, sem.at[0]),
        pltpu.make_async_copy(v_hbm, v_ref, sem.at[1]),
    ]
    for c in copies:
        c.start()
    core = lax.axis_index("blk")
    for c in copies:
        c.wait()
    q, v = hat(q_ref[...]), hat(v_ref[...])
    total = jnp.sum(q.astype(f32) * v.astype(f32)) / sharpness
    pos_ref[...] = jnp.full((8, 128), total, f32)

    @pl.when(core == ITEM)
    def _():
        mine_ref[...] = v

    @pl.when(core != ITEM)
    def _():
        mine_ref[...] = q


def tile_body(mine_ref, got_q_ref, got_v_ref, out_ref):
    core = lax.axis_index("blk")

    def fill(got_ref):
        mine, got = mine_ref[...], hat(got_ref[...])
        for k in range(GROUP):
            out_ref[k, core] = mine
            out_ref[k, 1 - core] = got

    @pl.when(core == ITEM)
    def _():
        fill(got_v_ref)

    @pl.when(core != ITEM)
    def _():
        fill(got_q_ref)


def half_body(block_ref, out_ref):
    core = lax.axis_index("blk")

    @pl.when(core == ITEM)
    def _():
        out_ref[...] = block_ref[:4].reshape(GROUP, ROWS, D)

    @pl.when(core != ITEM)
    def _():
        out_ref[...] = block_ref[:, ITEM]


def rest_body(block_ref, out_ref):
    out_ref[...] = block_ref[4:].reshape(GROUP, ROWS, D)


def by_role(item, query):
    core = lax.axis_index("blk")
    pl.when(core == ITEM)(item)
    pl.when(core != ITEM)(query)


def rows_of(ref):
    return ref[...].reshape(-1, D)


def own_queries(block_ref):
    return block_ref[:, 1 - ITEM].reshape(GROUP * ROWS, D)


def item_parts(block_ref):
    return [lambda k=k: block_ref[k].reshape(2 * ROWS, D) for k in range(GROUP)]


def got_parts(*refs):
    return [lambda ref=ref, k=k: ref[2 * k : 2 * k + 2].reshape(2 * ROWS, D) for ref in refs for k in range(4)]


def scores(parts, q, e_ref):
    total = jnp.zeros((1, GROUP * ROWS), f32)
    for k, part in enumerate(parts):
        t = lax.dot_general(part(), q, (((1,), (1,)), ((), ())), preferred_element_type=f32)
        e = jnp.exp2(t * (log2_e / sharpness))
        total = total + jnp.sum(e, axis=0, keepdims=True)
        e_ref[k] = e.astype(bf16)
    return total


def score0_body(block_ref, got_ref, e_ref, t_ref):
    def item():
        t_ref[:1] = scores(item_parts(block_ref)[:4], rows_of(got_ref), e_ref)

    def query():
        t_ref[:1] = scores(got_parts(got_ref), own_queries(block_ref), e_ref)

    by_role(item, query)


def score1_body(block_ref, got_a_ref, got_b_ref, t_ref, pos_ref, e_ref, s_ref):
    def send(total):
        total = total + t_ref[:1]
        total = jnp.concatenate([total[:, k * ROWS : (k + 1) * ROWS] for k in range(GROUP)], axis=0)
        for j in range(GROUP):
            s_ref[j, :8] = total

    def item():
        send(scores(item_parts(block_ref)[4:], rows_of(got_a_ref), e_ref))

    def query():
        send(scores(got_parts(got_b_ref), own_queries(block_ref), e_ref))

    by_role(item, query)
    for j in range(GROUP):
        s_ref[j, 8:16] = pos_ref[...]


def row_sums(s_ref):
    total = s_ref[0]
    for j in range(1, GROUP):
        total = total + s_ref[j]
    return total


def loss_part(sums, pos):
    return jnp.sum(jnp.log(sums)) - jnp.max(pos[:1])


def split(value):
    high = value.astype(bf16).astype(f32)
    return jnp.concatenate([high, value - high], axis=1).astype(bf16)


def joined(tail):
    tail = tail.astype(f32)
    return tail[:, :128] + tail[:, 128:]


def weigh(e_ref, q, r, store, ks=range(4)):
    for k in ks:
        parts = [
            (e_ref[k, :, j * ROWS : (j + 1) * ROWS].astype(f32) * r[j : j + 1]).astype(bf16)
            for j in range(GROUP)
        ]
        store(k, jnp.dot(jnp.concatenate(parts, axis=1), q, preferred_element_type=f32))


def pull(parts, e_refs, u_ref):
    total = None
    for i in range(0, GROUP, 2):
        v = jnp.concatenate([parts[i](), parts[i + 1]()], axis=0)
        k = i % 4
        e = e_refs[i // 4][k : k + 2].reshape(4 * ROWS, GROUP * ROWS)
        part = lax.dot_general(v, e, (((0,), (0,)), ((), ())), preferred_element_type=f32)
        total = part if total is None else total + part
    for k in range(GROUP):
        rows = slice(k * ROWS, (k + 1) * ROWS)
        u_ref[rows, :ROWS] = total[:ROWS, rows].astype(bf16)
        u_ref[rows, ROWS:] = total[ROWS:, rows].astype(bf16)


def into(ref):
    def store(k, w):
        ref[k * 256 : (k + 1) * 256] = w.astype(bf16)

    return store


def keeping(ref):
    def store(k, w):
        ref[k] = w

    return store


def first_body(e0_ref, e1_ref, block_ref, s_ref, give_ref):
    sums = row_sums(s_ref)
    give_ref[1024:1032] = split(sums[:8])
    give_ref[1032:1040] = split(sums[8:])

    def item():
        pull(item_parts(block_ref), (e0_ref, e1_ref), give_ref)

    def query():
        weigh(e0_ref, own_queries(block_ref), 1.0 / sums[:8], into(give_ref))

    by_role(item, query)


def second_body(e0_ref, e1_ref, block_ref, got_a_ref, s_ref, keep_ref, give_ref):
    r = 1.0 / row_sums(s_ref)[:8]

    def item():
        weigh(e0_ref, rows_of(got_a_ref), r, keeping(keep_ref), range(2))

    def query():
        weigh(e1_ref, own_queries(block_ref), r, into(give_ref))

    by_role(item, query)


def third_body(e0_ref, e1_ref, got_a_ref, got_b_ref, s_ref, keep0_ref, keep1_ref, u_ref):
    def item():
        r, q = 1.0 / row_sums(s_ref)[:8], rows_of(got_a_ref)
        weigh(e0_ref, q, r, lambda k, w: keeping(keep0_ref)(k - 2, w), range(2, 4))
        weigh(e1_ref, q, r, keeping(keep1_ref))

    def query():
        pull(got_parts(got_a_ref, got_b_ref), (e0_ref, e1_ref), u_ref)

    by_role(item, query)


def merge_body(keep0_ref, keep1_ref, u_ref, got_ref, s_ref, out_ref):
    def item():
        for k in range(4):
            keep = keep0_ref[k] if k < 2 else keep1_ref[k - 2]
            got = got_ref[k * 256 : (k + 1) * 256].astype(f32)
            out_ref[k, :256] = (keep + got).astype(bf16)
        sums = row_sums(s_ref)
        loss = loss_part(sums[:8], sums[8:])
        loss = loss + loss_part(joined(got_ref[1024:1032]), joined(got_ref[1032:1040]))
        tail = split(jnp.full((8, 128), loss, f32))
        for k in range(GROUP):
            out_ref[k, 256:264] = tail

    def query():
        for k in range(GROUP):
            rows = slice(k * ROWS, (k + 1) * ROWS)
            out_ref[k, (1 - ITEM) * 128 : (2 - ITEM) * 128] = u_ref[rows]
            out_ref[k, ITEM * 128 : (ITEM + 1) * 128] = got_ref[rows]
            out_ref[k, 256:264] = jnp.zeros((8, D), bf16)

    by_role(item, query)


def join_body(part_ref, keep_ref, got_ref, out_ref):
    out_ref[:4] = part_ref[:4]
    out_ref[4:, 256:264] = part_ref[4:, 256:264]

    def item():
        for k in range(4):
            got = got_ref[k * 256 : (k + 1) * 256].astype(f32)
            out_ref[4 + k, :256] = (keep_ref[k] + got).astype(bf16)

    def query():
        out_ref[4:, :256] = part_ref[4:, :256]

    by_role(item, query)


def summed(w_ref, first, rows):
    at = pl.ds(first, rows)
    total = w_ref[0, at].astype(f32)
    for k in range(1, GROUP):
        total = total + w_ref[k, at].astype(f32)
    return total


def give_body(w_ref, give_ref):
    core = lax.axis_index("blk")
    give_ref[:128] = summed(w_ref, pl.multiple_of((1 - core) * 128, 128), 128)
    give_ref[128:136] = jnp.concatenate([joined(summed(w_ref, 256, 8))] * 2, axis=1)


def slope(pull, hat, direction, length):
    grad = (pull - hat) / sharpness
    along = jnp.sum(direction * grad, axis=1, keepdims=True)
    return (grad - direction * along) / length


def query_slope(u, q_ref, v_ref, s_ref):
    q, q_len = unit(q_ref[...])
    sums = row_sums(s_ref)[:8]
    mine = lax.broadcasted_iota(jnp.int32, sums.shape, 0) == query_index()
    own = jnp.sum(jnp.where(mine, sums, 0.0), axis=0, keepdims=True)
    u = jnp.concatenate([(u[:, :128] / own).T, (u[:, 128:] / own).T], axis=1)
    return slope(u, hat(v_ref[...]).astype(f32), q, q_len)


def item_slope(w, q_ref, v_ref):
    v, v_len = unit(v_ref[...])
    return slope(w, hat(q_ref[...]).astype(f32), v, v_len)


def own_body(w_ref, q_ref, v_ref, s_ref, own_ref):
    core = lax.axis_index("blk")
    own = summed(w_ref, pl.multiple_of(core * 128, 128), 128)

    @pl.when(core == ITEM)
    def _():
        own_ref[...] = item_slope(own, q_ref, v_ref)

    @pl.when(core != ITEM)
    def _():
        own_ref[...] = query_slope(own, q_ref, v_ref, s_ref)


def final_body(q_ref, v_ref, own_ref, give_ref, got_ref, s_ref, qs_ref, vs_ref, loss_ref):
    core = lax.axis_index("blk")

    @pl.when(core == ITEM)
    def _():
        vs_ref[...] = own_ref[...]
        qs_ref[...] = query_slope(got_ref[:128], q_ref, v_ref, s_ref)
        loss_ref[0, 0] = jnp.max(give_ref[128:136]) / (128 * 128)

    @pl.when(core != ITEM)
    def _():
        qs_ref[...] = own_ref[...]
        vs_ref[...] = item_slope(got_ref[:128], q_ref, v_ref)
        loss_ref[0, 0] = jnp.max(got_ref[128:136]) / (128 * 128)


def per_device(queries, items):
    rows = (ROWS, D)
    bulk = (GROUP, 2, ROWS, D)
    in_hbm = [pltpu.with_memory_space_constraint(a, pltpu.HBM) for a in (queries, items)]
    mine, pos, q_raw, v_raw = call(
        norm_body,
        [(rows, bf16), ((8, 128), f32), (rows, bf16), (rows, bf16)],
        "norm",
        10**9,
        ins=[pl.BlockSpec(memory_space=pltpu.HBM)] * 2,
        scratch=[pltpu.SemaphoreType.DMA((2,))],
    )(*in_hbm)
    (tile,) = call(tile_body, [(bulk, bf16)], "tile")(mine, swap_cores(queries), swap_cores(items))
    block = exchange(tile, BULK)
    flops = 2 * 2048 * 1024 * 256
    cut = (GROUP, ROWS, D)
    (a,) = call(half_body, [(cut, bf16)], "half")(block)
    got_a = swap_cores(a)
    (b,) = call(rest_body, [(cut, bf16)], "rest")(block)
    got_b = swap_cores(b)
    scored = ((4, 256, 1024), bf16)
    e0, t = call(score0_body, [scored, ((8, GROUP * ROWS), f32)], "score0", flops)(block, got_a)
    e1, s = call(
        score1_body, [scored, ((GROUP, 16, 128), f32)], "score1", flops
    )(block, got_a, got_b, t, pos)
    sums = exchange(s, QUERY)
    pulled = (GROUP * ROWS, D)
    (give,) = call(first_body, [((1040, D), bf16)], "first", flops)(e0, e1, block, sums)
    got0 = swap_cores(give)
    keep0, give = call(
        second_body, [((2, 256, D), f32), (pulled, bf16)], "second", flops
    )(e0, e1, block, got_a, sums)
    got1 = swap_cores(give)
    keep1, keep2, u = call(
        third_body, [((2, 256, D), f32), ((4, 256, D), f32), (pulled, bf16)], "third", flops
    )(e0, e1, got_a, got_b, sums)
    packed = (GROUP, 264, D)
    (part,) = call(merge_body, [(packed, bf16)], "merge", flops)(keep0, keep1, u, got0, sums)
    (out,) = call(join_body, [(packed, bf16)], "join")(part, keep2, got1)
    out = exchange(out, BULK)
    (give,) = call(give_body, [((136, D), f32)], "give")(out)
    got = swap_cores(give)
    (own,) = call(own_body, [(rows, f32)], "own", flops)(out, q_raw, v_raw, sums)
    q_slope, v_slope, loss = call(
        final_body, [(rows, f32), (rows, f32), ((1, 1), f32, pltpu.SMEM)], "final"
    )(q_raw, v_raw, own, give, got, sums)
    return loss.reshape(()), q_slope, v_slope


def solution(mesh):
    split = Mesh(mesh.devices.reshape(2, 4, 4, 4), AXES)
    rows = P(AXES, None)
    return jax.shard_map(
        per_device, mesh=split, in_specs=(rows, rows), out_specs=(P(), rows, rows), check_vma=False
    )
```

```python
import math

import jax
import jax.numpy as jnp
from jax import lax
from jax.experimental import pallas as pl
from jax.experimental.pallas import tpu as pltpu
from jax.sharding import Mesh
from jax.sharding import PartitionSpec as P

AXES = ("blk", "z", "y", "x")
GROUP = 8
ROWS, D = 128, 256
ITEM = 1
RING_Q, RING_V, PAIR = "z", "y", "x"
NEAR, CROSS = ((0, 1), (2, 3)), ((1, 2), (3, 0))

sharpness = 0.05
tiny_square = 1e-12
log2_e = math.log2(math.e)
f32, bf16 = jnp.float32, jnp.bfloat16


ITEM_ORDER = ((7, 1, 0, 2, 6, 5, 4, 3), (2, 1, 0, 3, 4, 5, 6, 7))
QUERY_ORDER = ((3, 2, 7, 0, 1, 6, 5, 4), (3, 4, 1, 0, 7, 6, 5, 2))
SUM_ORDER = ((3, 1, 0, 2, 7, 5, 4, 6),) * 2


def groups(core, ring, pairs, fixed, orders):
    def device(at):
        return ((core * 4 + at["z"]) * 4 + at["y"]) * 4 + at["x"]

    return [
        [device({fixed: f, PAIR: pair[m // 4], ring: m % 4}) for m in order]
        for f in range(4)
        for pair, order in zip(pairs, orders)
    ]


def query_groups(core, orders):
    return groups(core, RING_Q, NEAR, RING_V, orders)


def item_groups(core, orders):
    return groups(core, RING_V, CROSS, RING_Q, orders)


def query_index():
    at = lax.axis_index(PAIR)
    member = at % 2 * 4 + lax.axis_index(RING_Q)
    index = jnp.int32(0)
    for k, (m0, m1) in enumerate(zip(*QUERY_ORDER)):
        index = jnp.where(member == jnp.where(at < 2, m0, m1), k, index)
    return index


BULK = item_groups(ITEM, ITEM_ORDER) + query_groups(1 - ITEM, QUERY_ORDER)
QUERY = query_groups(0, SUM_ORDER) + query_groups(1, SUM_ORDER)


def exchange(pieces, groups):
    return lax.all_to_all(pieces, AXES, 0, 0, tiled=True, axis_index_groups=groups)


def swap_cores(value):
    return lax.ppermute(value, "blk", [(0, 1), (1, 0)])


def call(body, outs, name, flops=0, ins=None, scratch=()):
    spec = pl.BlockSpec(memory_space=pltpu.VMEM)
    return pl.pallas_call(
        body,
        out_shape=[jax.ShapeDtypeStruct(s, d) for s, d, *_ in outs],
        out_specs=[pl.BlockSpec(memory_space=o[2]) if len(o) > 2 else spec for o in outs],
        **({"in_specs": ins} if ins else {}),
        scratch_shapes=list(scratch),
        compiler_params=pltpu.CompilerParams(vmem_limit_bytes=24 * 2**20),
        cost_estimate=pl.CostEstimate(flops=flops, bytes_accessed=0, transcendentals=0),
        name=name,
    )


def unit(matrix):
    wide = matrix.astype(f32)
    length = jnp.sqrt(jnp.sum(wide * wide, axis=1, keepdims=True) + tiny_square)
    return wide / length, length


def hat(matrix):
    return unit(matrix)[0].astype(bf16)


def norm_body(q_hbm, v_hbm, mine_ref, pos_ref, q_ref, v_ref, sem):
    copies = [
        pltpu.make_async_copy(q_hbm, q_ref, sem.at[0]),
        pltpu.make_async_copy(v_hbm, v_ref, sem.at[1]),
    ]
    for c in copies:
        c.start()
    core = lax.axis_index("blk")
    for c in copies:
        c.wait()
    q, v = hat(q_ref[...]), hat(v_ref[...])
    total = jnp.sum(q.astype(f32) * v.astype(f32)) / sharpness
    pos_ref[...] = jnp.full((8, 128), total, f32)

    @pl.when(core == ITEM)
    def _():
        mine_ref[...] = v

    @pl.when(core != ITEM)
    def _():
        mine_ref[...] = q


def tile_body(mine_ref, got_q_ref, got_v_ref, out_ref):
    core = lax.axis_index("blk")

    def fill(got_ref):
        mine, got = mine_ref[...], hat(got_ref[...])
        for k in range(GROUP):
            out_ref[k, core] = mine
            out_ref[k, 1 - core] = got

    @pl.when(core == ITEM)
    def _():
        fill(got_v_ref)

    @pl.when(core != ITEM)
    def _():
        fill(got_q_ref)


def half_body(block_ref, out_ref):
    core = lax.axis_index("blk")

    @pl.when(core == ITEM)
    def _():
        out_ref[...] = block_ref[:4].reshape(GROUP, ROWS, D)

    @pl.when(core != ITEM)
    def _():
        out_ref[...] = block_ref[:, ITEM]


def rest_body(block_ref, out_ref):
    out_ref[...] = block_ref[4:].reshape(GROUP, ROWS, D)


def by_role(item, query):
    core = lax.axis_index("blk")
    pl.when(core == ITEM)(item)
    pl.when(core != ITEM)(query)


def rows_of(ref):
    return ref[...].reshape(-1, D)


def own_queries(block_ref):
    return block_ref[:, 1 - ITEM].reshape(GROUP * ROWS, D)


def item_parts(block_ref):
    return [lambda k=k: block_ref[k].reshape(2 * ROWS, D) for k in range(GROUP)]


def got_parts(*refs):
    return [lambda ref=ref, k=k: ref[2 * k : 2 * k + 2].reshape(2 * ROWS, D) for ref in refs for k in range(4)]


def scores(parts, q, e_ref):
    total = jnp.zeros((1, GROUP * ROWS), f32)
    for k, part in enumerate(parts):
        t = lax.dot_general(part(), q, (((1,), (1,)), ((), ())), preferred_element_type=f32)
        e = jnp.exp2(t * (log2_e / sharpness))
        total = total + jnp.sum(e, axis=0, keepdims=True)
        e_ref[k] = e.astype(bf16)
    return total


def score0_body(block_ref, got_ref, e_ref, t_ref):
    def item():
        t_ref[:1] = scores(item_parts(block_ref)[:4], rows_of(got_ref), e_ref)

    def query():
        t_ref[:1] = scores(got_parts(got_ref), own_queries(block_ref), e_ref)

    by_role(item, query)


def score1_body(block_ref, got_a_ref, got_b_ref, t_ref, pos_ref, e_ref, s_ref):
    def send(total):
        total = total + t_ref[:1]
        total = jnp.concatenate([total[:, k * ROWS : (k + 1) * ROWS] for k in range(GROUP)], axis=0)
        for j in range(GROUP):
            s_ref[j, :8] = total

    def item():
        send(scores(item_parts(block_ref)[4:], rows_of(got_a_ref), e_ref))

    def query():
        send(scores(got_parts(got_b_ref), own_queries(block_ref), e_ref))

    by_role(item, query)
    for j in range(GROUP):
        s_ref[j, 8:16] = pos_ref[...]


def row_sums(s_ref):
    total = s_ref[0]
    for j in range(1, GROUP):
        total = total + s_ref[j]
    return total


def loss_part(sums, pos):
    return jnp.sum(jnp.log(sums)) - jnp.max(pos[:1])


def split(value):
    high = value.astype(bf16).astype(f32)
    return jnp.concatenate([high, value - high], axis=1).astype(bf16)


def joined(tail):
    tail = tail.astype(f32)
    return tail[:, :128] + tail[:, 128:]


def weigh(e_ref, q, r, store, ks=range(4)):
    for k in ks:
        parts = [
            (e_ref[k, :, j * ROWS : (j + 1) * ROWS].astype(f32) * r[j : j + 1]).astype(bf16)
            for j in range(GROUP)
        ]
        store(k, jnp.dot(jnp.concatenate(parts, axis=1), q, preferred_element_type=f32))


def pull(parts, e_refs, u_ref):
    total = None
    for i in range(0, GROUP, 2):
        v = jnp.concatenate([parts[i](), parts[i + 1]()], axis=0)
        k = i % 4
        e = e_refs[i // 4][k : k + 2].reshape(4 * ROWS, GROUP * ROWS)
        part = lax.dot_general(v, e, (((0,), (0,)), ((), ())), preferred_element_type=f32)
        total = part if total is None else total + part
    for k in range(GROUP):
        rows = slice(k * ROWS, (k + 1) * ROWS)
        u_ref[rows, :ROWS] = total[:ROWS, rows].astype(bf16)
        u_ref[rows, ROWS:] = total[ROWS:, rows].astype(bf16)


def into(ref):
    def store(k, w):
        ref[k * 256 : (k + 1) * 256] = w.astype(bf16)

    return store


def keeping(ref):
    def store(k, w):
        ref[k] = w

    return store


def first_body(e0_ref, e1_ref, block_ref, s_ref, give_ref):
    sums = row_sums(s_ref)
    give_ref[1024:1032] = split(sums[:8])
    give_ref[1032:1040] = split(sums[8:])

    def item():
        pull(item_parts(block_ref), (e0_ref, e1_ref), give_ref)

    def query():
        weigh(e0_ref, own_queries(block_ref), 1.0 / sums[:8], into(give_ref))

    by_role(item, query)


def second_body(e0_ref, e1_ref, block_ref, got_a_ref, s_ref, keep_ref, give_ref):
    r = 1.0 / row_sums(s_ref)[:8]

    def item():
        weigh(e0_ref, rows_of(got_a_ref), r, keeping(keep_ref), range(1))

    def query():
        weigh(e1_ref, own_queries(block_ref), r, into(give_ref))

    by_role(item, query)


def third_body(e0_ref, e1_ref, got_a_ref, got_b_ref, s_ref, keep0_ref, keep1_ref, u_ref):
    def item():
        r, q = 1.0 / row_sums(s_ref)[:8], rows_of(got_a_ref)
        weigh(e0_ref, q, r, lambda k, w: keeping(keep0_ref)(k - 1, w), range(1, 4))
        weigh(e1_ref, q, r, keeping(keep1_ref))

    def query():
        pull(got_parts(got_a_ref, got_b_ref), (e0_ref, e1_ref), u_ref)

    by_role(item, query)


def merge_body(keep0_ref, keep1_ref, u_ref, got_ref, s_ref, out_ref):
    def item():
        for k in range(4):
            keep = keep0_ref[k] if k < 1 else keep1_ref[k - 1]
            got = got_ref[k * 256 : (k + 1) * 256].astype(f32)
            out_ref[k, :256] = (keep + got).astype(bf16)
        sums = row_sums(s_ref)
        loss = loss_part(sums[:8], sums[8:])
        loss = loss + loss_part(joined(got_ref[1024:1032]), joined(got_ref[1032:1040]))
        tail = split(jnp.full((8, 128), loss, f32))
        for k in range(GROUP):
            out_ref[k, 256:264] = tail

    def query():
        for k in range(GROUP):
            rows = slice(k * ROWS, (k + 1) * ROWS)
            out_ref[k, (1 - ITEM) * 128 : (2 - ITEM) * 128] = u_ref[rows]
            out_ref[k, ITEM * 128 : (ITEM + 1) * 128] = got_ref[rows]
            out_ref[k, 256:264] = jnp.zeros((8, D), bf16)

    by_role(item, query)


def join_body(part_ref, keep_ref, got_ref, out_ref):
    out_ref[:4] = part_ref[:4]
    out_ref[4:, 256:264] = part_ref[4:, 256:264]

    def item():
        for k in range(4):
            got = got_ref[k * 256 : (k + 1) * 256].astype(f32)
            out_ref[4 + k, :256] = (keep_ref[k] + got).astype(bf16)

    def query():
        out_ref[4:, :256] = part_ref[4:, :256]

    by_role(item, query)


def summed(w_ref, first, rows):
    at = pl.ds(first, rows)
    total = w_ref[0, at].astype(f32)
    for k in range(1, GROUP):
        total = total + w_ref[k, at].astype(f32)
    return total


def give_body(w_ref, give_ref):
    core = lax.axis_index("blk")
    give_ref[:128] = summed(w_ref, pl.multiple_of((1 - core) * 128, 128), 128)
    give_ref[128:136] = jnp.concatenate([joined(summed(w_ref, 256, 8))] * 2, axis=1)


def slope(pull, hat, direction, length):
    grad = (pull - hat) / sharpness
    along = jnp.sum(direction * grad, axis=1, keepdims=True)
    return (grad - direction * along) / length


def query_slope(u, q_ref, v_ref, s_ref):
    q, q_len = unit(q_ref[...])
    sums = row_sums(s_ref)[:8]
    mine = lax.broadcasted_iota(jnp.int32, sums.shape, 0) == query_index()
    own = jnp.sum(jnp.where(mine, sums, 0.0), axis=0, keepdims=True)
    u = jnp.concatenate([(u[:, :128] / own).T, (u[:, 128:] / own).T], axis=1)
    return slope(u, hat(v_ref[...]).astype(f32), q, q_len)


def item_slope(w, q_ref, v_ref):
    v, v_len = unit(v_ref[...])
    return slope(w, hat(q_ref[...]).astype(f32), v, v_len)


def own_body(w_ref, q_ref, v_ref, s_ref, own_ref):
    core = lax.axis_index("blk")
    own = summed(w_ref, pl.multiple_of(core * 128, 128), 128)

    @pl.when(core == ITEM)
    def _():
        own_ref[...] = item_slope(own, q_ref, v_ref)

    @pl.when(core != ITEM)
    def _():
        own_ref[...] = query_slope(own, q_ref, v_ref, s_ref)


def final_body(q_ref, v_ref, own_ref, give_ref, got_ref, s_ref, qs_ref, vs_ref, loss_ref):
    core = lax.axis_index("blk")

    @pl.when(core == ITEM)
    def _():
        vs_ref[...] = own_ref[...]
        qs_ref[...] = query_slope(got_ref[:128], q_ref, v_ref, s_ref)
        loss_ref[0, 0] = jnp.max(give_ref[128:136]) / (128 * 128)

    @pl.when(core != ITEM)
    def _():
        qs_ref[...] = own_ref[...]
        vs_ref[...] = item_slope(got_ref[:128], q_ref, v_ref)
        loss_ref[0, 0] = jnp.max(got_ref[128:136]) / (128 * 128)


def per_device(queries, items):
    rows = (ROWS, D)
    bulk = (GROUP, 2, ROWS, D)
    in_hbm = [pltpu.with_memory_space_constraint(a, pltpu.HBM) for a in (queries, items)]
    mine, pos, q_raw, v_raw = call(
        norm_body,
        [(rows, bf16), ((8, 128), f32), (rows, bf16), (rows, bf16)],
        "norm",
        10**9,
        ins=[pl.BlockSpec(memory_space=pltpu.HBM)] * 2,
        scratch=[pltpu.SemaphoreType.DMA((2,))],
    )(*in_hbm)
    (tile,) = call(tile_body, [(bulk, bf16)], "tile")(mine, swap_cores(queries), swap_cores(items))
    block = exchange(tile, BULK)
    flops = 2 * 2048 * 1024 * 256
    cut = (GROUP, ROWS, D)
    (a,) = call(half_body, [(cut, bf16)], "half")(block)
    got_a = swap_cores(a)
    (b,) = call(rest_body, [(cut, bf16)], "rest")(block)
    got_b = swap_cores(b)
    scored = ((4, 256, 1024), bf16)
    e0, t = call(score0_body, [scored, ((8, GROUP * ROWS), f32)], "score0", flops)(block, got_a)
    e1, s = call(
        score1_body, [scored, ((GROUP, 16, 128), f32)], "score1", flops
    )(block, got_a, got_b, t, pos)
    sums = exchange(s, QUERY)
    pulled = (GROUP * ROWS, D)
    (give,) = call(first_body, [((1040, D), bf16)], "first", flops)(e0, e1, block, sums)
    got0 = swap_cores(give)
    keep0, give = call(
        second_body, [((1, 256, D), f32), (pulled, bf16)], "second", flops
    )(e0, e1, block, got_a, sums)
    got1 = swap_cores(give)
    keep1, keep2, u = call(
        third_body, [((3, 256, D), f32), ((4, 256, D), f32), (pulled, bf16)], "third", flops
    )(e0, e1, got_a, got_b, sums)
    packed = (GROUP, 264, D)
    (part,) = call(merge_body, [(packed, bf16)], "merge", flops)(keep0, keep1, u, got0, sums)
    (out,) = call(join_body, [(packed, bf16)], "join")(part, keep2, got1)
    out = exchange(out, BULK)
    (give,) = call(give_body, [((136, D), f32)], "give")(out)
    got = swap_cores(give)
    (own,) = call(own_body, [(rows, f32)], "own", flops)(out, q_raw, v_raw, sums)
    q_slope, v_slope, loss = call(
        final_body, [(rows, f32), (rows, f32), ((1, 1), f32, pltpu.SMEM)], "final"
    )(q_raw, v_raw, own, give, got, sums)
    return loss.reshape(()), q_slope, v_slope


def solution(mesh):
    split = Mesh(mesh.devices.reshape(2, 4, 4, 4), AXES)
    rows = P(AXES, None)
    return jax.shard_map(
        per_device, mesh=split, in_specs=(rows, rows), out_specs=(P(), rows, rows), check_vma=False
    )
```

```python
import math

import jax
import jax.numpy as jnp
from jax import lax
from jax.experimental import pallas as pl
from jax.experimental.pallas import tpu as pltpu
from jax.sharding import Mesh
from jax.sharding import PartitionSpec as P

AXES = ("blk", "z", "y", "x")
GROUP = 8
ROWS, D = 128, 256
ITEM = 1
RING_Q, RING_V, PAIR = "z", "y", "x"
NEAR, CROSS = ((0, 1), (2, 3)), ((1, 2), (3, 0))

sharpness = 0.05
tiny_square = 1e-12
log2_e = math.log2(math.e)
f32, bf16 = jnp.float32, jnp.bfloat16


ITEM_ORDER = ((7, 1, 0, 2, 6, 5, 4, 3), (2, 1, 0, 3, 4, 5, 6, 7))
QUERY_ORDER = ((3, 2, 7, 0, 1, 6, 5, 4), (3, 4, 1, 0, 7, 6, 5, 2))
SUM_ORDER = ((3, 1, 0, 2, 7, 5, 4, 6),) * 2


def groups(core, ring, pairs, fixed, orders):
    def device(at):
        return ((core * 4 + at["z"]) * 4 + at["y"]) * 4 + at["x"]

    return [
        [device({fixed: f, PAIR: pair[m // 4], ring: m % 4}) for m in order]
        for f in range(4)
        for pair, order in zip(pairs, orders)
    ]


def query_groups(core, orders):
    return groups(core, RING_Q, NEAR, RING_V, orders)


def item_groups(core, orders):
    return groups(core, RING_V, CROSS, RING_Q, orders)


def query_index():
    at = lax.axis_index(PAIR)
    member = at % 2 * 4 + lax.axis_index(RING_Q)
    index = jnp.int32(0)
    for k, (m0, m1) in enumerate(zip(*QUERY_ORDER)):
        index = jnp.where(member == jnp.where(at < 2, m0, m1), k, index)
    return index


BULK = item_groups(ITEM, ITEM_ORDER) + query_groups(1 - ITEM, QUERY_ORDER)
QUERY = query_groups(0, SUM_ORDER) + query_groups(1, SUM_ORDER)


def exchange(pieces, groups):
    return lax.all_to_all(pieces, AXES, 0, 0, tiled=True, axis_index_groups=groups)


def swap_cores(value):
    return lax.ppermute(value, "blk", [(0, 1), (1, 0)])


def call(body, outs, name, flops=0, ins=None, scratch=()):
    spec = pl.BlockSpec(memory_space=pltpu.VMEM)
    return pl.pallas_call(
        body,
        out_shape=[jax.ShapeDtypeStruct(s, d) for s, d, *_ in outs],
        out_specs=[pl.BlockSpec(memory_space=o[2]) if len(o) > 2 else spec for o in outs],
        **({"in_specs": ins} if ins else {}),
        scratch_shapes=list(scratch),
        compiler_params=pltpu.CompilerParams(vmem_limit_bytes=24 * 2**20),
        cost_estimate=pl.CostEstimate(flops=flops, bytes_accessed=0, transcendentals=0),
        name=name,
    )


def unit(matrix):
    wide = matrix.astype(f32)
    length = jnp.sqrt(jnp.sum(wide * wide, axis=1, keepdims=True) + tiny_square)
    return wide / length, length


def hat(matrix):
    return unit(matrix)[0].astype(bf16)


def norm_body(q_hbm, v_hbm, mine_ref, pos_ref, q_ref, v_ref, sem):
    copies = [
        pltpu.make_async_copy(q_hbm, q_ref, sem.at[0]),
        pltpu.make_async_copy(v_hbm, v_ref, sem.at[1]),
    ]
    for c in copies:
        c.start()
    core = lax.axis_index("blk")
    for c in copies:
        c.wait()
    q, v = hat(q_ref[...]), hat(v_ref[...])
    total = jnp.sum(q.astype(f32) * v.astype(f32)) / sharpness
    pos_ref[...] = jnp.full((8, 128), total, f32)

    @pl.when(core == ITEM)
    def _():
        mine_ref[...] = v

    @pl.when(core != ITEM)
    def _():
        mine_ref[...] = q


def tile_body(mine_ref, got_q_ref, got_v_ref, out_ref):
    core = lax.axis_index("blk")

    def fill(got_ref):
        mine, got = mine_ref[...], hat(got_ref[...])
        for k in range(GROUP):
            out_ref[k, core] = mine
            out_ref[k, 1 - core] = got

    @pl.when(core == ITEM)
    def _():
        fill(got_v_ref)

    @pl.when(core != ITEM)
    def _():
        fill(got_q_ref)


def half_body(block_ref, out_ref):
    core = lax.axis_index("blk")

    @pl.when(core == ITEM)
    def _():
        out_ref[...] = block_ref[:4].reshape(GROUP, ROWS, D)

    @pl.when(core != ITEM)
    def _():
        out_ref[...] = block_ref[:, ITEM]


def rest_body(block_ref, out_ref):
    out_ref[...] = block_ref[4:].reshape(GROUP, ROWS, D)


def by_role(item, query):
    core = lax.axis_index("blk")
    pl.when(core == ITEM)(item)
    pl.when(core != ITEM)(query)


def rows_of(ref):
    return ref[...].reshape(-1, D)


def own_queries(block_ref):
    return block_ref[:, 1 - ITEM].reshape(GROUP * ROWS, D)


def item_parts(block_ref):
    return [lambda k=k: block_ref[k].reshape(2 * ROWS, D) for k in range(GROUP)]


def got_parts(*refs):
    return [lambda ref=ref, k=k: ref[2 * k : 2 * k + 2].reshape(2 * ROWS, D) for ref in refs for k in range(4)]


def scores(parts, q, e_ref):
    total = jnp.zeros((1, GROUP * ROWS), f32)
    for k, part in enumerate(parts):
        t = lax.dot_general(part(), q, (((1,), (1,)), ((), ())), preferred_element_type=f32)
        e = jnp.exp2(t * (log2_e / sharpness))
        total = total + jnp.sum(e, axis=0, keepdims=True)
        e_ref[k] = e.astype(bf16)
    return total


def score0_body(block_ref, got_ref, e_ref, t_ref):
    def item():
        t_ref[:1] = scores(item_parts(block_ref)[:4], rows_of(got_ref), e_ref)

    def query():
        t_ref[:1] = scores(got_parts(got_ref), own_queries(block_ref), e_ref)

    by_role(item, query)


def score1_body(block_ref, got_a_ref, got_b_ref, t_ref, pos_ref, e_ref, s_ref):
    def send(total):
        total = total + t_ref[:1]
        total = jnp.concatenate([total[:, k * ROWS : (k + 1) * ROWS] for k in range(GROUP)], axis=0)
        for j in range(GROUP):
            s_ref[j, :8] = total

    def item():
        send(scores(item_parts(block_ref)[4:], rows_of(got_a_ref), e_ref))

    def query():
        send(scores(got_parts(got_b_ref), own_queries(block_ref), e_ref))

    by_role(item, query)
    for j in range(GROUP):
        s_ref[j, 8:16] = pos_ref[...]


def row_sums(s_ref):
    total = s_ref[0]
    for j in range(1, GROUP):
        total = total + s_ref[j]
    return total


def loss_part(sums, pos):
    return jnp.sum(jnp.log(sums)) - jnp.max(pos[:1])


def split(value):
    high = value.astype(bf16).astype(f32)
    return jnp.concatenate([high, value - high], axis=1).astype(bf16)


def joined(tail):
    tail = tail.astype(f32)
    return tail[:, :128] + tail[:, 128:]


def weigh(e_ref, q, r, store, ks=range(4)):
    for k in ks:
        parts = [
            (e_ref[k, :, j * ROWS : (j + 1) * ROWS].astype(f32) * r[j : j + 1]).astype(bf16)
            for j in range(GROUP)
        ]
        store(k, jnp.dot(jnp.concatenate(parts, axis=1), q, preferred_element_type=f32))


def pull(parts, e_refs, u_ref):
    total = None
    for i in range(0, GROUP, 2):
        v = jnp.concatenate([parts[i](), parts[i + 1]()], axis=0)
        k = i % 4
        e = e_refs[i // 4][k : k + 2].reshape(4 * ROWS, GROUP * ROWS)
        part = lax.dot_general(v, e, (((0,), (0,)), ((), ())), preferred_element_type=f32)
        total = part if total is None else total + part
    for k in range(GROUP):
        rows = slice(k * ROWS, (k + 1) * ROWS)
        u_ref[rows, :ROWS] = total[:ROWS, rows].astype(bf16)
        u_ref[rows, ROWS:] = total[ROWS:, rows].astype(bf16)


def into(ref):
    def store(k, w):
        ref[k * 256 : (k + 1) * 256] = w.astype(bf16)

    return store


def keeping(ref):
    def store(k, w):
        ref[k] = w

    return store


def first_body(e0_ref, e1_ref, block_ref, s_ref, give_ref):
    sums = row_sums(s_ref)
    give_ref[1024:1032] = split(sums[:8])
    give_ref[1032:1040] = split(sums[8:])

    def item():
        pull(item_parts(block_ref), (e0_ref, e1_ref), give_ref)

    def query():
        weigh(e0_ref, own_queries(block_ref), 1.0 / sums[:8], into(give_ref))

    by_role(item, query)


def second_body(e0_ref, e1_ref, block_ref, got_a_ref, s_ref, keep_ref, give_ref):
    r = 1.0 / row_sums(s_ref)[:8]

    def item():
        weigh(e0_ref, rows_of(got_a_ref), r, keeping(keep_ref), range(2))

    def query():
        weigh(e1_ref, own_queries(block_ref), r, into(give_ref))

    by_role(item, query)


def third_body(e0_ref, e1_ref, got_a_ref, got_b_ref, s_ref, keep0_ref, keep1_ref, u_ref):
    def item():
        r, q = 1.0 / row_sums(s_ref)[:8], rows_of(got_a_ref)
        weigh(e0_ref, q, r, lambda k, w: keeping(keep0_ref)(k - 2, w), range(2, 4))
        weigh(e1_ref, q, r, keeping(keep1_ref))

    def query():
        pull(got_parts(got_a_ref, got_b_ref), (e0_ref, e1_ref), u_ref)

    by_role(item, query)


def merge_body(keep0_ref, keep1_ref, u_ref, got_ref, s_ref, out_ref):
    def item():
        for k in range(4):
            keep = keep0_ref[k] if k < 2 else keep1_ref[k - 2]
            got = got_ref[k * 256 : (k + 1) * 256].astype(f32)
            out_ref[k, :256] = (keep + got).astype(bf16)
        sums = row_sums(s_ref)
        loss = loss_part(sums[:8], sums[8:])
        loss = loss + loss_part(joined(got_ref[1024:1032]), joined(got_ref[1032:1040]))
        tail = split(jnp.full((8, 128), loss, f32))
        for k in range(GROUP):
            out_ref[k, 256:264] = tail

    def query():
        for k in range(GROUP):
            rows = slice(k * ROWS, (k + 1) * ROWS)
            out_ref[k, (1 - ITEM) * 128 : (2 - ITEM) * 128] = u_ref[rows]
            out_ref[k, ITEM * 128 : (ITEM + 1) * 128] = got_ref[rows]
            out_ref[k, 256:264] = jnp.zeros((8, D), bf16)

    by_role(item, query)


def join_body(part_ref, keep_ref, got_ref, out_ref):
    out_ref[:4] = part_ref[:4]
    out_ref[4:, 256:264] = part_ref[4:, 256:264]

    def item():
        for k in range(4):
            got = got_ref[k * 256 : (k + 1) * 256].astype(f32)
            out_ref[4 + k, :256] = (keep_ref[k] + got).astype(bf16)

    def query():
        out_ref[4:, :256] = part_ref[4:, :256]

    by_role(item, query)


def summed(w_ref, first, rows):
    at = pl.ds(first, rows)
    total = w_ref[0, at].astype(f32)
    for k in range(1, GROUP):
        total = total + w_ref[k, at].astype(f32)
    return total


def give_body(w_ref, give_ref):
    core = lax.axis_index("blk")
    give_ref[:128] = summed(w_ref, pl.multiple_of((1 - core) * 128, 128), 128)
    give_ref[128:136] = jnp.concatenate([joined(summed(w_ref, 256, 8))] * 2, axis=1)


def slope(pull, hat, direction, length):
    grad = (pull - hat) / sharpness
    along = jnp.sum(direction * grad, axis=1, keepdims=True)
    return (grad - direction * along) / length


def query_pull(u, s_ref):
    sums = row_sums(s_ref)[:8]
    mine = lax.broadcasted_iota(jnp.int32, sums.shape, 0) == query_index()
    own = jnp.sum(jnp.where(mine, sums, 0.0), axis=0, keepdims=True)
    return jnp.concatenate([(u[:, :128] / own).T, (u[:, 128:] / own).T], axis=1)


def own_body(w_ref, q_ref, v_ref, s_ref, own_ref, direction_ref, hat_ref, length_ref):
    core = lax.axis_index("blk")
    own = summed(w_ref, pl.multiple_of(core * 128, 128), 128)
    q, q_len = unit(q_ref[...])
    v, v_len = unit(v_ref[...])
    q_hat, v_hat = q.astype(bf16).astype(f32), v.astype(bf16).astype(f32)

    def leave(direction, other_hat, length):
        direction_ref[...] = direction
        hat_ref[...] = other_hat
        length_ref[...] = jnp.broadcast_to(length, length_ref.shape)

    def item():
        own_ref[...] = slope(own, q_hat, v, v_len)
        leave(q, v_hat, q_len)

    def query():
        own_ref[...] = slope(query_pull(own, s_ref), v_hat, q, q_len)
        leave(v, q_hat, v_len)

    by_role(item, query)


def final_body(own_ref, direction_ref, hat_ref, length_ref, give_ref, got_ref, s_ref, qs_ref, vs_ref, loss_ref):
    def other(pulled):
        return slope(pulled, hat_ref[...], direction_ref[...], length_ref[...])

    def item():
        vs_ref[...] = own_ref[...]
        qs_ref[...] = other(query_pull(got_ref[:128], s_ref))
        loss_ref[0, 0] = jnp.max(give_ref[128:136]) / (128 * 128)

    def query():
        qs_ref[...] = own_ref[...]
        vs_ref[...] = other(got_ref[:128])
        loss_ref[0, 0] = jnp.max(got_ref[128:136]) / (128 * 128)

    by_role(item, query)


def per_device(queries, items):
    rows = (ROWS, D)
    bulk = (GROUP, 2, ROWS, D)
    in_hbm = [pltpu.with_memory_space_constraint(a, pltpu.HBM) for a in (queries, items)]
    mine, pos, q_raw, v_raw = call(
        norm_body,
        [(rows, bf16), ((8, 128), f32), (rows, bf16), (rows, bf16)],
        "norm",
        10**9,
        ins=[pl.BlockSpec(memory_space=pltpu.HBM)] * 2,
        scratch=[pltpu.SemaphoreType.DMA((2,))],
    )(*in_hbm)
    (tile,) = call(tile_body, [(bulk, bf16)], "tile")(mine, swap_cores(queries), swap_cores(items))
    block = exchange(tile, BULK)
    flops = 2 * 2048 * 1024 * 256
    cut = (GROUP, ROWS, D)
    (a,) = call(half_body, [(cut, bf16)], "half")(block)
    got_a = swap_cores(a)
    (b,) = call(rest_body, [(cut, bf16)], "rest")(block)
    got_b = swap_cores(b)
    scored = ((4, 256, 1024), bf16)
    e0, t = call(score0_body, [scored, ((8, GROUP * ROWS), f32)], "score0", flops)(block, got_a)
    e1, s = call(
        score1_body, [scored, ((GROUP, 16, 128), f32)], "score1", flops
    )(block, got_a, got_b, t, pos)
    sums = exchange(s, QUERY)
    pulled = (GROUP * ROWS, D)
    (give,) = call(first_body, [((1040, D), bf16)], "first", flops)(e0, e1, block, sums)
    got0 = swap_cores(give)
    keep0, give = call(
        second_body, [((2, 256, D), f32), (pulled, bf16)], "second", flops
    )(e0, e1, block, got_a, sums)
    got1 = swap_cores(give)
    keep1, keep2, u = call(
        third_body, [((2, 256, D), f32), ((4, 256, D), f32), (pulled, bf16)], "third", flops
    )(e0, e1, got_a, got_b, sums)
    packed = (GROUP, 264, D)
    (part,) = call(merge_body, [(packed, bf16)], "merge", flops)(keep0, keep1, u, got0, sums)
    (out,) = call(join_body, [(packed, bf16)], "join")(part, keep2, got1)
    out = exchange(out, BULK)
    (give,) = call(give_body, [((136, D), f32)], "give")(out)
    got = swap_cores(give)
    ready = call(own_body, [(rows, f32)] * 4, "own", flops)(out, q_raw, v_raw, sums)
    q_slope, v_slope, loss = call(
        final_body, [(rows, f32), (rows, f32), ((1, 1), f32, pltpu.SMEM)], "final"
    )(*ready, give, got, sums)
    return loss.reshape(()), q_slope, v_slope


def solution(mesh):
    split = Mesh(mesh.devices.reshape(2, 4, 4, 4), AXES)
    rows = P(AXES, None)
    return jax.shard_map(
        per_device, mesh=split, in_specs=(rows, rows), out_specs=(P(), rows, rows), check_vma=False
    )
```

```python
import math

import jax
import jax.numpy as jnp
from jax import lax
from jax.experimental import pallas as pl
from jax.experimental.pallas import tpu as pltpu
from jax.sharding import Mesh
from jax.sharding import PartitionSpec as P

AXES = ("blk", "z", "y", "x")
GROUP = 8
ROWS, D = 128, 256
ITEM = 1
RING_Q, RING_V, PAIR = "z", "y", "x"
NEAR, CROSS = ((0, 1), (2, 3)), ((1, 2), (3, 0))

sharpness = 0.05
tiny_square = 1e-12
log2_e = math.log2(math.e)
f32, bf16 = jnp.float32, jnp.bfloat16


ITEM_ORDER = ((7, 1, 0, 2, 6, 5, 4, 3), (2, 1, 0, 3, 4, 5, 6, 7))
QUERY_ORDER = ((3, 2, 7, 0, 1, 6, 5, 4), (3, 4, 1, 0, 7, 6, 5, 2))
SUM_ORDER = ((3, 1, 0, 2, 7, 5, 4, 6),) * 2


def groups(core, ring, pairs, fixed, orders):
    def device(at):
        return ((core * 4 + at["z"]) * 4 + at["y"]) * 4 + at["x"]

    return [
        [device({fixed: f, PAIR: pair[m // 4], ring: m % 4}) for m in order]
        for f in range(4)
        for pair, order in zip(pairs, orders)
    ]


def query_groups(core, orders):
    return groups(core, RING_Q, NEAR, RING_V, orders)


def item_groups(core, orders):
    return groups(core, RING_V, CROSS, RING_Q, orders)


def query_index():
    at = lax.axis_index(PAIR)
    member = at % 2 * 4 + lax.axis_index(RING_Q)
    index = jnp.int32(0)
    for k, (m0, m1) in enumerate(zip(*QUERY_ORDER)):
        index = jnp.where(member == jnp.where(at < 2, m0, m1), k, index)
    return index


BULK = item_groups(ITEM, ITEM_ORDER) + query_groups(1 - ITEM, QUERY_ORDER)
QUERY = query_groups(0, SUM_ORDER) + query_groups(1, SUM_ORDER)


def exchange(pieces, groups):
    return lax.all_to_all(pieces, AXES, 0, 0, tiled=True, axis_index_groups=groups)


def swap_cores(value):
    return lax.ppermute(value, "blk", [(0, 1), (1, 0)])


def call(body, outs, name, flops=0, ins=None, scratch=()):
    spec = pl.BlockSpec(memory_space=pltpu.VMEM)
    return pl.pallas_call(
        body,
        out_shape=[jax.ShapeDtypeStruct(s, d) for s, d, *_ in outs],
        out_specs=[pl.BlockSpec(memory_space=o[2]) if len(o) > 2 else spec for o in outs],
        **({"in_specs": ins} if ins else {}),
        scratch_shapes=list(scratch),
        compiler_params=pltpu.CompilerParams(vmem_limit_bytes=24 * 2**20),
        cost_estimate=pl.CostEstimate(flops=flops, bytes_accessed=0, transcendentals=0),
        name=name,
    )


def unit(matrix):
    wide = matrix.astype(f32)
    length = jnp.sqrt(jnp.sum(wide * wide, axis=1, keepdims=True) + tiny_square)
    return wide / length, length


def hat(matrix):
    return unit(matrix)[0].astype(bf16)


def norm_body(q_hbm, v_hbm, mine_ref, pos_ref, q_ref, v_ref, sem):
    copies = [
        pltpu.make_async_copy(q_hbm, q_ref, sem.at[0]),
        pltpu.make_async_copy(v_hbm, v_ref, sem.at[1]),
    ]
    for c in copies:
        c.start()
    core = lax.axis_index("blk")
    for c in copies:
        c.wait()
    q, v = hat(q_ref[...]), hat(v_ref[...])
    total = jnp.sum(q.astype(f32) * v.astype(f32)) / sharpness
    pos_ref[...] = jnp.full((8, 128), total, f32)

    @pl.when(core == ITEM)
    def _():
        mine_ref[...] = v

    @pl.when(core != ITEM)
    def _():
        mine_ref[...] = q


def tile_body(mine_ref, got_q_ref, got_v_ref, out_ref):
    core = lax.axis_index("blk")

    def fill(got_ref):
        mine, got = mine_ref[...], hat(got_ref[...])
        for k in range(GROUP):
            out_ref[k, core] = mine
            out_ref[k, 1 - core] = got

    @pl.when(core == ITEM)
    def _():
        fill(got_v_ref)

    @pl.when(core != ITEM)
    def _():
        fill(got_q_ref)


def half_body(block_ref, out_ref):
    core = lax.axis_index("blk")

    @pl.when(core == ITEM)
    def _():
        out_ref[...] = block_ref[:4].reshape(GROUP, ROWS, D)

    @pl.when(core != ITEM)
    def _():
        out_ref[...] = block_ref[:, ITEM]


def rest_body(block_ref, out_ref):
    out_ref[...] = block_ref[4:].reshape(GROUP, ROWS, D)


def by_role(item, query):
    core = lax.axis_index("blk")
    pl.when(core == ITEM)(item)
    pl.when(core != ITEM)(query)


def rows_of(ref):
    return ref[...].reshape(-1, D)


def own_queries(block_ref):
    return block_ref[:, 1 - ITEM].reshape(GROUP * ROWS, D)


def item_parts(block_ref):
    return [lambda k=k: block_ref[k].reshape(2 * ROWS, D) for k in range(GROUP)]


def got_parts(*refs):
    return [lambda ref=ref, k=k: ref[2 * k : 2 * k + 2].reshape(2 * ROWS, D) for ref in refs for k in range(4)]


def scores(parts, q, e_ref):
    total = jnp.zeros((1, GROUP * ROWS), f32)
    for k, part in enumerate(parts):
        t = lax.dot_general(part(), q, (((1,), (1,)), ((), ())), preferred_element_type=f32)
        e = jnp.exp2(t * (log2_e / sharpness))
        total = total + jnp.sum(e, axis=0, keepdims=True)
        e_ref[k] = e.astype(bf16)
    return total


def score0_body(block_ref, got_ref, e_ref, t_ref):
    def item():
        t_ref[:1] = scores(item_parts(block_ref)[:4], rows_of(got_ref), e_ref)

    def query():
        t_ref[:1] = scores(got_parts(got_ref), own_queries(block_ref), e_ref)

    by_role(item, query)


def score1_body(block_ref, got_a_ref, got_b_ref, t_ref, pos_ref, e_ref, s_ref):
    def send(total):
        total = total + t_ref[:1]
        total = jnp.concatenate([total[:, k * ROWS : (k + 1) * ROWS] for k in range(GROUP)], axis=0)
        for j in range(GROUP):
            s_ref[j, :8] = total

    def item():
        send(scores(item_parts(block_ref)[4:], rows_of(got_a_ref), e_ref))

    def query():
        send(scores(got_parts(got_b_ref), own_queries(block_ref), e_ref))

    by_role(item, query)
    for j in range(GROUP):
        s_ref[j, 8:16] = pos_ref[...]


def row_sums(s_ref):
    total = s_ref[0]
    for j in range(1, GROUP):
        total = total + s_ref[j]
    return total


def loss_part(sums, pos):
    return jnp.sum(jnp.log(sums)) - jnp.max(pos[:1])


def split(value):
    high = value.astype(bf16).astype(f32)
    return jnp.concatenate([high, value - high], axis=1).astype(bf16)


def joined(tail):
    tail = tail.astype(f32)
    return tail[:, :128] + tail[:, 128:]


def weigh(e_ref, q, r, store, ks=range(4)):
    for k in ks:
        parts = [
            (e_ref[k, :, j * ROWS : (j + 1) * ROWS].astype(f32) * r[j : j + 1]).astype(bf16)
            for j in range(GROUP)
        ]
        store(k, jnp.dot(jnp.concatenate(parts, axis=1), q, preferred_element_type=f32))


def pull(parts, e_refs, u_ref):
    total = None
    for i in range(0, GROUP, 2):
        v = jnp.concatenate([parts[i](), parts[i + 1]()], axis=0)
        k = i % 4
        e = e_refs[i // 4][k : k + 2].reshape(4 * ROWS, GROUP * ROWS)
        part = lax.dot_general(v, e, (((0,), (0,)), ((), ())), preferred_element_type=f32)
        total = part if total is None else total + part
    for k in range(GROUP):
        rows = slice(k * ROWS, (k + 1) * ROWS)
        u_ref[rows, :ROWS] = total[:ROWS, rows].astype(bf16)
        u_ref[rows, ROWS:] = total[ROWS:, rows].astype(bf16)


def into(ref):
    def store(k, w):
        ref[k * 256 : (k + 1) * 256] = w.astype(bf16)

    return store


def keeping(ref):
    def store(k, w):
        ref[k] = w

    return store


def first_body(e0_ref, e1_ref, block_ref, s_ref, give_ref):
    sums = row_sums(s_ref)
    give_ref[1024:1032] = split(sums[:8])
    give_ref[1032:1040] = split(sums[8:])

    def item():
        pull(item_parts(block_ref), (e0_ref, e1_ref), give_ref)

    def query():
        weigh(e0_ref, own_queries(block_ref), 1.0 / sums[:8], into(give_ref))

    by_role(item, query)


def second_body(e0_ref, e1_ref, block_ref, got_a_ref, s_ref, keep_ref, give_ref):
    r = 1.0 / row_sums(s_ref)[:8]

    def item():
        weigh(e0_ref, rows_of(got_a_ref), r, keeping(keep_ref), range(2))

    def query():
        weigh(e1_ref, own_queries(block_ref), r, into(give_ref))

    by_role(item, query)


def third_body(e0_ref, e1_ref, got_a_ref, got_b_ref, s_ref, keep0_ref, keep1_ref, u_ref):
    def item():
        r, q = 1.0 / row_sums(s_ref)[:8], rows_of(got_a_ref)
        weigh(e0_ref, q, r, lambda k, w: keeping(keep0_ref)(k - 2, w), range(2, 4))
        weigh(e1_ref, q, r, keeping(keep1_ref))

    def query():
        pull(got_parts(got_a_ref, got_b_ref), (e0_ref, e1_ref), u_ref)

    by_role(item, query)


def merge_body(keep0_ref, keep1_ref, u_ref, got_ref, s_ref, out_ref):
    def item():
        for k in range(4):
            keep = keep0_ref[k] if k < 2 else keep1_ref[k - 2]
            got = got_ref[k * 256 : (k + 1) * 256].astype(f32)
            out_ref[k, :256] = (keep + got).astype(bf16)
        sums = row_sums(s_ref)
        loss = loss_part(sums[:8], sums[8:])
        loss = loss + loss_part(joined(got_ref[1024:1032]), joined(got_ref[1032:1040]))
        tail = split(jnp.full((8, 128), loss, f32))
        for k in range(GROUP):
            out_ref[k, 256:264] = tail

    def query():
        for k in range(GROUP):
            rows = slice(k * ROWS, (k + 1) * ROWS)
            out_ref[k, (1 - ITEM) * 128 : (2 - ITEM) * 128] = u_ref[rows]
            out_ref[k, ITEM * 128 : (ITEM + 1) * 128] = got_ref[rows]
            out_ref[k, 256:264] = jnp.zeros((8, D), bf16)

    by_role(item, query)


def join_body(part_ref, keep_ref, got_ref, out_ref):
    out_ref[:4] = part_ref[:4]
    out_ref[4:, 256:264] = part_ref[4:, 256:264]

    def item():
        for k in range(4):
            got = got_ref[k * 256 : (k + 1) * 256].astype(f32)
            out_ref[4 + k, :256] = (keep_ref[k] + got).astype(bf16)

    def query():
        out_ref[4:, :256] = part_ref[4:, :256]

    by_role(item, query)


def summed(w_ref, first, rows):
    at = pl.ds(first, rows)
    total = w_ref[0, at].astype(f32)
    for k in range(1, GROUP):
        total = total + w_ref[k, at].astype(f32)
    return total


def give_body(w_ref, give_ref):
    core = lax.axis_index("blk")
    give_ref[:128] = summed(w_ref, pl.multiple_of((1 - core) * 128, 128), 128)
    give_ref[128:136] = jnp.concatenate([joined(summed(w_ref, 256, 8))] * 2, axis=1)


def slope(pull, hat, direction, length):
    grad = (pull - hat) / sharpness
    along = jnp.sum(direction * grad, axis=1, keepdims=True)
    return (grad - direction * along) / length


def own_share(s_ref):
    sums = row_sums(s_ref)[:8]
    mine = lax.broadcasted_iota(jnp.int32, sums.shape, 0) == query_index()
    return 1.0 / jnp.sum(jnp.where(mine, sums, 0.0), axis=0, keepdims=True)


def query_pull(u, share):
    return jnp.concatenate([(u[:, :128] * share).T, (u[:, 128:] * share).T], axis=1)


def own_body(w_ref, q_ref, v_ref, s_ref, own_ref, direction_ref, hat_ref, length_ref, share_ref):
    core = lax.axis_index("blk")
    own = summed(w_ref, pl.multiple_of(core * 128, 128), 128)
    share = own_share(s_ref)
    share_ref[...] = jnp.broadcast_to(share, share_ref.shape)
    q, q_len = unit(q_ref[...])
    v, v_len = unit(v_ref[...])
    q_hat, v_hat = q.astype(bf16).astype(f32), v.astype(bf16).astype(f32)

    def leave(direction, other_hat, length):
        direction_ref[...] = direction
        hat_ref[...] = other_hat
        length_ref[...] = jnp.broadcast_to(length, length_ref.shape)

    def item():
        own_ref[...] = slope(own, q_hat, v, v_len)
        leave(q, v_hat, q_len)

    def query():
        own_ref[...] = slope(query_pull(own, share), v_hat, q, q_len)
        leave(v, q_hat, v_len)

    by_role(item, query)


def final_body(own_ref, direction_ref, hat_ref, length_ref, share_ref, give_ref, got_ref, qs_ref, vs_ref, loss_ref):
    def other(pulled):
        return slope(pulled, hat_ref[...], direction_ref[...], length_ref[...])

    def item():
        vs_ref[...] = own_ref[...]
        qs_ref[...] = other(query_pull(got_ref[:128], share_ref[:1]))
        loss_ref[0, 0] = jnp.max(give_ref[128:136]) / (128 * 128)

    def query():
        qs_ref[...] = own_ref[...]
        vs_ref[...] = other(got_ref[:128])
        loss_ref[0, 0] = jnp.max(got_ref[128:136]) / (128 * 128)

    by_role(item, query)


def per_device(queries, items):
    rows = (ROWS, D)
    bulk = (GROUP, 2, ROWS, D)
    in_hbm = [pltpu.with_memory_space_constraint(a, pltpu.HBM) for a in (queries, items)]
    mine, pos, q_raw, v_raw = call(
        norm_body,
        [(rows, bf16), ((8, 128), f32), (rows, bf16), (rows, bf16)],
        "norm",
        10**9,
        ins=[pl.BlockSpec(memory_space=pltpu.HBM)] * 2,
        scratch=[pltpu.SemaphoreType.DMA((2,))],
    )(*in_hbm)
    (tile,) = call(tile_body, [(bulk, bf16)], "tile")(mine, swap_cores(queries), swap_cores(items))
    block = exchange(tile, BULK)
    flops = 2 * 2048 * 1024 * 256
    cut = (GROUP, ROWS, D)
    (a,) = call(half_body, [(cut, bf16)], "half")(block)
    got_a = swap_cores(a)
    (b,) = call(rest_body, [(cut, bf16)], "rest")(block)
    got_b = swap_cores(b)
    scored = ((4, 256, 1024), bf16)
    e0, t = call(score0_body, [scored, ((8, GROUP * ROWS), f32)], "score0", flops)(block, got_a)
    e1, s = call(
        score1_body, [scored, ((GROUP, 16, 128), f32)], "score1", flops
    )(block, got_a, got_b, t, pos)
    sums = exchange(s, QUERY)
    pulled = (GROUP * ROWS, D)
    (give,) = call(first_body, [((1040, D), bf16)], "first", flops)(e0, e1, block, sums)
    got0 = swap_cores(give)
    keep0, give = call(
        second_body, [((2, 256, D), f32), (pulled, bf16)], "second", flops
    )(e0, e1, block, got_a, sums)
    got1 = swap_cores(give)
    keep1, keep2, u = call(
        third_body, [((2, 256, D), f32), ((4, 256, D), f32), (pulled, bf16)], "third", flops
    )(e0, e1, got_a, got_b, sums)
    packed = (GROUP, 264, D)
    (part,) = call(merge_body, [(packed, bf16)], "merge", flops)(keep0, keep1, u, got0, sums)
    (out,) = call(join_body, [(packed, bf16)], "join")(part, keep2, got1)
    out = exchange(out, BULK)
    (give,) = call(give_body, [((136, D), f32)], "give")(out)
    got = swap_cores(give)
    ready = call(own_body, [(rows, f32)] * 4 + [((8, 128), f32)], "own", flops)(out, q_raw, v_raw, sums)
    q_slope, v_slope, loss = call(
        final_body, [(rows, f32), (rows, f32), ((1, 1), f32, pltpu.SMEM)], "final"
    )(*ready, give, got)
    return loss.reshape(()), q_slope, v_slope


def solution(mesh):
    split = Mesh(mesh.devices.reshape(2, 4, 4, 4), AXES)
    rows = P(AXES, None)
    return jax.shard_map(
        per_device, mesh=split, in_specs=(rows, rows), out_specs=(P(), rows, rows), check_vma=False
    )
```
